8 devices in a mesh: dp: 1 (over z), yz: 2 (over y), x: 4 (over x, core).
Axes of the slice: x: 2, y: 2, z: 1, core: 2. Of those that a mesh axis runs over, the one named last changes fastest.
Arguments:
- x_in: bfloat16 [128, 4096], P('dp', ('x', 'yz'))
- ln_gain: bfloat16 [4096], P(('x', 'yz'))
- w_qkv: bfloat16 [4096, 4608], P('x', 'yz')
- w_gate: bfloat16 [4096, 16384], P('x', 'yz')
- w_up: bfloat16 [4096, 16384], P('x', 'yz')
- w_attn_out: bfloat16 [4096, 4096], P('yz', 'x')
- w_mlp_out: bfloat16 [16384, 4096], P('yz', 'x')
- k_cache: bfloat16 [128, 4096, 256], P(('dp', 'x', 'yz'))
- v_cache: bfloat16 [128, 4096, 256], P(('dp', 'x', 'yz'))
- ctx_len: int32 [128], P(('dp', 'x', 'yz'))
Outputs:
- output 1: bfloat16 [128, 4096], P('dp', ('x', 'yz'))
- output 2: bfloat16 [128, 4096, 256], P(('dp', 'x', 'yz'))
- output 3: bfloat16 [128, 4096, 256], P(('dp', 'x', 'yz'))
All inputs are finite; a program needn't handle non-finite values.
Results may differ from the reference program's by a relative error of at most 0.00714708.
Values are sent between devices in bfloat16 or wider.
A program may use at most 1 GiB of HBM per device.

```python
import jax
import jax.numpy as jnp
from jax import lax

BATCH_SIZE = 128
D_MODEL = 4096
NUM_HEADS = 16
HEAD_DIM = 256
FF_DIM = 16384
CACHE_LEN = 4096


def setup_inputs(seed: int = 0, part: int = 0) -> dict:
    part_key = jax.random.fold_in(jax.random.key(seed), part)
    shared_key = jax.random.key(seed + 1)
    x_key, kc_key, vc_key, vm_key, len_key = jax.random.split(part_key, 5)
    g_key, qkv_key, gate_key, up_key, ao_key, mo_key = jax.random.split(shared_key, 6)
    qkv_cols = (NUM_HEADS + 2) * HEAD_DIM
    attn_cols = NUM_HEADS * HEAD_DIM
    x_in = jax.random.normal(x_key, (BATCH_SIZE, D_MODEL), jnp.float32)
    ln_gain = jax.random.uniform(g_key, (D_MODEL,), jnp.float32, 0.5, 1.5)
    w_qkv = jax.random.normal(qkv_key, (D_MODEL, qkv_cols), jnp.float32) * D_MODEL ** -0.5
    w_gate = jax.random.normal(gate_key, (D_MODEL, FF_DIM), jnp.float32) * D_MODEL ** -0.5
    w_up = jax.random.normal(up_key, (D_MODEL, FF_DIM), jnp.float32) * D_MODEL ** -0.5
    w_attn_out = jax.random.normal(ao_key, (attn_cols, D_MODEL), jnp.float32) * attn_cols ** -0.5
    w_mlp_out = jax.random.normal(mo_key, (FF_DIM, D_MODEL), jnp.float32) * FF_DIM ** -0.5
    k_cache = jax.random.normal(kc_key, (BATCH_SIZE, CACHE_LEN, HEAD_DIM), jnp.float32)
    v_mean = jax.random.normal(vm_key, (BATCH_SIZE, 1, HEAD_DIM), jnp.float32)
    v_cache = v_mean + 0.7 * jax.random.normal(vc_key, (BATCH_SIZE, CACHE_LEN, HEAD_DIM), jnp.float32)
    ctx_len = jax.random.randint(len_key, (BATCH_SIZE,), CACHE_LEN // 8, CACHE_LEN, jnp.int32)
    ctx_len = ctx_len.at[0].set(CACHE_LEN - 1).at[1].set(CACHE_LEN // 8)
    return {
        "x_in": x_in.astype(jnp.bfloat16),
        "ln_gain": ln_gain.astype(jnp.bfloat16),
        "w_qkv": w_qkv.astype(jnp.bfloat16),
        "w_gate": w_gate.astype(jnp.bfloat16),
        "w_up": w_up.astype(jnp.bfloat16),
        "w_attn_out": w_attn_out.astype(jnp.bfloat16),
        "w_mlp_out": w_mlp_out.astype(jnp.bfloat16),
        "k_cache": k_cache.astype(jnp.bfloat16),
        "v_cache": v_cache.astype(jnp.bfloat16),
        "ctx_len": ctx_len,
    }


def apply_rope(vecs, positions):
    half_dim = vecs.shape[-1] // 2
    inv_freq = 10000.0 ** (-jnp.arange(half_dim, dtype=jnp.float32) / half_dim)
    angles = positions.astype(jnp.float32)[..., None] * inv_freq
    cos_t = jnp.cos(angles)
    sin_t = jnp.sin(angles)
    first_half = vecs[..., :half_dim]
    second_half = vecs[..., half_dim:]
    return jnp.concatenate([first_half * cos_t - second_half * sin_t, second_half * cos_t + first_half * sin_t], axis=-1)


def layer_norm(x_in, ln_gain):
    x_f32 = x_in.astype(jnp.float32)
    row_mean = jnp.sum(x_f32, axis=-1, keepdims=True) / D_MODEL
    row_var = jnp.sum(x_f32 * x_f32, axis=-1, keepdims=True) / D_MODEL - row_mean * row_mean
    normed = (x_f32 - row_mean) * lax.rsqrt(row_var + 1e-6) * ln_gain.astype(jnp.float32)
    return normed.astype(jnp.bfloat16)


def reference(x_in, ln_gain, w_qkv, w_gate, w_up, w_attn_out, w_mlp_out, k_cache, v_cache, ctx_len):
    normed = layer_norm(x_in, ln_gain)
    qkv_proj = jnp.dot(normed, w_qkv, preferred_element_type=jnp.float32).astype(jnp.bfloat16)
    gate_proj = jnp.dot(normed, w_gate, preferred_element_type=jnp.float32).astype(jnp.bfloat16)
    up_proj = jnp.dot(normed, w_up, preferred_element_type=jnp.float32).astype(jnp.bfloat16)
    mlp_act = (jax.nn.silu(gate_proj.astype(jnp.float32)) * up_proj.astype(jnp.float32)).astype(jnp.bfloat16)
    attn_cols = NUM_HEADS * HEAD_DIM
    q_heads = qkv_proj[:, :attn_cols].reshape(BATCH_SIZE, NUM_HEADS, HEAD_DIM)
    k_new = qkv_proj[:, attn_cols:attn_cols + HEAD_DIM]
    v_new = qkv_proj[:, attn_cols + HEAD_DIM:]
    q_rot = apply_rope(q_heads.astype(jnp.float32), ctx_len[:, None]).astype(jnp.bfloat16)
    k_rot = apply_rope(k_new.astype(jnp.float32), ctx_len).astype(jnp.bfloat16)
    positions = jnp.arange(CACHE_LEN)
    new_slot = (positions[None, :] == ctx_len[:, None])[:, :, None]
    k_out = jnp.where(new_slot, k_rot[:, None, :], k_cache)
    v_out = jnp.where(new_slot, v_new[:, None, :], v_cache)
    block_rows = 8
    n_blocks = BATCH_SIZE // block_rows

    def attend(block_in):
        q_blk, k_blk, v_blk, len_blk = block_in
        scores = jnp.einsum("bhd,btd->bht", q_blk.astype(jnp.float32), k_blk.astype(jnp.float32)) * HEAD_DIM ** -0.5
        visible = (positions[None, :] <= len_blk[:, None])[:, None, :]
        scores = jnp.where(visible, scores, -1e30)
        attn_probs = jax.nn.softmax(scores, axis=-1).astype(jnp.bfloat16)
        return jnp.einsum("bht,btd->bhd", attn_probs.astype(jnp.float32), v_blk.astype(jnp.float32)).astype(jnp.bfloat16)

    attn_heads = lax.map(attend, (
        q_rot.reshape(n_blocks, block_rows, NUM_HEADS, HEAD_DIM),
        k_out.reshape(n_blocks, block_rows, CACHE_LEN, HEAD_DIM),
        v_out.reshape(n_blocks, block_rows, CACHE_LEN, HEAD_DIM),
        ctx_len.reshape(n_blocks, block_rows),
    ))
    attn_flat = attn_heads.reshape(BATCH_SIZE, attn_cols)
    z_sum = jnp.dot(attn_flat, w_attn_out, preferred_element_type=jnp.float32) + jnp.dot(mlp_act, w_mlp_out, preferred_element_type=jnp.float32)
    y_out = (x_in.astype(jnp.float32) + z_sum).astype(jnp.bfloat16)
    return (y_out, k_out, v_out)
```

```python
import functools

import jax
import jax.numpy as jnp
from jax import lax
from jax.experimental import pallas as pl
from jax.experimental.pallas import tpu as pltpu
from jax.sharding import PartitionSpec as P

MESH = pl.DeviceIdType.MESH
VMEM_LIMIT = 67043328
TILE = 512
NT = 8
QC = 768
NQ = 3

f32 = jnp.float32
bf16 = jnp.bfloat16


def local_copy(src, dst, sem):
    return pltpu.make_async_copy(src, dst, sem)


def remote_copy(src, dst, ssem, rsem, dev):
    return pltpu.make_async_remote_copy(src, dst, ssem, rsem, device_id=dev, device_id_type=MESH)


def in_proj_kernel(x_ref, g_ref, wq_ref, wg_ref, wu_ref, qkv_ref, s_ref, d_ref,
                   wqv, wv, xr, gr, st, stx, h, qp, qr, qxs, qxr, qf, qyr, sbuf, rbuf, obuf,
                   wqsem, wsem, xs_sem, xr_sem, gs_sem, gr_sem, sts_sem, str_sem,
                   qds_sem, qdr_sem, qxs_sem, qxr_sem, qys_sem, qyr_sem, ds_sem, dr_sem, out_sem):
    d_model = 4096
    x = lax.axis_index("x")
    yz = lax.axis_index("yz")
    core = lax.rem(x, 2)
    x_core = x + 1 - 2 * core
    x_chip = lax.rem(x + 2, 4)
    x_diag = x_chip + 1 - 2 * core
    me = 2 * x + yz
    partner = {"x": x_core}
    xpeer = {"x": x_chip}
    ypeer = {"yz": 1 - yz}

    def wq_copy(j):
        return local_copy(wq_ref.at[:, pl.ds(QC * j, QC)], wqv.at[j], wqsem.at[j])

    quarters = (x_diag, x_chip, x_core, x)

    def w_copy(w_hbm, quarter, t, slot):
        cols = pl.multiple_of(quarter * 2048 + t * TILE, TILE)
        return local_copy(w_hbm.at[:, pl.ds(cols, TILE)], wv.at[slot], wsem.at[slot])

    for j in range(NQ):
        wq_copy(j).start()
    for ph in range(4):
        for t in range(4):
            w_copy(wg_ref, quarters[ph], t, ph * NT + 2 * t).start()
            w_copy(wu_ref, quarters[ph], t, ph * NT + 2 * t + 1).start()

    def w_wait(slot):
        local_copy(wg_ref.at[:, pl.ds(0, TILE)], wv.at[slot], wsem.at[slot]).wait()

    xf = x_ref[...].astype(f32)
    s1 = jnp.sum(xf, axis=1, keepdims=True)
    s2 = jnp.sum(xf * xf, axis=1, keepdims=True)
    lane = lax.broadcasted_iota(jnp.int32, (128, 128), 1)
    stat = jnp.where(lane == 0, s1, s2).T
    st[me] = stat[0:8]

    barrier = pltpu.get_barrier_semaphore()
    others = []
    for dx in range(4):
        for dy in range(2):
            if dx or dy:
                others.append((lax.rem(x + dx, 4), lax.rem(yz + dy, 2)))
    for ox, oy in others:
        pl.semaphore_signal(barrier, inc=1, device_id={"x": ox, "yz": oy}, device_id_type=MESH)
    pl.semaphore_wait(barrier, 7)

    for n, (ox, oy) in enumerate(others):
        remote_copy(st.at[me], stx.at[me], sts_sem.at[n], str_sem.at[me], {"x": ox, "yz": oy}).start()
    x_send = remote_copy(x_ref, xr, xs_sem, xr_sem, ypeer)
    g_send = remote_copy(g_ref, gr, gs_sem, gr_sem, ypeer)
    x_send.start()
    g_send.start()
    stx[me] = st[me]
    for n, (ox, oy) in enumerate(others):
        src = 2 * ox + oy
        remote_copy(st.at[me], stx.at[src], sts_sem.at[n], str_sem.at[src], {"x": ox, "yz": oy}).wait()
    tot = jnp.sum(stx[...], axis=0)
    tot = jnp.concatenate([tot, jnp.zeros((120, 128), f32)], axis=0).T
    mean = tot[:, 0:1] / d_model
    var = tot[:, 1:2] / d_model - mean * mean
    rstd = lax.rsqrt(var + 1e-6)
    own_cols = pl.multiple_of(yz * 512, 512)
    peer_cols = pl.multiple_of((1 - yz) * 512, 512)
    h[:, pl.ds(own_cols, 512)] = ((xf - mean) * rstd * g_ref[0:1, :]).astype(bf16)
    x_send.wait()
    g_send.wait()
    h[:, pl.ds(peer_cols, 512)] = ((xr[...].astype(f32) - mean) * rstd * gr[0:1, :]).astype(bf16)

    def q_compute(j):
        wq_copy(j).wait()
        part = jnp.dot(h[...], wqv[j], preferred_element_type=f32)
        qp[j] = part.reshape(4, 32, QC)

    def q_pair(j, k):
        block = (x_diag, x_core)[k]
        return remote_copy(qp.at[j, block], qr.at[j, k], qds_sem.at[j, k], qdr_sem.at[j, k], partner)

    def q_pair_start(j):
        q_pair(j, 0).start()
        q_pair(j, 1).start()

    def q_chip(j):
        return remote_copy(qxs.at[j], qxr.at[j], qxs_sem.at[j], qxr_sem.at[j], xpeer)

    def q_sum(j):
        q_pair(j, 0).wait()
        qxs[j] = qp[j, x_chip] + qr[j, 0]

    def tile(slot):
        w_wait(slot)
        return jnp.dot(h[...], wv[slot], preferred_element_type=f32)

    def d_copy(i):
        return remote_copy(sbuf.at[i], rbuf.at[i], ds_sem.at[i], dr_sem.at[i], partner)

    def s_out(i):
        return local_copy(obuf.at[i], s_ref.at[i], out_sem.at[i])

    def d_out(i):
        return local_copy(obuf.at[NT + i], d_ref.at[i], out_sem.at[NT + i])

    q_compute(0)
    q_compute(1)
    q_pair_start(0)
    q_compute(2)
    q_pair_start(1)

    after = {
        0: lambda: q_pair_start(2),
        1: lambda: q_sum(0),
        2: lambda: (q_chip(0).start(), q_sum(1)),
        3: lambda: (q_chip(1).start(), q_sum(2)),
        4: lambda: q_chip(2).start(),
    }
    for i in range(NT):
        sbuf[i] = tile(i)
        if i:
            d_copy(i - 1).start()
        if i in after:
            after[i]()

    for i in range(NT):
        part = tile(NT + i)
        if i == 0:
            d_copy(NT - 1).start()
        d_copy(i).wait()
        obuf[i] = part + rbuf[i]
        if i:
            s_out(i - 1).start()

    def send_body(i, _):
        sbuf[NT + i] = tile(2 * NT + i)

        @pl.when(i == 0)
        def _():
            s_out(NT - 1).start()

        @pl.when(i > 0)
        def _():
            d_copy(NT + i - 1).start()
        return 0

    lax.fori_loop(0, NT, send_body, 0)

    def keep_body(i, _):
        part = tile(3 * NT + i)

        @pl.when(i == 0)
        def _():
            d_copy(2 * NT - 1).start()
        d_copy(NT + i).wait()
        obuf[NT + i] = part + rbuf[NT + i]

        @pl.when(i > 0)
        def _():
            d_out(i - 1).start()
        return 0

    lax.fori_loop(0, NT, keep_body, 0)

    own_rows = pl.multiple_of(yz * 16, 16)
    peer_rows = pl.multiple_of((1 - yz) * 16, 16)

    def q_y(j):
        return remote_copy(qf.at[j, pl.ds(peer_rows, 16)], qyr.at[j], qys_sem.at[j], qyr_sem.at[j], ypeer)

    for j in range(NQ):
        q_pair(j, 1).wait()
        if j == 0:
            d_out(NT - 1).start()
        q_chip(j).wait()
        qf[j] = (qp[j, x] + qr[j, 1] + qxr[j]).astype(bf16)
        if j:
            q_y(j - 1).start()
    for j in range(NQ):
        qkv_ref[yz, :, pl.ds(QC * j, QC)] = qf[j, pl.ds(own_rows, 16)]
    q_y(NQ - 1).start()
    for j in range(NQ):
        q_y(j).wait()
        qkv_ref[1 - yz, :, pl.ds(QC * j, QC)] = qyr[j]
    for i in range(NT):
        s_out(i).wait()
        d_out(i).wait()


def in_proj(x_loc, gain, wq, wg, wu):
    anyspec = pl.BlockSpec(memory_space=pltpu.HBM)
    vspec = pl.BlockSpec(memory_space=pltpu.VMEM)
    dma = pltpu.SemaphoreType.DMA
    return pl.pallas_call(
        in_proj_kernel,
        out_shape=[
            jax.ShapeDtypeStruct((2, 16, NQ * QC), bf16),
            jax.ShapeDtypeStruct((NT, 128, TILE), f32),
            jax.ShapeDtypeStruct((NT, 128, TILE), f32),
        ],
        in_specs=[vspec, vspec, anyspec, anyspec, anyspec],
        out_specs=[vspec, anyspec, anyspec],
        scratch_shapes=[
            pltpu.VMEM((NQ, 1024, QC), bf16),
            pltpu.VMEM((4 * NT, 1024, TILE), bf16),
            pltpu.VMEM((128, 512), bf16),
            pltpu.VMEM((8, 512), f32),
            pltpu.VMEM((8, 8, 128), f32),
            pltpu.VMEM((8, 8, 128), f32),
            pltpu.VMEM((128, 1024), bf16),
            pltpu.VMEM((NQ, 4, 32, QC), f32),
            pltpu.VMEM((NQ, 2, 32, QC), f32),
            pltpu.VMEM((NQ, 32, QC), f32),
            pltpu.VMEM((NQ, 32, QC), f32),
            pltpu.VMEM((NQ, 32, QC), bf16),
            pltpu.VMEM((NQ, 16, QC), bf16),
            pltpu.VMEM((2 * NT, 128, TILE), f32),
            pltpu.VMEM((2 * NT, 128, TILE), f32),
            pltpu.VMEM((2 * NT, 128, TILE), f32),
            dma((NQ,)), dma((4 * NT,)), dma, dma, dma, dma, dma((7,)), dma((8,)),
            dma((NQ, 2)), dma((NQ, 2)), dma((NQ,)), dma((NQ,)), dma((NQ,)), dma((NQ,)),
            dma((2 * NT,)), dma((2 * NT,)), dma((2 * NT,)),
        ],
        compiler_params=pltpu.CompilerParams(
            collective_id=0, has_side_effects=True, vmem_limit_bytes=VMEM_LIMIT),
        cost_estimate=pl.CostEstimate(flops=5_000_000_000, bytes_accessed=45_000_000, transcendentals=0),
        name="in_proj",
    )(x_loc, gain, wq, wg, wu)


SLOTS = 5


def attend_kernel(len_ref, qkv_ref, cos_ref, sin_ref, k_ref, v_ref, ko_ref, vo_ref, o_ref,
                  kb, vb, qs, kns, vns, osc, ksem, vsem, kosem, vosem):
    n = k_ref.shape[0]
    t_len = k_ref.shape[1]

    def k_in(r, s):
        return local_copy(k_ref.at[r], kb.at[s], ksem.at[s])

    def v_in(r, s):
        return local_copy(v_ref.at[r], vb.at[s], vsem.at[s])

    def k_out(r, s):
        return local_copy(kb.at[s], ko_ref.at[r], kosem.at[s])

    def v_out(r, s):
        return local_copy(vb.at[s], vo_ref.at[r], vosem.at[s])

    AHEAD = 3
    for r in range(AHEAD):
        k_in(r, r).start()
        v_in(r, r).start()

    cos_t = cos_ref[...]
    sin_t = sin_ref[...]
    for g in range(17):
        part, base = (0, g * 256) if g < 9 else (1, (g - 9) * 256)
        a = qkv_ref[part, :, base:base + 128].astype(f32)
        b = qkv_ref[part, :, base + 128:base + 256].astype(f32)
        lo = (a * cos_t - b * sin_t).astype(bf16).astype(f32)
        hi = (b * cos_t + a * sin_t).astype(bf16).astype(f32)
        if g < 16:
            qs[:, g, 0:128] = lo
            qs[:, g, 128:256] = hi
        else:
            kns[:, 0:128] = lo
            kns[:, 128:256] = hi
    vns[...] = qkv_ref[1, :, 2048:2304].astype(f32)

    row16 = lax.broadcasted_iota(jnp.int32, (16, 256), 0)
    pos = lax.broadcasted_iota(jnp.int32, (16, t_len), 1)

    def body(r, _):
        s = lax.rem(r, SLOTS)
        nxt = r + AHEAD

        @pl.when(nxt < n)
        def _():
            s2 = lax.rem(nxt, SLOTS)

            @pl.when(nxt >= SLOTS)
            def _():
                k_out(nxt - SLOTS, s2).wait()
                v_out(nxt - SLOTS, s2).wait()
            k_in(nxt, s2).start()
            v_in(nxt, s2).start()

        p = len_ref[r]
        base = pl.multiple_of((p // 16) * 16, 16)
        hit = row16 == p - base
        k_in(r, s).wait()
        krow = kb[s, pl.ds(base, 16), :]
        kb[s, pl.ds(base, 16), :] = jnp.where(hit, kns[pl.ds(r, 1), :].astype(bf16), krow)
        q = qs[r].astype(bf16)
        sc = lax.dot_general(q, kb[s], (((1,), (1,)), ((), ())), preferred_element_type=f32) * (256 ** -0.5)
        k_out(r, s).start()
        v_in(r, s).wait()
        vrow = vb[s, pl.ds(base, 16), :]
        vb[s, pl.ds(base, 16), :] = jnp.where(hit, vns[pl.ds(r, 1), :].astype(bf16), vrow)
        sc = jnp.where(pos <= p, sc, -1e30)
        m = jnp.max(sc, axis=1, keepdims=True)
        e = jnp.exp(sc - m)
        den = jnp.sum(e, axis=1, keepdims=True)
        pr = (e / den).astype(bf16)
        osc[r] = jnp.dot(pr, vb[s], preferred_element_type=f32).astype(bf16).astype(f32)
        v_out(r, s).start()
        return 0

    lax.fori_loop(0, n, body, 0)
    for g in range(16):
        o_ref[:, 256 * g:256 * (g + 1)] = osc[:, g, :].astype(bf16)
    for r in range(n - SLOTS, n):
        k_out(r, r % SLOTS).wait()
        v_out(r, r % SLOTS).wait()


def attend(lens, qkv, cos_t, sin_t, kc, vc):
    anyspec = pl.BlockSpec(memory_space=pltpu.HBM)
    vspec = pl.BlockSpec(memory_space=pltpu.VMEM)
    dma = pltpu.SemaphoreType.DMA
    n, t_len, hd = kc.shape
    return pl.pallas_call(
        attend_kernel,
        out_shape=[
            jax.ShapeDtypeStruct(kc.shape, bf16),
            jax.ShapeDtypeStruct(vc.shape, bf16),
            jax.ShapeDtypeStruct((n, 4096), bf16),
        ],
        in_specs=[pl.BlockSpec(memory_space=pltpu.SMEM), vspec, vspec, vspec, anyspec, anyspec],
        out_specs=[anyspec, anyspec, vspec],
        scratch_shapes=[
            pltpu.VMEM((SLOTS, t_len, hd), bf16),
            pltpu.VMEM((SLOTS, t_len, hd), bf16),
            pltpu.VMEM((n, 16, hd), f32),
            pltpu.VMEM((n, hd), f32),
            pltpu.VMEM((n, hd), f32),
            pltpu.VMEM((n, 16, hd), f32),
            dma((SLOTS,)), dma((SLOTS,)), dma((SLOTS,)), dma((SLOTS,)),
        ],
        compiler_params=pltpu.CompilerParams(vmem_limit_bytes=40 * 2 ** 20),
        cost_estimate=pl.CostEstimate(flops=40_000_000_000, bytes_accessed=134_000_000, transcendentals=1_000_000),
        name="attend",
    )(lens, qkv, cos_t, sin_t, kc, vc)


def out_proj_kernel(o_ref, x_ref, d_ref, r_ref, wao_ref, wmo_ref, y_ref,
                    db, rb, wao, wmo, ab, ob, zs, zk, zr,
                    dsem, rsem, waosem, wmosem, a1s, a1r, a2s, a2r, a3s, a3r,
                    o0s, o0r, o1s, o1r, o2s, o2r, o3s, o3r, zss, zrs):
    x = lax.axis_index("x")
    yz = lax.axis_index("yz")
    core = lax.rem(x, 2)
    x_core = x + 1 - 2 * core
    x_chip = lax.rem(x + 2, 4)
    x_diag = x_chip + 1 - 2 * core
    partner = {"x": x_core}
    xpeer = {"x": x_chip}
    ypeer = {"yz": 1 - yz}

    def d_in(i):
        return local_copy(d_ref.at[i], db.at[i], dsem.at[i])

    def r_in(i):
        return local_copy(r_ref.at[i], rb.at[i], rsem.at[i])

    for i in range(NT):
        d_in(i).start()
        r_in(i).start()
    order = (x, x_core, x_chip, x_diag)

    def wmo_in(n, t):
        rows = pl.multiple_of(order[n] * 2048 + t * TILE, TILE)
        return local_copy(wmo_ref.at[pl.ds(rows, TILE), :], wmo.at[n * 4 + t], wmosem.at[n * 4 + t])

    wao_in = local_copy(wao_ref, wao, waosem)
    for n in range(4):
        for t in range(4):
            wmo_in(n, t).start()
        if n == 1:
            wao_in.start()

    barrier = pltpu.get_barrier_semaphore()
    for dev in (partner, xpeer, ypeer):
        pl.semaphore_signal(barrier, inc=1, device_id=dev, device_id_type=MESH)
    pl.semaphore_wait(barrier, 3)

    own_half = pl.multiple_of(yz * 2048, 2048)
    peer_half = pl.multiple_of((1 - yz) * 2048, 2048)
    mine = 2 * x + yz
    o_y = remote_copy(o_ref.at[:, pl.ds(peer_half, 2048)], ob.at[mine], o0s, o0r, ypeer)
    o_y.start()
    ob[mine] = o_ref[:, pl.ds(own_half, 2048)]

    def a_part(t):
        return remote_copy(ab.at[x, t], ab.at[x, t], a1s.at[t], a1r.at[t], partner)

    def a_chip(t):
        return remote_copy(ab.at[x, t], ab.at[x, t], a2s.at[t], a2r.at[t], xpeer)

    def a_fwd(t):
        return remote_copy(ab.at[x_chip, t], ab.at[x_chip, t], a3s.at[t], a3r.at[t], partner)

    def o_block(b):
        return ob.at[pl.ds(2 * b, 2)]

    o_part = remote_copy(o_block(x), o_block(x), o1s, o1r, partner)
    o_chip = remote_copy(o_block(x), o_block(x), o2s, o2r, xpeer)
    o_fwd = remote_copy(o_block(x_chip), o_block(x_chip), o3s, o3r, partner)

    for t in range(4):
        for i in (2 * t, 2 * t + 1):
            d_in(i).wait()
            r_in(i).wait()
        gate = (db[2 * t] + rb[2 * t]).astype(bf16).astype(f32)
        up = (db[2 * t + 1] + rb[2 * t + 1]).astype(bf16).astype(f32)
        ab[x, t] = (jax.nn.silu(gate) * up).astype(bf16)
        if t:
            a_chip(t - 1).start()
            a_part(t - 1).start()
        if t == 2:
            o_y.wait()
            o_chip.start()
            o_part.start()

    mc = pl.multiple_of((1 - yz) * 512, 512)
    kc = pl.multiple_of(yz * 512, 512)

    def mlp(n, t, first=False):
        wmo_in(n, t).wait()
        a = ab[order[n], t]
        w = wmo.at[n * 4 + t]
        ps = jnp.dot(a, w[:, pl.ds(mc, 512)], preferred_element_type=f32)
        pk = jnp.dot(a, w[:, pl.ds(kc, 512)], preferred_element_type=f32)
        if first:
            zs[...] = ps
            zk[...] = pk
        else:
            zs[...] += ps
            zk[...] += pk

    mlp(0, 0, first=True)
    a_chip(3).start()
    a_part(3).start()
    for t in range(1, 4):
        mlp(0, t)
    o_part.wait()
    for t in range(4):
        a_part(t).wait()
        mlp(1, t)
    for t in range(4):
        a_chip(t).wait()
        a_fwd(t).start()
        if t == 1:
            o_chip.wait()
            o_fwd.start()
        mlp(2, t)
        if t == 2:
            o_fwd.wait()
            wao_in.wait()
            attn = ob[...].reshape(128, 2048)
            zs[...] += jnp.dot(attn, wao[:, pl.ds(mc, 512)], preferred_element_type=f32)
            zk[...] += jnp.dot(attn, wao[:, pl.ds(kc, 512)], preferred_element_type=f32)
        if t:
            a_fwd(t - 1).wait()
            mlp(3, t - 1)
    a_fwd(3).wait()
    mlp(3, 3)
    z_y = remote_copy(zs, zr, zss, zrs, ypeer)
    z_y.start()
    z_y.wait()
    y_ref[...] = (x_ref[...].astype(f32) + (zk[...] + zr[...])).astype(bf16)


def out_proj(o, x_loc, d, r, wao, wmo):
    anyspec = pl.BlockSpec(memory_space=pltpu.HBM)
    vspec = pl.BlockSpec(memory_space=pltpu.VMEM)
    dma = pltpu.SemaphoreType.DMA
    return pl.pallas_call(
        out_proj_kernel,
        out_shape=jax.ShapeDtypeStruct((128, 512), bf16),
        in_specs=[vspec, vspec, anyspec, anyspec, anyspec, anyspec],
        out_specs=vspec,
        scratch_shapes=[
            pltpu.VMEM((NT, 128, TILE), f32),
            pltpu.VMEM((NT, 128, TILE), f32),
            pltpu.VMEM((2048, 1024), bf16),
            pltpu.VMEM((16, TILE, 1024), bf16),
            pltpu.VMEM((4, 4, 128, TILE), bf16),
            pltpu.VMEM((8, 16, 2048), bf16),
            pltpu.VMEM((128, 512), f32),
            pltpu.VMEM((128, 512), f32),
            pltpu.VMEM((128, 512), f32),
            dma((NT,)), dma((NT,)), dma, dma((16,)),
            dma((4,)), dma((4,)), dma((4,)), dma((4,)), dma((4,)), dma((4,)),
            dma, dma, dma, dma, dma, dma, dma, dma, dma, dma,
        ],
        compiler_params=pltpu.CompilerParams(
            collective_id=1, has_side_effects=True, vmem_limit_bytes=48 * 2 ** 20),
        cost_estimate=pl.CostEstimate(flops=3_000_000_000, bytes_accessed=26_000_000, transcendentals=0),
        name="out_proj",
    )(o, x_loc, d, r, wao, wmo)


def solution(mesh):
    both_axes = ("x", "yz")
    row_spec = P("dp", both_axes)
    in_w_spec = P("x", "yz")
    out_w_spec = P("yz", "x")
    cache_spec = P(("dp", "x", "yz"), None, None)
    len_spec = P(("dp", "x", "yz"))
    swap = [(0, 2), (2, 0), (1, 3), (3, 1)]

    def local_layer(x_loc, gain_loc, wqkv_loc, wgate_loc, wup_loc, wao_loc, wmo_loc, kc_loc, vc_loc, len_loc):
        gain = jnp.broadcast_to(gain_loc.astype(f32)[None, :], (8, 512))
        inv_freq = 10000.0 ** (-jnp.arange(128, dtype=f32) / 128)
        angles = len_loc.astype(f32)[:, None] * inv_freq
        cos_t = jnp.cos(angles)
        sin_t = jnp.sin(angles)
        qkv, s, d = in_proj(x_loc, gain, wqkv_loc, wgate_loc, wup_loc)
        r = lax.ppermute(s, "x", swap)
        k_all, v_all, o = attend(len_loc, qkv, cos_t, sin_t, kc_loc, vc_loc)
        y_loc = out_proj(o, x_loc, d, r, wao_loc, wmo_loc)
        return y_loc, k_all, v_all

    in_specs = (row_spec, P(both_axes), in_w_spec, in_w_spec, in_w_spec, out_w_spec, out_w_spec, cache_spec, cache_spec, len_spec)
    out_specs = (row_spec, cache_spec, cache_spec)
    return jax.shard_map(local_layer, mesh=mesh, in_specs=in_specs, out_specs=out_specs, check_vma=False)
```

```python
import functools

import jax
import jax.numpy as jnp
from jax import lax
from jax.experimental import pallas as pl
from jax.experimental.pallas import tpu as pltpu
from jax.sharding import PartitionSpec as P

MESH = pl.DeviceIdType.MESH
VMEM_LIMIT = 67043328
TILE = 512
NT = 8
QC = 768
NQ = 3
W_FIRST = 8
W_AHEAD = 12

f32 = jnp.float32
bf16 = jnp.bfloat16


def local_copy(src, dst, sem):
    return pltpu.make_async_copy(src, dst, sem)


def remote_copy(src, dst, ssem, rsem, dev):
    return pltpu.make_async_remote_copy(src, dst, ssem, rsem, device_id=dev, device_id_type=MESH)


def in_proj_kernel(x_hbm, g_hbm, wq_ref, wg_ref, wu_ref, qkv_ref, s_ref, d_ref,
                   wqv, wv, x_ref, g_ref, xr, gr, qout, st, stx, h, qp, qr, qxs, qxr, qf, qyr, sbuf, rbuf, obuf,
                   wqsem, wsem, xs_sem, xr_sem, gs_sem, gr_sem, sts_sem, str_sem,
                   qds_sem, qdr_sem, qxs_sem, qxr_sem, qys_sem, qyr_sem, ds_sem, dr_sem, out_sem, xin_sem, gin_sem, qo_sem):
    d_model = 4096
    x = lax.axis_index("x")
    yz = lax.axis_index("yz")
    core = lax.rem(x, 2)
    x_core = x + 1 - 2 * core
    x_chip = lax.rem(x + 2, 4)
    x_diag = x_chip + 1 - 2 * core
    me = 2 * x + yz
    partner = {"x": x_core}
    xpeer = {"x": x_chip}
    ypeer = {"yz": 1 - yz}

    barrier = pltpu.get_barrier_semaphore()
    others = []
    for dx in range(4):
        for dy in range(2):
            if dx or dy:
                others.append((lax.rem(x + dx, 4), lax.rem(yz + dy, 2)))
    for ox, oy in others:
        pl.semaphore_signal(barrier, inc=1, device_id={"x": ox, "yz": oy}, device_id_type=MESH)
    x_in = local_copy(x_hbm, x_ref, xin_sem)
    g_in = local_copy(g_hbm, g_ref, gin_sem)
    x_in.start()
    g_in.start()

    def wq_copy(j):
        return local_copy(wq_ref.at[:, pl.ds(QC * j, QC)], wqv.at[j], wqsem.at[j])

    quarters = (x_diag, x_chip, x_core, x)

    def w_start(slot):
        phase = slot // NT
        q = quarters[0]
        for n in range(1, 4):
            q = jnp.where(phase == n, quarters[n], q)
        cols = pl.multiple_of(q * 2048 + (slot % NT) // 2 * TILE, TILE)

        def start(w_hbm):
            local_copy(w_hbm.at[:, pl.ds(cols, TILE)], wv.at[slot], wsem.at[slot]).start()

        if isinstance(slot, int):
            start(wg_ref if slot % 2 == 0 else wu_ref)
        else:
            pl.when(slot % 2 == 0)(lambda: start(wg_ref))
            pl.when(slot % 2 == 1)(lambda: start(wu_ref))

    def w_wait(slot):
        local_copy(wg_ref.at[:, pl.ds(0, TILE)], wv.at[slot], wsem.at[slot]).wait()

    x_in.wait()
    for j in range(NQ):
        wq_copy(j).start()
    for slot in range(W_FIRST):
        w_start(slot)
    g_in.wait()
    xf = x_ref[...].astype(f32)
    s1 = jnp.sum(xf, axis=1, keepdims=True)
    s2 = jnp.sum(xf * xf, axis=1, keepdims=True)
    lane = lax.broadcasted_iota(jnp.int32, (128, 128), 1)
    stat = jnp.where(lane == 0, s1, s2).T
    st[me] = stat[0:8]

    pl.semaphore_wait(barrier, 7)

    x_send = remote_copy(x_ref, xr, xs_sem, xr_sem, ypeer)
    g_send = remote_copy(g_ref, gr, gs_sem, gr_sem, ypeer)
    for n, (ox, oy) in enumerate(others):
        remote_copy(st.at[me], stx.at[me], sts_sem.at[n], str_sem.at[me], {"x": ox, "yz": oy}).start()
    g_send.start()
    x_send.start()
    stx[me] = st[me]
    for n, (ox, oy) in enumerate(others):
        src = 2 * ox + oy
        remote_copy(st.at[me], stx.at[src], sts_sem.at[n], str_sem.at[src], {"x": ox, "yz": oy}).wait()
    tot = jnp.sum(stx[...], axis=0)
    tot = jnp.concatenate([tot, jnp.zeros((120, 128), f32)], axis=0).T
    mean = tot[:, 0:1] / d_model
    var = tot[:, 1:2] / d_model - mean * mean
    rstd = lax.rsqrt(var + 1e-6)
    own_cols = pl.multiple_of(yz * 512, 512)
    peer_cols = pl.multiple_of((1 - yz) * 512, 512)
    h[:, pl.ds(own_cols, 512)] = ((xf - mean) * rstd * g_ref[...].astype(f32).reshape(1, 512)).astype(bf16)
    x_send.wait()
    g_send.wait()
    h[:, pl.ds(peer_cols, 512)] = ((xr[...].astype(f32) - mean) * rstd * gr[...].astype(f32).reshape(1, 512)).astype(bf16)

    for slot in range(W_FIRST, W_AHEAD):
        w_start(slot)

    def q_compute(j):
        wq_copy(j).wait()
        part = jnp.dot(h[...], wqv[j], preferred_element_type=f32)
        qp[j] = part.reshape(4, 32, QC)

    def q_pair(j, k):
        block = (x_diag, x_core)[k]
        return remote_copy(qp.at[j, block], qr.at[j, k], qds_sem.at[j, k], qdr_sem.at[j, k], partner)

    def q_pair_start(j):
        q_pair(j, 0).start()
        q_pair(j, 1).start()

    def q_chip(j):
        return remote_copy(qxs.at[j], qxr.at[j], qxs_sem.at[j], qxr_sem.at[j], xpeer)

    def q_sum(j):
        q_pair(j, 0).wait()
        qxs[j] = qp[j, x_chip] + qr[j, 0]

    def tile(slot):
        w_wait(slot)
        if isinstance(slot, int):
            if slot + W_AHEAD < 4 * NT:
                w_start(slot + W_AHEAD)
        else:
            @pl.when(slot + W_AHEAD < 4 * NT)
            def _():
                w_start(slot + W_AHEAD)
        return jnp.dot(h[...], wv[slot], preferred_element_type=f32)

    def d_copy(i):
        return remote_copy(sbuf.at[i], rbuf.at[i], ds_sem.at[i], dr_sem.at[i], partner)

    def s_out(i):
        return local_copy(obuf.at[i], s_ref.at[i], out_sem.at[i])

    def d_out(i):
        return local_copy(obuf.at[NT + i], d_ref.at[i], out_sem.at[NT + i])

    q_compute(0)
    q_compute(1)
    q_pair_start(0)
    q_compute(2)
    q_pair_start(1)

    after = {
        0: lambda: q_pair_start(2),
        1: lambda: q_sum(0),
        2: lambda: (q_chip(0).start(), q_sum(1)),
        3: lambda: (q_chip(1).start(), q_sum(2)),
        4: lambda: q_chip(2).start(),
    }
    for i in range(NT):
        sbuf[i] = tile(i)
        if i:
            d_copy(i - 1).start()
        if i in after:
            after[i]()

    for i in range(NT):
        part = tile(NT + i)
        if i == 0:
            d_copy(NT - 1).start()
        d_copy(i).wait()
        obuf[i] = part + rbuf[i]
        if i:
            s_out(i - 1).start()

    own_rows = pl.multiple_of(yz * 16, 16)
    peer_rows = pl.multiple_of((1 - yz) * 16, 16)

    def q_y(j):
        return remote_copy(qf.at[j, pl.ds(peer_rows, 16)], qyr.at[j], qys_sem.at[j], qyr_sem.at[j], ypeer)

    def q_final(j):
        q_pair(j, 1).wait()
        q_chip(j).wait()
        qf[j] = (qp[j, x] + qr[j, 1] + qxr[j]).astype(bf16)
        qout[yz, :, pl.ds(QC * j, QC)] = qf[j, pl.ds(own_rows, 16)]

    def send_tiles(lo, hi):
        def body(i, _):
            sbuf[NT + i] = tile(2 * NT + i)

            @pl.when(i == 0)
            def _():
                s_out(NT - 1).start()

            @pl.when(i > 0)
            def _():
                d_copy(NT + i - 1).start()
            return 0

        lax.fori_loop(lo, hi, body, 0)

    def keep_tiles(lo, hi):
        def body(i, _):
            part = tile(3 * NT + i)

            @pl.when(i == 0)
            def _():
                d_copy(2 * NT - 1).start()
            d_copy(NT + i).wait()
            obuf[NT + i] = part + rbuf[NT + i]

            @pl.when(i > 0)
            def _():
                d_out(i - 1).start()
            return 0

        lax.fori_loop(lo, hi, body, 0)

    send_tiles(0, 3)
    q_final(0)
    send_tiles(3, 4)
    q_y(0).start()
    send_tiles(4, 8)
    keep_tiles(0, 2)
    q_final(1)
    keep_tiles(2, 3)
    q_y(1).start()
    keep_tiles(3, 7)
    q_final(2)
    keep_tiles(7, 8)
    q_y(2).start()
    d_out(NT - 1).start()
    for j in range(NQ):
        q_y(j).wait()
        qout[1 - yz, :, pl.ds(QC * j, QC)] = qyr[j]
    for i in range(NT):
        s_out(i).wait()
        d_out(i).wait()
    q_out = local_copy(qout, qkv_ref, qo_sem)
    q_out.start()
    q_out.wait()


def in_proj(x_loc, gain, wq, wg, wu):
    anyspec = pl.BlockSpec(memory_space=pltpu.HBM)
    dma = pltpu.SemaphoreType.DMA
    return pl.pallas_call(
        in_proj_kernel,
        out_shape=[
            jax.ShapeDtypeStruct((2, 16, NQ * QC), bf16),
            jax.ShapeDtypeStruct((NT, 128, TILE), f32),
            jax.ShapeDtypeStruct((NT, 128, TILE), f32),
        ],
        in_specs=[anyspec] * 5,
        out_specs=[anyspec] * 3,
        scratch_shapes=[
            pltpu.VMEM((NQ, 1024, QC), bf16),
            pltpu.VMEM((4 * NT, 1024, TILE), bf16),
            pltpu.VMEM((128, 512), bf16),
            pltpu.VMEM((512,), bf16),
            pltpu.VMEM((128, 512), bf16),
            pltpu.VMEM((512,), bf16),
            pltpu.VMEM((2, 16, NQ * QC), bf16),
            pltpu.VMEM((8, 8, 128), f32),
            pltpu.VMEM((8, 8, 128), f32),
            pltpu.VMEM((128, 1024), bf16),
            pltpu.VMEM((NQ, 4, 32, QC), f32),
            pltpu.VMEM((NQ, 2, 32, QC), f32),
            pltpu.VMEM((NQ, 32, QC), f32),
            pltpu.VMEM((NQ, 32, QC), f32),
            pltpu.VMEM((NQ, 32, QC), bf16),
            pltpu.VMEM((NQ, 16, QC), bf16),
            pltpu.VMEM((2 * NT, 128, TILE), f32),
            pltpu.VMEM((2 * NT, 128, TILE), f32),
            pltpu.VMEM((2 * NT, 128, TILE), f32),
            dma((NQ,)), dma((4 * NT,)), dma, dma, dma, dma, dma((7,)), dma((8,)),
            dma((NQ, 2)), dma((NQ, 2)), dma((NQ,)), dma((NQ,)), dma((NQ,)), dma((NQ,)),
            dma((2 * NT,)), dma((2 * NT,)), dma((2 * NT,)), dma, dma, dma,
        ],
        compiler_params=pltpu.CompilerParams(
            collective_id=0, has_side_effects=True, vmem_limit_bytes=VMEM_LIMIT),
        cost_estimate=pl.CostEstimate(flops=5_000_000_000, bytes_accessed=45_000_000, transcendentals=0),
        name="in_proj",
    )(x_loc, gain, wq, wg, wu)


SLOTS = 6


def attend_kernel(len_hbm, qkv_hbm, k_ref, v_ref, ko_ref, vo_ref, o_ref,
                  kb, vb, len_ref, qkv_ref, qs, kns, vns, osc, ksem, vsem, kosem, vosem, isem):
    n = k_ref.shape[0]
    t_len = k_ref.shape[1]

    def k_in(r, s):
        return local_copy(k_ref.at[r], kb.at[s], ksem.at[s])

    def v_in(r, s):
        return local_copy(v_ref.at[r], vb.at[s], vsem.at[s])

    def k_out(r, s):
        return local_copy(kb.at[s], ko_ref.at[r], kosem.at[s])

    def v_out(r, s):
        return local_copy(vb.at[s], vo_ref.at[r], vosem.at[s])

    AHEAD = 4
    len_in = local_copy(len_hbm, len_ref, isem.at[0])
    qkv_in = local_copy(qkv_hbm, qkv_ref, isem.at[1])
    len_in.start()
    qkv_in.start()
    k_in(0, 0).start()
    v_in(0, 0).start()
    len_in.wait()
    qkv_in.wait()
    for r in range(1, AHEAD):
        k_in(r, r).start()
        v_in(r, r).start()
    row = lax.broadcasted_iota(jnp.int32, (16, 128), 0)
    lens = jnp.zeros((16, 128), jnp.int32)
    for r in range(16):
        lens = jnp.where(row == r, len_ref[r], lens)
    half = lax.broadcasted_iota(jnp.int32, (16, 128), 1).astype(f32)
    angles = lens.astype(f32) * 10000.0 ** (-half / 128)
    cos_t = jnp.cos(angles)
    sin_t = jnp.sin(angles)
    for g in range(17):
        part, base = (0, g * 256) if g < 9 else (1, (g - 9) * 256)
        a = qkv_ref[part, :, base:base + 128].astype(f32)
        b = qkv_ref[part, :, base + 128:base + 256].astype(f32)
        lo = (a * cos_t - b * sin_t).astype(bf16).astype(f32)
        hi = (b * cos_t + a * sin_t).astype(bf16).astype(f32)
        if g < 16:
            qs[:, g, 0:128] = lo
            qs[:, g, 128:256] = hi
        else:
            kns[:, 0:128] = lo
            kns[:, 128:256] = hi
    vns[...] = qkv_ref[1, :, 2048:2304].astype(f32)

    row16 = lax.broadcasted_iota(jnp.int32, (16, 256), 0)
    pos = lax.broadcasted_iota(jnp.int32, (16, t_len), 1)

    def body(r, _):
        s = lax.rem(r, SLOTS)
        nxt = r + AHEAD

        @pl.when(nxt < n)
        def _():
            s2 = lax.rem(nxt, SLOTS)

            @pl.when(nxt >= SLOTS)
            def _():
                k_out(nxt - SLOTS, s2).wait()
                v_out(nxt - SLOTS, s2).wait()
            k_in(nxt, s2).start()
            v_in(nxt, s2).start()

        p = len_ref[r]
        base = pl.multiple_of((p // 16) * 16, 16)
        hit = row16 == p - base
        k_in(r, s).wait()
        krow = kb[s, pl.ds(base, 16), :]
        kb[s, pl.ds(base, 16), :] = jnp.where(hit, kns[pl.ds(r, 1), :].astype(bf16), krow)
        q = qs[r].astype(bf16)
        sc = lax.dot_general(q, kb[s], (((1,), (1,)), ((), ())), preferred_element_type=f32) * (256 ** -0.5)
        k_out(r, s).start()
        v_in(r, s).wait()
        vrow = vb[s, pl.ds(base, 16), :]
        vb[s, pl.ds(base, 16), :] = jnp.where(hit, vns[pl.ds(r, 1), :].astype(bf16), vrow)
        sc = jnp.where(pos <= p, sc, -1e30)
        m = jnp.max(sc, axis=1, keepdims=True)
        e = jnp.exp(sc - m)
        den = jnp.sum(e, axis=1, keepdims=True)
        pr = (e / den).astype(bf16)
        v_out(r, s).start()
        osc[r] = jnp.dot(pr, vb[s], preferred_element_type=f32).astype(bf16).astype(f32)
        return 0

    lax.fori_loop(0, n, body, 0)
    for g in range(16):
        o_ref[:, 256 * g:256 * (g + 1)] = osc[:, g, :].astype(bf16)
    for r in range(n - SLOTS, n):
        k_out(r, r % SLOTS).wait()
        v_out(r, r % SLOTS).wait()


def attend(lens, qkv, kc, vc):
    anyspec = pl.BlockSpec(memory_space=pltpu.HBM)
    vspec = pl.BlockSpec(memory_space=pltpu.VMEM)
    dma = pltpu.SemaphoreType.DMA
    n, t_len, hd = kc.shape
    return pl.pallas_call(
        attend_kernel,
        out_shape=[
            jax.ShapeDtypeStruct(kc.shape, bf16),
            jax.ShapeDtypeStruct(vc.shape, bf16),
            jax.ShapeDtypeStruct((n, 4096), bf16),
        ],
        in_specs=[anyspec] * 4,
        out_specs=[anyspec, anyspec, vspec],
        scratch_shapes=[
            pltpu.VMEM((SLOTS, t_len, hd), bf16),
            pltpu.VMEM((SLOTS, t_len, hd), bf16),
            pltpu.SMEM((n,), jnp.int32),
            pltpu.VMEM((2, 16, NQ * QC), bf16),
            pltpu.VMEM((n, 16, hd), f32),
            pltpu.VMEM((n, hd), f32),
            pltpu.VMEM((n, hd), f32),
            pltpu.VMEM((n, 16, hd), f32),
            dma((SLOTS,)), dma((SLOTS,)), dma((SLOTS,)), dma((SLOTS,)), dma((2,)),
        ],
        compiler_params=pltpu.CompilerParams(vmem_limit_bytes=VMEM_LIMIT),
        cost_estimate=pl.CostEstimate(flops=40_000_000_000, bytes_accessed=134_000_000, transcendentals=1_000_000),
        name="attend",
    )(lens, qkv, kc, vc)


UNITS = ((0, 0, 128), (1, 0, 128), (2, 0, 64), (3, 0, 64), (2, 64, 64), (3, 64, 64))
NU = len(UNITS)


def out_proj_kernel(o_ref, x_hbm, d_ref, r_ref, wao_ref, wmo_ref, y_ref,
                    x_ref, db, rb, wao, wmo, ab, ob, zs, zk, zr,
                    xsem, dsem, rsem, waosem, wmosem, a1s, a1r, a2s, a2r, a3s, a3r,
                    o0s, o0r, o1s, o1r, o2s, o2r, o3s, o3r, zss, zrs):
    x = lax.axis_index("x")
    yz = lax.axis_index("yz")
    core = lax.rem(x, 2)
    x_core = x + 1 - 2 * core
    x_chip = lax.rem(x + 2, 4)
    x_diag = x_chip + 1 - 2 * core
    partner = {"x": x_core}
    xpeer = {"x": x_chip}
    ypeer = {"yz": 1 - yz}

    barrier = pltpu.get_barrier_semaphore()
    for dev in (partner, xpeer, ypeer):
        pl.semaphore_signal(barrier, inc=1, device_id=dev, device_id_type=MESH)

    def d_in(i):
        return local_copy(d_ref.at[i], db.at[i], dsem.at[i])

    def r_in(i):
        return local_copy(r_ref.at[i], rb.at[i], rsem.at[i])

    for i in range(NT):
        d_in(i).start()
        r_in(i).start()
    x_in = local_copy(x_hbm, x_ref, xsem)
    x_in.start()
    order = (x, x_core, x_chip, x_diag)

    def wmo_in(n, t):
        rows = pl.multiple_of(order[n] * 2048 + t * TILE, TILE)
        return local_copy(wmo_ref.at[pl.ds(rows, TILE), :], wmo.at[4 * n + t], wmosem.at[4 * n + t])

    wao_in = local_copy(wao_ref, wao, waosem)

    def wmo_start(n):
        for t in range(4):
            wmo_in(n, t).start()

    def a_tile(t):
        for i in (2 * t, 2 * t + 1):
            d_in(i).wait()
            r_in(i).wait()
        gate = (db[2 * t] + rb[2 * t]).astype(bf16).astype(f32)
        up = (db[2 * t + 1] + rb[2 * t + 1]).astype(bf16).astype(f32)
        ab[x, t] = (jax.nn.silu(gate) * up).astype(bf16)

    def unit(owner, u):
        t, r0, n = UNITS[u]
        return ab.at[owner, t, pl.ds(r0, n)]

    def a_part(u):
        return remote_copy(unit(x, u), unit(x, u), a1s.at[u], a1r.at[u], partner)

    def a_chip(u):
        return remote_copy(unit(x, u), unit(x, u), a2s.at[u], a2r.at[u], xpeer)

    def a_fwd(u):
        return remote_copy(unit(x_chip, u), unit(x_chip, u), a3s.at[u], a3r.at[u], partner)

    def a_send(u):
        a_chip(u).start()
        a_part(u).start()

    def o_block(b):
        return ob.at[pl.ds(2 * b, 2)]

    own_half = pl.multiple_of(yz * 2048, 2048)
    peer_half = pl.multiple_of((1 - yz) * 2048, 2048)
    mine = 2 * x + yz
    o_y = remote_copy(o_ref.at[:, pl.ds(peer_half, 2048)], ob.at[mine], o0s, o0r, ypeer)
    o_part = remote_copy(o_block(x), o_block(x), o1s, o1r, partner)
    o_chip = remote_copy(o_block(x), o_block(x), o2s, o2r, xpeer)
    o_fwd = remote_copy(o_block(x_chip), o_block(x_chip), o3s, o3r, partner)

    mc = pl.multiple_of((1 - yz) * 512, 512)
    kc = pl.multiple_of(yz * 512, 512)

    def mlp(n, u, wait=True, first=False):
        t, r0, m = UNITS[u]
        rows = pl.ds(r0, m)
        if wait:
            wmo_in(n, t).wait()
        a = ab[order[n], t, rows]
        w = wmo.at[4 * n + t]
        ps = jnp.dot(a, w[:, pl.ds(mc, 512)], preferred_element_type=f32)
        zs[rows] = ps if first else zs[rows] + ps
        pk = jnp.dot(a, w[:, pl.ds(kc, 512)], preferred_element_type=f32)
        zk[rows] = pk if first else zk[rows] + pk

    def mlp_tile(n, t, first=False):
        wmo_in(n, t).wait()
        a = ab[order[n], t]
        w = wmo.at[4 * n + t]
        ps = jnp.dot(a, w[:, pl.ds(mc, 512)], preferred_element_type=f32)
        zs[...] = ps if first else zs[...] + ps
        pk = jnp.dot(a, w[:, pl.ds(kc, 512)], preferred_element_type=f32)
        zk[...] = pk if first else zk[...] + pk

    a_tile(0)
    ob[mine] = o_ref[:, pl.ds(own_half, 2048)]
    pl.semaphore_wait(barrier, 3)
    o_y.start()
    a_send(0)
    a_tile(1)
    wmo_start(0)
    a_tile(2)
    a_send(1)
    a_tile(3)
    wmo_start(1)
    mlp_tile(0, 0, first=True)
    mlp_tile(0, 1)
    o_y.wait()
    o_chip.start()
    o_part.start()
    for u in range(2, NU):
        a_send(u)
    wmo_start(2)
    wao_in.start()
    mlp_tile(0, 2)
    mlp_tile(0, 3)
    a_part(0).wait()
    mlp_tile(1, 0)
    a_part(1).wait()
    mlp_tile(1, 1)
    a_chip(0).wait()
    a_fwd(0).start()
    wmo_start(3)
    mlp(2, 0)
    for u in range(2, NU):
        a_part(u).wait()
    mlp_tile(1, 2)
    mlp_tile(1, 3)
    a_chip(1).wait()
    a_fwd(1).start()
    mlp(2, 1)
    a_fwd(0).wait()
    mlp(3, 0)
    o_part.wait()
    o_chip.wait()
    o_fwd.start()
    a_fwd(1).wait()
    mlp(3, 1)
    wao_in.wait()
    a_chip(2).wait()
    a_fwd(2).start()
    mlp(2, 2)
    o_fwd.wait()
    attn = ob[...].reshape(128, 2048)
    zs[...] += jnp.dot(attn, wao[:, pl.ds(mc, 512)], preferred_element_type=f32)
    zk[...] += jnp.dot(attn, wao[:, pl.ds(kc, 512)], preferred_element_type=f32)

    def z_y(c):
        rows = pl.ds(64 * c, 64)
        return remote_copy(zs.at[rows], zr.at[rows], zss.at[c], zrs.at[c], ypeer)

    a_chip(3).wait()
    a_fwd(3).start()
    mlp(2, 3)
    a_fwd(2).wait()
    mlp(3, 2)
    a_fwd(3).wait()
    mlp(3, 3)
    z_y(0).start()
    a_chip(4).wait()
    a_fwd(4).start()
    mlp(2, 4, wait=False)
    a_chip(5).wait()
    a_fwd(5).start()
    mlp(2, 5, wait=False)
    a_fwd(4).wait()
    mlp(3, 4, wait=False)
    a_fwd(5).wait()
    mlp(3, 5, wait=False)
    z_y(1).start()
    x_in.wait()
    for c in range(2):
        z_y(c).wait()
        rows = pl.ds(64 * c, 64)
        y_ref[rows, :] = (x_ref[rows, :].astype(f32) + (zk[rows, :] + zr[rows, :])).astype(bf16)


def out_proj(o, x_loc, d, r, wao, wmo):
    anyspec = pl.BlockSpec(memory_space=pltpu.HBM)
    vspec = pl.BlockSpec(memory_space=pltpu.VMEM)
    dma = pltpu.SemaphoreType.DMA
    return pl.pallas_call(
        out_proj_kernel,
        out_shape=jax.ShapeDtypeStruct((128, 512), bf16),
        in_specs=[vspec, anyspec, anyspec, anyspec, anyspec, anyspec],
        out_specs=vspec,
        scratch_shapes=[
            pltpu.VMEM((128, 512), bf16),
            pltpu.VMEM((NT, 128, TILE), f32),
            pltpu.VMEM((NT, 128, TILE), f32),
            pltpu.VMEM((2048, 1024), bf16),
            pltpu.VMEM((16, TILE, 1024), bf16),
            pltpu.VMEM((4, 4, 128, TILE), bf16),
            pltpu.VMEM((8, 16, 2048), bf16),
            pltpu.VMEM((128, 512), f32),
            pltpu.VMEM((128, 512), f32),
            pltpu.VMEM((128, 512), f32),
            dma, dma((NT,)), dma((NT,)), dma, dma((16,)),
            dma((NU,)), dma((NU,)), dma((NU,)), dma((NU,)), dma((NU,)), dma((NU,)),
            dma, dma, dma, dma, dma, dma, dma, dma, dma((2,)), dma((2,)),
        ],
        compiler_params=pltpu.CompilerParams(
            collective_id=1, has_side_effects=True, vmem_limit_bytes=48 * 2 ** 20),
        cost_estimate=pl.CostEstimate(flops=3_000_000_000, bytes_accessed=26_000_000, transcendentals=0),
        name="out_proj",
    )(o, x_loc, d, r, wao, wmo)


def solution(mesh):
    both_axes = ("x", "yz")
    row_spec = P("dp", both_axes)
    in_w_spec = P("x", "yz")
    out_w_spec = P("yz", "x")
    cache_spec = P(("dp", "x", "yz"), None, None)
    len_spec = P(("dp", "x", "yz"))
    swap = [(0, 2), (2, 0), (1, 3), (3, 1)]

    def local_layer(x_loc, gain_loc, wqkv_loc, wgate_loc, wup_loc, wao_loc, wmo_loc, kc_loc, vc_loc, len_loc):
        qkv, s, d = in_proj(x_loc, gain_loc, wqkv_loc, wgate_loc, wup_loc)
        r = lax.ppermute(s, "x", swap)
        k_all, v_all, o = attend(len_loc, qkv, kc_loc, vc_loc)
        y_loc = out_proj(o, x_loc, d, r, wao_loc, wmo_loc)
        return y_loc, k_all, v_all

    in_specs = (row_spec, P(both_axes), in_w_spec, in_w_spec, in_w_spec, out_w_spec, out_w_spec, cache_spec, cache_spec, len_spec)
    out_specs = (row_spec, cache_spec, cache_spec)
    return jax.shard_map(local_layer, mesh=mesh, in_specs=in_specs, out_specs=out_specs, check_vma=False)
```

```python
import functools

import jax
import jax.numpy as jnp
from jax import lax
from jax.experimental import pallas as pl
from jax.experimental.pallas import tpu as pltpu
from jax.sharding import PartitionSpec as P

MESH = pl.DeviceIdType.MESH
VMEM_LIMIT = 67043328
OUT_ROOM = 8000000
TILE = 512
SA = 5
SPLIT = 10
NT = 8
QC = 768
NQ = 3
W_FIRST = 8
W_AHEAD = 12

f32 = jnp.float32
bf16 = jnp.bfloat16


def local_copy(src, dst, sem):
    return pltpu.make_async_copy(src, dst, sem)


def remote_copy(src, dst, ssem, rsem, dev):
    return pltpu.make_async_remote_copy(src, dst, ssem, rsem, device_id=dev, device_id_type=MESH)


def in_proj_kernel(x_hbm, g_hbm, wq_ref, wg_ref, wu_ref, qkv_ref, sa_ref, sb_ref, r0_ref, d_ref,
                   wqv, wv, x_ref, g_ref, xr, gr, qout, st, stx, h, qp, qr, qxs, qxr, qf, qyr, sbuf, rbuf, obuf,
                   wqsem, wsem, xs_sem, xr_sem, gs_sem, gr_sem, sts_sem, str_sem,
                   qds_sem, qdr_sem, qxs_sem, qxr_sem, qys_sem, qyr_sem, ds_sem, dr_sem, out_sem, xin_sem, gin_sem, qo_sem, es_sem, er_sem):
    d_model = 4096
    x = lax.axis_index("x")
    yz = lax.axis_index("yz")
    core = lax.rem(x, 2)
    x_core = x + 1 - 2 * core
    x_chip = lax.rem(x + 2, 4)
    x_diag = x_chip + 1 - 2 * core
    me = 2 * x + yz
    partner = {"x": x_core}
    xpeer = {"x": x_chip}
    ypeer = {"yz": 1 - yz}

    barrier = pltpu.get_barrier_semaphore()
    others = []
    for dx in range(4):
        for dy in range(2):
            if dx or dy:
                others.append((lax.rem(x + dx, 4), lax.rem(yz + dy, 2)))
    for ox, oy in others:
        pl.semaphore_signal(barrier, inc=1, device_id={"x": ox, "yz": oy}, device_id_type=MESH)
    x_in = local_copy(x_hbm, x_ref, xin_sem)
    g_in = local_copy(g_hbm, g_ref, gin_sem)
    x_in.start()
    g_in.start()

    def wq_copy(j):
        return local_copy(wq_ref.at[:, pl.ds(QC * j, QC)], wqv.at[j], wqsem.at[j])

    quarters = (x_diag, x_chip, x_core, x)

    def w_start(slot):
        phase = slot // NT
        q = quarters[0]
        for n in range(1, 4):
            q = jnp.where(phase == n, quarters[n], q)
        cols = pl.multiple_of(q * 2048 + (slot % NT) // 2 * TILE, TILE)

        def start(w_hbm):
            local_copy(w_hbm.at[:, pl.ds(cols, TILE)], wv.at[slot], wsem.at[slot]).start()

        if isinstance(slot, int):
            start(wg_ref if slot % 2 == 0 else wu_ref)
        else:
            pl.when(slot % 2 == 0)(lambda: start(wg_ref))
            pl.when(slot % 2 == 1)(lambda: start(wu_ref))

    def w_wait(slot):
        local_copy(wg_ref.at[:, pl.ds(0, TILE)], wv.at[slot], wsem.at[slot]).wait()

    x_in.wait()
    for j in range(NQ):
        wq_copy(j).start()
    for slot in range(W_FIRST):
        w_start(slot)
    g_in.wait()
    xf = x_ref[...].astype(f32)
    s1 = jnp.sum(xf, axis=1, keepdims=True)
    s2 = jnp.sum(xf * xf, axis=1, keepdims=True)
    lane = lax.broadcasted_iota(jnp.int32, (128, 128), 1)
    stat = jnp.where(lane == 0, s1, s2).T
    st[me] = stat[0:8]

    pl.semaphore_wait(barrier, 7)

    x_send = remote_copy(x_ref, xr, xs_sem, xr_sem, ypeer)
    g_send = remote_copy(g_ref, gr, gs_sem, gr_sem, ypeer)
    for n, (ox, oy) in enumerate(others):
        remote_copy(st.at[me], stx.at[me], sts_sem.at[n], str_sem.at[me], {"x": ox, "yz": oy}).start()
    g_send.start()
    x_send.start()
    stx[me] = st[me]
    for n, (ox, oy) in enumerate(others):
        src = 2 * ox + oy
        remote_copy(st.at[me], stx.at[src], sts_sem.at[n], str_sem.at[src], {"x": ox, "yz": oy}).wait()
    tot = jnp.sum(stx[...], axis=0)
    tot = jnp.concatenate([tot, jnp.zeros((120, 128), f32)], axis=0).T
    mean = tot[:, 0:1] / d_model
    var = tot[:, 1:2] / d_model - mean * mean
    rstd = lax.rsqrt(var + 1e-6)
    own_cols = pl.multiple_of(yz * 512, 512)
    peer_cols = pl.multiple_of((1 - yz) * 512, 512)
    h[:, pl.ds(own_cols, 512)] = ((xf - mean) * rstd * g_ref[...].astype(f32).reshape(1, 512)).astype(bf16)
    x_send.wait()
    g_send.wait()
    h[:, pl.ds(peer_cols, 512)] = ((xr[...].astype(f32) - mean) * rstd * gr[...].astype(f32).reshape(1, 512)).astype(bf16)

    for slot in range(W_FIRST, W_AHEAD):
        w_start(slot)

    def q_compute(j):
        wq_copy(j).wait()
        part = jnp.dot(h[...], wqv[j], preferred_element_type=f32)
        qp[j] = part.reshape(4, 32, QC)

    def q_pair(j, k):
        block = (x_diag, x_core)[k]
        return remote_copy(qp.at[j, block], qr.at[j, k], qds_sem.at[j, k], qdr_sem.at[j, k], partner)

    def q_pair_start(j):
        q_pair(j, 0).start()
        q_pair(j, 1).start()

    def q_chip(j):
        return remote_copy(qxs.at[j], qxr.at[j], qxs_sem.at[j], qxr_sem.at[j], xpeer)

    def q_sum(j):
        q_pair(j, 0).wait()
        qxs[j] = qp[j, x_chip] + qr[j, 0]

    def tile(slot):
        w_wait(slot)
        if isinstance(slot, int):
            if slot + W_AHEAD < 4 * NT:
                w_start(slot + W_AHEAD)
        else:
            @pl.when(slot + W_AHEAD < 4 * NT)
            def _():
                w_start(slot + W_AHEAD)
        return jnp.dot(h[...], wv[slot], preferred_element_type=f32)

    def d_copy(i):
        return remote_copy(sbuf.at[i], rbuf.at[i], ds_sem.at[i], dr_sem.at[i], partner)

    def s_out(i):
        dst = sa_ref.at[i - 1] if i <= SA else sb_ref.at[i - 1 - SA]
        return local_copy(obuf.at[i], dst, out_sem.at[i])

    def d_out(i):
        return local_copy(obuf.at[NT + i], d_ref.at[i], out_sem.at[NT + i])

    early = remote_copy(obuf.at[0], r0_ref.at[0], es_sem, er_sem, xpeer)

    q_compute(0)
    q_compute(1)
    q_pair_start(0)
    q_compute(2)
    q_pair_start(1)

    after = {
        0: lambda: q_pair_start(2),
        1: lambda: q_sum(0),
        2: lambda: (q_chip(0).start(), q_sum(1)),
        3: lambda: (q_chip(1).start(), q_sum(2)),
        4: lambda: q_chip(2).start(),
    }
    for i in range(NT):
        sbuf[i] = tile(i)
        if i:
            d_copy(i - 1).start()
        if i in after:
            after[i]()

    for i in range(NT):
        part = tile(NT + i)
        if i == 0:
            d_copy(NT - 1).start()
        d_copy(i).wait()
        obuf[i] = part + rbuf[i]
        if i == 1:
            early.start()
        elif i:
            s_out(i - 1).start()

    own_rows = pl.multiple_of(yz * 16, 16)
    peer_rows = pl.multiple_of((1 - yz) * 16, 16)

    def q_y(j):
        return remote_copy(qf.at[j, pl.ds(peer_rows, 16)], qyr.at[j], qys_sem.at[j], qyr_sem.at[j], ypeer)

    def q_final(j):
        q_pair(j, 1).wait()
        q_chip(j).wait()
        qf[j] = (qp[j, x] + qr[j, 1] + qxr[j]).astype(bf16)
        qout[yz, :, pl.ds(QC * j, QC)] = qf[j, pl.ds(own_rows, 16)]

    def send_tiles(lo, hi):
        def body(i, _):
            sbuf[NT + i] = tile(2 * NT + i)

            @pl.when(i == 0)
            def _():
                s_out(NT - 1).start()

            @pl.when(i > 0)
            def _():
                d_copy(NT + i - 1).start()
            return 0

        lax.fori_loop(lo, hi, body, 0)

    def keep_tiles(lo, hi):
        def body(i, _):
            part = tile(3 * NT + i)

            @pl.when(i == 0)
            def _():
                d_copy(2 * NT - 1).start()
            d_copy(NT + i).wait()
            obuf[NT + i] = part + rbuf[NT + i]

            @pl.when(i > 0)
            def _():
                d_out(i - 1).start()
            return 0

        lax.fori_loop(lo, hi, body, 0)

    send_tiles(0, 3)
    q_final(0)
    send_tiles(3, 4)
    q_y(0).start()
    send_tiles(4, 8)
    keep_tiles(0, 2)
    q_final(1)
    keep_tiles(2, 3)
    q_y(1).start()
    keep_tiles(3, 7)
    q_final(2)
    keep_tiles(7, 8)
    q_y(2).start()
    d_out(NT - 1).start()
    for j in range(NQ):
        q_y(j).wait()
        qout[1 - yz, :, pl.ds(QC * j, QC)] = qyr[j]
    q_out = local_copy(qout, qkv_ref, qo_sem)
    q_out.start()
    for i in range(NT):
        if i:
            s_out(i).wait()
        d_out(i).wait()
    q_out.wait()
    early.wait()


def in_proj(x_loc, gain, wq, wg, wu):
    anyspec = pl.BlockSpec(memory_space=pltpu.HBM)
    dma = pltpu.SemaphoreType.DMA
    return pl.pallas_call(
        in_proj_kernel,
        out_shape=[
            jax.ShapeDtypeStruct((2, 16, NQ * QC), bf16),
            jax.ShapeDtypeStruct((SA, 128, TILE), f32),
            jax.ShapeDtypeStruct((NT - 1 - SA, 128, TILE), f32),
            jax.ShapeDtypeStruct((1, 128, TILE), f32),
            jax.ShapeDtypeStruct((NT, 128, TILE), f32),
        ],
        in_specs=[anyspec] * 5,
        out_specs=[anyspec] * 5,
        scratch_shapes=[
            pltpu.VMEM((NQ, 1024, QC), bf16),
            pltpu.VMEM((4 * NT, 1024, TILE), bf16),
            pltpu.VMEM((128, 512), bf16),
            pltpu.VMEM((512,), bf16),
            pltpu.VMEM((128, 512), bf16),
            pltpu.VMEM((512,), bf16),
            pltpu.VMEM((2, 16, NQ * QC), bf16),
            pltpu.VMEM((8, 8, 128), f32),
            pltpu.VMEM((8, 8, 128), f32),
            pltpu.VMEM((128, 1024), bf16),
            pltpu.VMEM((NQ, 4, 32, QC), f32),
            pltpu.VMEM((NQ, 2, 32, QC), f32),
            pltpu.VMEM((NQ, 32, QC), f32),
            pltpu.VMEM((NQ, 32, QC), f32),
            pltpu.VMEM((NQ, 32, QC), bf16),
            pltpu.VMEM((NQ, 16, QC), bf16),
            pltpu.VMEM((2 * NT, 128, TILE), f32),
            pltpu.VMEM((2 * NT, 128, TILE), f32),
            pltpu.VMEM((2 * NT, 128, TILE), f32),
            dma((NQ,)), dma((4 * NT,)), dma, dma, dma, dma, dma((7,)), dma((8,)),
            dma((NQ, 2)), dma((NQ, 2)), dma((NQ,)), dma((NQ,)), dma((NQ,)), dma((NQ,)),
            dma((2 * NT,)), dma((2 * NT,)), dma((2 * NT,)), dma, dma, dma, dma, dma,
        ],
        compiler_params=pltpu.CompilerParams(
            collective_id=0, has_side_effects=True, vmem_limit_bytes=VMEM_LIMIT),
        cost_estimate=pl.CostEstimate(flops=5_000_000_000, bytes_accessed=45_000_000, transcendentals=0),
        name="in_proj",
    )(x_loc, gain, wq, wg, wu)


SLOTS = 6


def attend_kernel(lo, hi, len_hbm, qkv_hbm, k_ref, v_ref, *refs):
    if lo:
        refs = refs[2:]
    (ko_ref, vo_ref, o_hbm, o_ref, kb, vb, len_ref, qkv_ref, qs, kns, vns, osc,
     ksem, vsem, kosem, vosem, isem, osem) = refs
    t_len = k_ref.shape[1]

    def k_in(r, s):
        return local_copy(k_ref.at[r], kb.at[s], ksem.at[s])

    def v_in(r, s):
        return local_copy(v_ref.at[r], vb.at[s], vsem.at[s])

    def k_out(r, s):
        return local_copy(kb.at[s], ko_ref.at[r], kosem.at[s])

    def v_out(r, s):
        return local_copy(vb.at[s], vo_ref.at[r], vosem.at[s])

    AHEAD = 4
    len_in = local_copy(len_hbm, len_ref, isem.at[0])
    qkv_in = local_copy(qkv_hbm, qkv_ref, isem.at[1])
    len_in.start()
    qkv_in.start()
    for r in range(lo, lo + 2):
        k_in(r, r % SLOTS).start()
        v_in(r, r % SLOTS).start()
    len_in.wait()
    qkv_in.wait()
    for r in range(lo + 2, lo + AHEAD):
        k_in(r, r % SLOTS).start()
        v_in(r, r % SLOTS).start()
    row = lax.broadcasted_iota(jnp.int32, (16, 128), 0)
    lens = jnp.zeros((16, 128), jnp.int32)
    for r in range(16):
        lens = jnp.where(row == r, len_ref[r], lens)
    half = lax.broadcasted_iota(jnp.int32, (16, 128), 1).astype(f32)
    angles = lens.astype(f32) * 10000.0 ** (-half / 128)
    cos_t = jnp.cos(angles)
    sin_t = jnp.sin(angles)
    for g in range(17):
        part, base = (0, g * 256) if g < 9 else (1, (g - 9) * 256)
        a = qkv_ref[part, :, base:base + 128].astype(f32)
        b = qkv_ref[part, :, base + 128:base + 256].astype(f32)
        lower = (a * cos_t - b * sin_t).astype(bf16).astype(f32)
        upper = (b * cos_t + a * sin_t).astype(bf16).astype(f32)
        if g < 16:
            qs[:, g, 0:128] = lower
            qs[:, g, 128:256] = upper
        else:
            kns[:, 0:128] = lower
            kns[:, 128:256] = upper
    vns[...] = qkv_ref[1, :, 2048:2304].astype(f32)

    row16 = lax.broadcasted_iota(jnp.int32, (16, 256), 0)
    pos = lax.broadcasted_iota(jnp.int32, (16, t_len), 1)

    def body(r, _):
        s = lax.rem(r, SLOTS)
        nxt = r + AHEAD

        @pl.when(nxt < hi)
        def _():
            s2 = lax.rem(nxt, SLOTS)

            @pl.when(nxt - SLOTS >= lo)
            def _():
                k_out(nxt - SLOTS, s2).wait()
                v_out(nxt - SLOTS, s2).wait()
            k_in(nxt, s2).start()
            v_in(nxt, s2).start()

        p = len_ref[r]
        base = pl.multiple_of((p // 16) * 16, 16)
        hit = row16 == p - base
        k_in(r, s).wait()
        krow = kb[s, pl.ds(base, 16), :]
        kb[s, pl.ds(base, 16), :] = jnp.where(hit, kns[pl.ds(r, 1), :].astype(bf16), krow)
        q = qs[r].astype(bf16)
        sc = lax.dot_general(q, kb[s], (((1,), (1,)), ((), ())), preferred_element_type=f32) * (256 ** -0.5)
        k_out(r, s).start()
        v_in(r, s).wait()
        vrow = vb[s, pl.ds(base, 16), :]
        vb[s, pl.ds(base, 16), :] = jnp.where(hit, vns[pl.ds(r, 1), :].astype(bf16), vrow)
        sc = jnp.where(pos <= p, sc, -1e30)
        m = jnp.max(sc, axis=1, keepdims=True)
        e = jnp.exp(sc - m)
        den = jnp.sum(e, axis=1, keepdims=True)
        pr = (e / den).astype(bf16)
        v_out(r, s).start()
        osc[r] = jnp.dot(pr, vb[s], preferred_element_type=f32).astype(bf16).astype(f32)
        return 0

    lax.fori_loop(lo, hi, body, 0)
    for g in range(16):
        o_ref[:, 256 * g:256 * (g + 1)] = osc[:, g, :].astype(bf16)
    o_out = local_copy(o_ref, o_hbm, osem)
    o_out.start()
    for r in range(max(lo, hi - SLOTS), hi):
        k_out(r, r % SLOTS).wait()
        v_out(r, r % SLOTS).wait()
    o_out.wait()


def attend(lo, hi, lens, qkv, kc, vc, *prev):
    anyspec = pl.BlockSpec(memory_space=pltpu.HBM)
    dma = pltpu.SemaphoreType.DMA
    n, t_len, hd = kc.shape
    return pl.pallas_call(
        functools.partial(attend_kernel, lo, hi),
        out_shape=[
            jax.ShapeDtypeStruct(kc.shape, bf16),
            jax.ShapeDtypeStruct(vc.shape, bf16),
            jax.ShapeDtypeStruct((n, 4096), bf16),
        ],
        in_specs=[anyspec] * (4 + len(prev)),
        out_specs=[anyspec] * 3,
        input_output_aliases={4: 0, 5: 1} if prev else {},
        scratch_shapes=[
            pltpu.VMEM((n, 4096), bf16),
            pltpu.VMEM((SLOTS, t_len, hd), bf16),
            pltpu.VMEM((SLOTS, t_len, hd), bf16),
            pltpu.SMEM((n,), jnp.int32),
            pltpu.VMEM((2, 16, NQ * QC), bf16),
            pltpu.VMEM((n, 16, hd), f32),
            pltpu.VMEM((n, hd), f32),
            pltpu.VMEM((n, hd), f32),
            pltpu.VMEM((n, 16, hd), f32),
            dma((SLOTS,)), dma((SLOTS,)), dma((SLOTS,)), dma((SLOTS,)), dma((2,)), dma,
        ],
        compiler_params=pltpu.CompilerParams(vmem_limit_bytes=VMEM_LIMIT),
        cost_estimate=pl.CostEstimate(flops=2_500_000_000 * (hi - lo), bytes_accessed=8_400_000 * (hi - lo), transcendentals=1_000_000),
        name=f"attend{lo}",
    )(lens, qkv, kc, vc, *prev)


NA = 3


def act_kernel(d_ref, r0_ref, r_ref, a_hbm, db, rb, a_ref, dsem, rsem, asem):
    def d_in(i):
        return local_copy(d_ref.at[i], db.at[i], dsem.at[i])

    def r_in(i):
        return local_copy(r_ref.at[i - 1] if i else r0_ref.at[0], rb.at[i], rsem.at[i])

    def a_out(t):
        return local_copy(a_ref.at[t], a_hbm.at[t], asem.at[t])

    for i in range(2 * NA):
        d_in(i).start()
        r_in(i).start()

    def total(i):
        d_in(i).wait()
        r_in(i).wait()
        return (db[i] + rb[i]).astype(bf16).astype(f32)

    for t in range(NA):
        a_ref[t] = (jax.nn.silu(total(2 * t)) * total(2 * t + 1)).astype(bf16)
        if t:
            a_out(t - 1).start()
    a_out(NA - 1).start()
    for t in range(NA):
        a_out(t).wait()


def act(d, r0, r):
    anyspec = pl.BlockSpec(memory_space=pltpu.HBM)
    dma = pltpu.SemaphoreType.DMA
    return pl.pallas_call(
        act_kernel,
        out_shape=jax.ShapeDtypeStruct((NA, 128, TILE), bf16),
        in_specs=[anyspec] * 3,
        out_specs=anyspec,
        scratch_shapes=[
            pltpu.VMEM((2 * NA, 128, TILE), f32),
            pltpu.VMEM((2 * NA, 128, TILE), f32),
            pltpu.VMEM((NA, 128, TILE), bf16),
            dma((2 * NA,)), dma((2 * NA,)), dma((NA,)),
        ],
        compiler_params=pltpu.CompilerParams(vmem_limit_bytes=VMEM_LIMIT),
        cost_estimate=pl.CostEstimate(flops=5_000_000, bytes_accessed=4_000_000, transcendentals=200_000),
        name="act",
    )(d, r0, r)


def out_proj_kernel(o1_hbm, o2_hbm, x_hbm, d_ref, r_ref, ao_ref, ax_ref, wao_ref, wmo_ref, y_ref,
                    o1_ref, o2_ref, o_ref, x_ref, db, rb, wao, wmo, ab, ob, zs, zk, zr,
                    osem, xsem, dsem, rsem, asem, waosem, wmosem, pss, psr, fss, fsr, e_s, e_r,
                    o0s, o0r, o1s, o1r, o2s, o2r, o3s, o3r, zss, zrs):
    x = lax.axis_index("x")
    yz = lax.axis_index("yz")
    core = lax.rem(x, 2)
    x_core = x + 1 - 2 * core
    x_chip = lax.rem(x + 2, 4)
    x_diag = x_chip + 1 - 2 * core
    partner = {"x": x_core}
    xpeer = {"x": x_chip}
    ypeer = {"yz": 1 - yz}

    barrier = pltpu.get_barrier_semaphore()
    for dev in (partner, xpeer, ypeer):
        pl.semaphore_signal(barrier, inc=1, device_id=dev, device_id_type=MESH)

    o_in = [local_copy(o1_hbm, o1_ref, osem.at[0]), local_copy(o2_hbm, o2_ref, osem.at[1])]
    for c in o_in:
        c.start()
    first = pl.ds(0, NA)
    own_in = local_copy(ao_ref, ab.at[x, first], asem.at[0])
    chip_in = local_copy(ax_ref, ab.at[x_chip, first], asem.at[1])
    own_in.start()
    chip_in.start()
    loads = [local_copy(d_ref.at[pl.ds(2 * NA, 2)], db, dsem), local_copy(r_ref, rb, rsem)]
    for c in loads:
        c.start()
    for c in o_in:
        c.wait()
    x_in = local_copy(x_hbm, x_ref, xsem)
    x_in.start()

    order = (x, x_chip, x_core, x_diag)

    def wmo_in(n, t):
        rows = pl.multiple_of(order[n] * 2048 + t * TILE, TILE)
        return local_copy(wmo_ref.at[pl.ds(rows, TILE), :], wmo.at[4 * n + t], wmosem.at[4 * n + t])

    wao_in = local_copy(wao_ref, wao, waosem)

    def wmo_start(n):
        for t in range(4):
            wmo_in(n, t).start()

    wmo_start(0)
    row = lax.broadcasted_iota(jnp.int32, (16, 4096), 0)
    o_ref[...] = jnp.where(row < SPLIT, o1_ref[...].astype(f32), o2_ref[...].astype(f32)).astype(bf16)
    own_half = pl.multiple_of(yz * 2048, 2048)
    peer_half = pl.multiple_of((1 - yz) * 2048, 2048)
    mine = 2 * x + yz
    theirs = 2 * x + 1 - yz
    ob[mine] = o_ref[:, pl.ds(own_half, 2048)]

    for c in loads:
        c.wait()
    gate = (db[0] + rb[0]).astype(bf16).astype(f32)
    up = (db[1] + rb[1]).astype(bf16).astype(f32)
    ab[x, NA] = (jax.nn.silu(gate) * up).astype(bf16)
    pl.semaphore_wait(barrier, 3)

    o_y = remote_copy(o_ref.at[:, pl.ds(peer_half, 2048)], ob.at[mine], o0s, o0r, ypeer)

    def o_hop(k, ss, rs, dev, owner):
        block = ob.at[2 * owner + (yz if k == 0 else 1 - yz)]
        return remote_copy(block, block, ss.at[k], rs.at[k], dev)

    o_part = [o_hop(k, o1s, o1r, partner, x) for k in range(2)]
    o_chip = [o_hop(k, o2s, o2r, xpeer, x) for k in range(2)]
    o_fwd = [o_hop(k, o3s, o3r, partner, x_chip) for k in range(2)]

    def a_hop(owner, tiles, ss, rs, k, dev):
        block = ab.at[owner, tiles]
        return remote_copy(block, block, ss.at[k], rs.at[k], dev)

    last = pl.ds(NA, 1)
    a_part = [a_hop(x, first, pss, psr, 0, partner), a_hop(x, last, pss, psr, 1, partner)]
    a_fwd = [a_hop(x_chip, first, fss, fsr, 0, partner), a_hop(x_chip, last, fss, fsr, 1, partner)]
    a_chip = remote_copy(ab.at[x, last], ab.at[x, last], e_s, e_r, xpeer)

    o_y.start()
    o_chip[0].start()
    a_chip.start()
    o_part[0].start()
    a_part[1].start()
    own_in.wait()
    a_part[0].start()
    chip_in.wait()
    a_fwd[0].start()
    wmo_start(1)
    wmo_start(2)

    mc = pl.multiple_of((1 - yz) * 512, 512)
    kc = pl.multiple_of(yz * 512, 512)

    def mlp(n, t, init=False):
        wmo_in(n, t).wait()
        a = ab[order[n], t]
        w = wmo.at[4 * n + t]
        ps = jnp.dot(a, w[:, pl.ds(mc, 512)], preferred_element_type=f32)
        zs[...] = ps if init else zs[...] + ps
        pk = jnp.dot(a, w[:, pl.ds(kc, 512)], preferred_element_type=f32)
        zk[...] = pk if init else zk[...] + pk

    mlp(0, 0, init=True)
    mlp(0, 1)
    mlp(0, 2)
    mlp(0, 3)
    o_y.wait()
    o_chip[1].start()
    o_part[1].start()
    wmo_start(3)
    wao_in.start()
    mlp(1, 0)
    mlp(1, 1)
    o_chip[0].wait()
    o_fwd[0].start()
    mlp(1, 2)
    a_part[0].wait()
    mlp(2, 0)
    mlp(2, 1)
    a_chip.wait()
    a_fwd[1].start()
    mlp(1, 3)
    mlp(2, 2)
    a_part[1].wait()
    mlp(2, 3)
    a_fwd[0].wait()
    mlp(3, 0)
    mlp(3, 1)
    mlp(3, 2)
    a_fwd[1].wait()
    mlp(3, 3)

    chip = x // 2
    own_rows = pl.multiple_of(64 * chip, 64)
    chip_rows = pl.multiple_of(32 * x_chip, 32)
    diag_rows = pl.multiple_of(32 * x_diag, 32)

    def z_y(c, base, m):
        rows = pl.ds(base, m)
        return remote_copy(zs.at[rows], zr.at[rows], zss.at[c], zrs.at[c], ypeer)

    def attn_rows(base, m):
        rows = pl.ds(base, m)
        attn = ob[pl.ds(base // 16, m // 16)].reshape(m, 2048)
        zs[rows] += jnp.dot(attn, wao[:, pl.ds(mc, 512)], preferred_element_type=f32)
        zk[rows] += jnp.dot(attn, wao[:, pl.ds(kc, 512)], preferred_element_type=f32)

    blocks = ((own_rows, 64), (chip_rows, 32), (diag_rows, 32))
    wao_in.wait()
    for k in range(2):
        o_part[k].wait()
    attn_rows(*blocks[0])
    z_y(0, *blocks[0]).start()
    o_chip[1].wait()
    o_fwd[1].start()
    attn_rows(*blocks[1])
    z_y(1, *blocks[1]).start()
    for k in range(2):
        o_fwd[k].wait()
    attn_rows(*blocks[2])
    z_y(2, *blocks[2]).start()
    x_in.wait()
    for c, (base, m) in enumerate(blocks):
        z_y(c, base, m).wait()
        rows = pl.ds(base, m)
        y_ref[rows, :] = (x_ref[rows, :].astype(f32) + (zk[rows, :] + zr[rows, :])).astype(bf16)


def out_proj(o1, o2, x_loc, d, r, a_own, a_chip, wao, wmo):
    anyspec = pl.BlockSpec(memory_space=pltpu.HBM)
    vspec = pl.BlockSpec(memory_space=pltpu.VMEM)
    dma = pltpu.SemaphoreType.DMA
    two = dma((2,))
    return pl.pallas_call(
        out_proj_kernel,
        out_shape=jax.ShapeDtypeStruct((128, 512), bf16),
        in_specs=[anyspec] * 9,
        out_specs=vspec,
        scratch_shapes=[
            pltpu.VMEM((16, 4096), bf16),
            pltpu.VMEM((16, 4096), bf16),
            pltpu.VMEM((16, 4096), bf16),
            pltpu.VMEM((128, 512), bf16),
            pltpu.VMEM((2, 128, TILE), f32),
            pltpu.VMEM((2, 128, TILE), f32),
            pltpu.VMEM((2048, 1024), bf16),
            pltpu.VMEM((16, TILE, 1024), bf16),
            pltpu.VMEM((4, 4, 128, TILE), bf16),
            pltpu.VMEM((8, 16, 2048), bf16),
            pltpu.VMEM((128, 512), f32),
            pltpu.VMEM((128, 512), f32),
            pltpu.VMEM((128, 512), f32),
            two, dma, dma, dma, two, dma, dma((16,)),
            two, two, two, two, dma, dma,
            dma, dma, two, two, two, two, two, two, dma((3,)), dma((3,)),
        ],
        compiler_params=pltpu.CompilerParams(
            collective_id=1, has_side_effects=True, vmem_limit_bytes=VMEM_LIMIT - OUT_ROOM),
        cost_estimate=pl.CostEstimate(flops=3_000_000_000, bytes_accessed=26_000_000, transcendentals=0),
        name="out_proj",
    )(o1, o2, x_loc, d, r, a_own, a_chip, wao, wmo)


def solution(mesh):
    both_axes = ("x", "yz")
    row_spec = P("dp", both_axes)
    in_w_spec = P("x", "yz")
    out_w_spec = P("yz", "x")
    cache_spec = P(("dp", "x", "yz"), None, None)
    len_spec = P(("dp", "x", "yz"))
    swap = [(0, 2), (2, 0), (1, 3), (3, 1)]

    def local_layer(x_loc, gain_loc, wqkv_loc, wgate_loc, wup_loc, wao_loc, wmo_loc, kc_loc, vc_loc, len_loc):
        qkv, sa, sb, r0, d = in_proj(x_loc, gain_loc, wqkv_loc, wgate_loc, wup_loc)
        ra = lax.ppermute(sa, "x", swap)
        k_all, v_all, o1 = attend(0, SPLIT, len_loc, qkv, kc_loc, vc_loc)
        sb, o1 = lax.optimization_barrier((sb, o1))
        rb = lax.ppermute(sb, "x", swap)
        a_own = act(d, r0, ra)
        a_chip = lax.ppermute(a_own, "x", swap)
        k_all, v_all, o2 = attend(SPLIT, 16, len_loc, qkv, kc_loc, vc_loc, k_all, v_all)
        y_loc = out_proj(o1, o2, x_loc, d, rb, a_own, a_chip, wao_loc, wmo_loc)
        return y_loc, k_all, v_all

    in_specs = (row_spec, P(both_axes), in_w_spec, in_w_spec, in_w_spec, out_w_spec, out_w_spec, cache_spec, cache_spec, len_spec)
    out_specs = (row_spec, cache_spec, cache_spec)
    return jax.shard_map(local_layer, mesh=mesh, in_specs=in_specs, out_specs=out_specs, check_vma=False)
```

```python
import functools

import jax
import jax.numpy as jnp
from jax import lax
from jax.experimental import pallas as pl
from jax.experimental.pallas import tpu as pltpu
from jax.sharding import PartitionSpec as P

MESH = pl.DeviceIdType.MESH
VMEM_LIMIT = 67043328
ROWS = 128
HD = 256
LOC = 512
OUT_ROOM = 8000000
TILE = 512
SA = 5
SPLIT = 10
NT = 8
QC = 768
NQ = 3
W_FIRST = 8
W_AHEAD = 12

f32 = jnp.float32
bf16 = jnp.bfloat16


def local_copy(src, dst, sem):
    return pltpu.make_async_copy(src, dst, sem)


def remote_copy(src, dst, ssem, rsem, dev):
    return pltpu.make_async_remote_copy(src, dst, ssem, rsem, device_id=dev, device_id_type=MESH)


def in_proj_kernel(x_hbm, g_hbm, wq_ref, wg_ref, wu_ref, qkv_ref, sa_ref, sb_ref, r0_ref, d_ref,
                   wqv, wv, x_ref, g_ref, xr, gr, qout, st, stx, h, qp, qr, qxs, qxr, qf, qyr, sbuf, rbuf, obuf,
                   wqsem, wsem, xs_sem, xr_sem, gs_sem, gr_sem, sts_sem, str_sem,
                   qds_sem, qdr_sem, qxs_sem, qxr_sem, qys_sem, qyr_sem, ds_sem, dr_sem, out_sem, xin_sem, gin_sem, qo_sem, es_sem, er_sem):
    d_model = 4096
    x = lax.axis_index("x")
    yz = lax.axis_index("yz")
    core = lax.rem(x, 2)
    x_core = x + 1 - 2 * core
    x_chip = lax.rem(x + 2, 4)
    x_diag = x_chip + 1 - 2 * core
    me = 2 * x + yz
    partner = {"x": x_core}
    xpeer = {"x": x_chip}
    ypeer = {"yz": 1 - yz}

    barrier = pltpu.get_barrier_semaphore()
    others = []
    for dx in range(4):
        for dy in range(2):
            if dx or dy:
                others.append((lax.rem(x + dx, 4), lax.rem(yz + dy, 2)))
    for ox, oy in others:
        pl.semaphore_signal(barrier, inc=1, device_id={"x": ox, "yz": oy}, device_id_type=MESH)
    x_in = local_copy(x_hbm, x_ref, xin_sem)
    g_in = local_copy(g_hbm, g_ref, gin_sem)
    x_in.start()
    g_in.start()

    def wq_copy(j):
        return local_copy(wq_ref.at[:, pl.ds(QC * j, QC)], wqv.at[j], wqsem.at[j])

    quarters = (x_diag, x_chip, x_core, x)

    def w_start(slot):
        phase = slot // NT
        q = quarters[0]
        for n in range(1, 4):
            q = jnp.where(phase == n, quarters[n], q)
        cols = pl.multiple_of(q * 2048 + (slot % NT) // 2 * TILE, TILE)

        def start(w_hbm):
            local_copy(w_hbm.at[:, pl.ds(cols, TILE)], wv.at[slot], wsem.at[slot]).start()

        if isinstance(slot, int):
            start(wg_ref if slot % 2 == 0 else wu_ref)
        else:
            pl.when(slot % 2 == 0)(lambda: start(wg_ref))
            pl.when(slot % 2 == 1)(lambda: start(wu_ref))

    def w_wait(slot):
        local_copy(wg_ref.at[:, pl.ds(0, TILE)], wv.at[slot], wsem.at[slot]).wait()

    x_in.wait()
    for j in range(NQ):
        wq_copy(j).start()
    for slot in range(W_FIRST):
        w_start(slot)
    g_in.wait()
    xf = x_ref[...].astype(f32)
    s1 = jnp.sum(xf, axis=1, keepdims=True)
    s2 = jnp.sum(xf * xf, axis=1, keepdims=True)
    lane = lax.broadcasted_iota(jnp.int32, (ROWS, ROWS), 1)
    stat = jnp.where(lane == 0, s1, s2).T
    st[me] = stat[0:8]

    pl.semaphore_wait(barrier, 7)

    x_send = remote_copy(x_ref, xr, xs_sem, xr_sem, ypeer)
    g_send = remote_copy(g_ref, gr, gs_sem, gr_sem, ypeer)
    for n, (ox, oy) in enumerate(others):
        remote_copy(st.at[me], stx.at[me], sts_sem.at[n], str_sem.at[me], {"x": ox, "yz": oy}).start()
    g_send.start()
    x_send.start()
    stx[me] = st[me]
    for n, (ox, oy) in enumerate(others):
        src = 2 * ox + oy
        remote_copy(st.at[me], stx.at[src], sts_sem.at[n], str_sem.at[src], {"x": ox, "yz": oy}).wait()
    tot = jnp.sum(stx[...], axis=0)
    tot = jnp.concatenate([tot, jnp.zeros((120, ROWS), f32)], axis=0).T
    mean = tot[:, 0:1] / d_model
    var = tot[:, 1:2] / d_model - mean * mean
    rstd = lax.rsqrt(var + 1e-6)
    own_cols = pl.multiple_of(yz * LOC, LOC)
    peer_cols = pl.multiple_of((1 - yz) * LOC, LOC)
    h[:, pl.ds(own_cols, LOC)] = ((xf - mean) * rstd * g_ref[...].astype(f32).reshape(1, LOC)).astype(bf16)
    x_send.wait()
    g_send.wait()
    h[:, pl.ds(peer_cols, LOC)] = ((xr[...].astype(f32) - mean) * rstd * gr[...].astype(f32).reshape(1, LOC)).astype(bf16)

    for slot in range(W_FIRST, W_AHEAD):
        w_start(slot)

    def q_compute(j):
        wq_copy(j).wait()
        part = jnp.dot(h[...], wqv[j], preferred_element_type=f32)
        qp[j] = part.reshape(4, 32, QC)

    def q_pair(j, k):
        block = (x_diag, x_core)[k]
        return remote_copy(qp.at[j, block], qr.at[j, k], qds_sem.at[j, k], qdr_sem.at[j, k], partner)

    def q_pair_start(j):
        q_pair(j, 0).start()
        q_pair(j, 1).start()

    def q_chip(j):
        return remote_copy(qxs.at[j], qxr.at[j], qxs_sem.at[j], qxr_sem.at[j], xpeer)

    def q_sum(j):
        q_pair(j, 0).wait()
        qxs[j] = qp[j, x_chip] + qr[j, 0]

    def tile(slot):
        w_wait(slot)
        if isinstance(slot, int):
            if slot + W_AHEAD < 4 * NT:
                w_start(slot + W_AHEAD)
        else:
            @pl.when(slot + W_AHEAD < 4 * NT)
            def _():
                w_start(slot + W_AHEAD)
        return jnp.dot(h[...], wv[slot], preferred_element_type=f32)

    def d_copy(i):
        return remote_copy(sbuf.at[i], rbuf.at[i], ds_sem.at[i], dr_sem.at[i], partner)

    def s_out(i):
        dst = sa_ref.at[i - 1] if i <= SA else sb_ref.at[i - 1 - SA]
        return local_copy(obuf.at[i], dst, out_sem.at[i])

    def d_out(i):
        return local_copy(obuf.at[NT + i], d_ref.at[i], out_sem.at[NT + i])

    early = remote_copy(obuf.at[0], r0_ref.at[0], es_sem, er_sem, xpeer)

    q_compute(0)
    q_compute(1)
    q_pair_start(0)
    q_compute(2)
    q_pair_start(1)

    after = {
        0: lambda: q_pair_start(2),
        1: lambda: q_sum(0),
        2: lambda: (q_chip(0).start(), q_sum(1)),
        3: lambda: (q_chip(1).start(), q_sum(2)),
        4: lambda: q_chip(2).start(),
    }
    for i in range(NT):
        sbuf[i] = tile(i)
        if i:
            d_copy(i - 1).start()
        if i in after:
            after[i]()

    for i in range(NT):
        part = tile(NT + i)
        if i == 0:
            d_copy(NT - 1).start()
        d_copy(i).wait()
        obuf[i] = part + rbuf[i]
        if i == 1:
            early.start()
        elif i:
            s_out(i - 1).start()

    own_rows = pl.multiple_of(yz * 16, 16)
    peer_rows = pl.multiple_of((1 - yz) * 16, 16)

    def q_y(j):
        return remote_copy(qf.at[j, pl.ds(peer_rows, 16)], qyr.at[j], qys_sem.at[j], qyr_sem.at[j], ypeer)

    def q_final(j):
        q_pair(j, 1).wait()
        q_chip(j).wait()
        qf[j] = (qp[j, x] + qr[j, 1] + qxr[j]).astype(bf16)
        qout[yz, :, pl.ds(QC * j, QC)] = qf[j, pl.ds(own_rows, 16)]

    def send_tiles(lo, hi):
        def body(i, _):
            sbuf[NT + i] = tile(2 * NT + i)

            @pl.when(i == 0)
            def _():
                s_out(NT - 1).start()

            @pl.when(i > 0)
            def _():
                d_copy(NT + i - 1).start()
            return 0

        lax.fori_loop(lo, hi, body, 0)

    def keep_tiles(lo, hi):
        def body(i, _):
            part = tile(3 * NT + i)

            @pl.when(i == 0)
            def _():
                d_copy(2 * NT - 1).start()
            d_copy(NT + i).wait()
            obuf[NT + i] = part + rbuf[NT + i]

            @pl.when(i > 0)
            def _():
                d_out(i - 1).start()
            return 0

        lax.fori_loop(lo, hi, body, 0)

    send_tiles(0, 3)
    q_final(0)
    send_tiles(3, 4)
    q_y(0).start()
    send_tiles(4, 8)
    keep_tiles(0, 2)
    q_final(1)
    keep_tiles(2, 3)
    q_y(1).start()
    keep_tiles(3, 7)
    q_final(2)
    keep_tiles(7, 8)
    q_y(2).start()
    d_out(NT - 1).start()
    for j in range(NQ):
        q_y(j).wait()
        qout[1 - yz, :, pl.ds(QC * j, QC)] = qyr[j]
    q_out = local_copy(qout, qkv_ref, qo_sem)
    q_out.start()
    for i in range(NT):
        if i:
            s_out(i).wait()
        d_out(i).wait()
    q_out.wait()
    early.wait()


def in_proj(x_loc, gain, wq, wg, wu):
    anyspec = pl.BlockSpec(memory_space=pltpu.HBM)
    dma = pltpu.SemaphoreType.DMA
    return pl.pallas_call(
        in_proj_kernel,
        out_shape=[
            jax.ShapeDtypeStruct((2, 16, NQ * QC), bf16),
            jax.ShapeDtypeStruct((SA, ROWS, TILE), f32),
            jax.ShapeDtypeStruct((NT - 1 - SA, ROWS, TILE), f32),
            jax.ShapeDtypeStruct((1, ROWS, TILE), f32),
            jax.ShapeDtypeStruct((NT, ROWS, TILE), f32),
        ],
        in_specs=[anyspec] * 5,
        out_specs=[anyspec] * 5,
        scratch_shapes=[
            pltpu.VMEM((NQ, 1024, QC), bf16),
            pltpu.VMEM((4 * NT, 1024, TILE), bf16),
            pltpu.VMEM((ROWS, LOC), bf16),
            pltpu.VMEM((LOC,), bf16),
            pltpu.VMEM((ROWS, LOC), bf16),
            pltpu.VMEM((LOC,), bf16),
            pltpu.VMEM((2, 16, NQ * QC), bf16),
            pltpu.VMEM((8, 8, ROWS), f32),
            pltpu.VMEM((8, 8, ROWS), f32),
            pltpu.VMEM((ROWS, 1024), bf16),
            pltpu.VMEM((NQ, 4, 32, QC), f32),
            pltpu.VMEM((NQ, 2, 32, QC), f32),
            pltpu.VMEM((NQ, 32, QC), f32),
            pltpu.VMEM((NQ, 32, QC), f32),
            pltpu.VMEM((NQ, 32, QC), bf16),
            pltpu.VMEM((NQ, 16, QC), bf16),
            pltpu.VMEM((2 * NT, ROWS, TILE), f32),
            pltpu.VMEM((2 * NT, ROWS, TILE), f32),
            pltpu.VMEM((2 * NT, ROWS, TILE), f32),
            dma((NQ,)), dma((4 * NT,)), dma, dma, dma, dma, dma((7,)), dma((8,)),
            dma((NQ, 2)), dma((NQ, 2)), dma((NQ,)), dma((NQ,)), dma((NQ,)), dma((NQ,)),
            dma((2 * NT,)), dma((2 * NT,)), dma((2 * NT,)), dma, dma, dma, dma, dma,
        ],
        compiler_params=pltpu.CompilerParams(
            collective_id=0, has_side_effects=True, vmem_limit_bytes=VMEM_LIMIT),
        cost_estimate=pl.CostEstimate(flops=5_000_000_000, bytes_accessed=45_000_000, transcendentals=0),
        name="in_proj",
    )(x_loc, gain, wq, wg, wu)


SLOTS = 6


def attend_kernel(lo, hi, len_hbm, qkv_hbm, k_ref, v_ref, *refs):
    if lo:
        refs = refs[2:]
    (ko_ref, vo_ref, o_hbm, o_ref, kb, vb, len_ref, qkv_ref, qs, kns, vns, osc,
     ksem, vsem, kosem, vosem, isem, osem) = refs
    t_len = k_ref.shape[1]

    def k_in(r, s):
        return local_copy(k_ref.at[r], kb.at[s], ksem.at[s])

    def v_in(r, s):
        return local_copy(v_ref.at[r], vb.at[s], vsem.at[s])

    def k_out(r, s):
        return local_copy(kb.at[s], ko_ref.at[r], kosem.at[s])

    def v_out(r, s):
        return local_copy(vb.at[s], vo_ref.at[r], vosem.at[s])

    AHEAD = 4
    len_in = local_copy(len_hbm, len_ref, isem.at[0])
    qkv_in = local_copy(qkv_hbm, qkv_ref, isem.at[1])
    len_in.start()
    qkv_in.start()
    for r in range(lo, lo + 2):
        k_in(r, r % SLOTS).start()
        v_in(r, r % SLOTS).start()
    len_in.wait()
    qkv_in.wait()
    for r in range(lo + 2, lo + AHEAD):
        k_in(r, r % SLOTS).start()
        v_in(r, r % SLOTS).start()
    row = lax.broadcasted_iota(jnp.int32, (16, ROWS), 0)
    lens = jnp.zeros((16, ROWS), jnp.int32)
    for r in range(16):
        lens = jnp.where(row == r, len_ref[r], lens)
    half = lax.broadcasted_iota(jnp.int32, (16, ROWS), 1).astype(f32)
    angles = lens.astype(f32) * 10000.0 ** (-half / ROWS)
    cos_t = jnp.cos(angles)
    sin_t = jnp.sin(angles)
    for g in range(17):
        part, base = (0, g * HD) if g < 9 else (1, (g - 9) * HD)
        a = qkv_ref[part, :, base:base + ROWS].astype(f32)
        b = qkv_ref[part, :, base + ROWS:base + HD].astype(f32)
        lower = (a * cos_t - b * sin_t).astype(bf16).astype(f32)
        upper = (b * cos_t + a * sin_t).astype(bf16).astype(f32)
        if g < 16:
            qs[:, g, 0:ROWS] = lower
            qs[:, g, ROWS:HD] = upper
        else:
            kns[:, 0:ROWS] = lower
            kns[:, ROWS:HD] = upper
    vns[...] = qkv_ref[1, :, 2048:2304].astype(f32)

    row16 = lax.broadcasted_iota(jnp.int32, (16, HD), 0)
    pos = lax.broadcasted_iota(jnp.int32, (16, t_len), 1)

    def body(r, _):
        s = lax.rem(r, SLOTS)
        nxt = r + AHEAD

        @pl.when(nxt < hi)
        def _():
            s2 = lax.rem(nxt, SLOTS)

            @pl.when(nxt - SLOTS >= lo)
            def _():
                k_out(nxt - SLOTS, s2).wait()
                v_out(nxt - SLOTS, s2).wait()
            k_in(nxt, s2).start()
            v_in(nxt, s2).start()

        p = len_ref[r]
        base = pl.multiple_of((p // 16) * 16, 16)
        hit = row16 == p - base
        k_in(r, s).wait()
        krow = kb[s, pl.ds(base, 16), :]
        kb[s, pl.ds(base, 16), :] = jnp.where(hit, kns[pl.ds(r, 1), :].astype(bf16), krow)
        v_in(r, s).wait()
        vrow = vb[s, pl.ds(base, 16), :]
        vb[s, pl.ds(base, 16), :] = jnp.where(hit, vns[pl.ds(r, 1), :].astype(bf16), vrow)
        q = qs[r].astype(bf16)
        sc = lax.dot_general(q, kb[s], (((1,), (1,)), ((), ())), preferred_element_type=f32) * (HD ** -0.5)
        k_out(r, s).start()
        v_out(r, s).start()
        sc = jnp.where(pos <= p, sc, -1e30)
        m = jnp.max(sc, axis=1, keepdims=True)
        e = jnp.exp(sc - m)
        den = jnp.sum(e, axis=1, keepdims=True)
        pr = (e / den).astype(bf16)
        osc[r] = jnp.dot(pr, vb[s], preferred_element_type=f32).astype(bf16).astype(f32)
        return 0

    lax.fori_loop(lo, hi, body, 0)
    for g in range(16):
        o_ref[:, HD * g:HD * (g + 1)] = osc[:, g, :].astype(bf16)
    o_out = local_copy(o_ref, o_hbm, osem)
    o_out.start()
    for r in range(max(lo, hi - SLOTS), hi):
        k_out(r, r % SLOTS).wait()
        v_out(r, r % SLOTS).wait()
    o_out.wait()


def attend(lo, hi, lens, qkv, kc, vc, *prev):
    anyspec = pl.BlockSpec(memory_space=pltpu.HBM)
    dma = pltpu.SemaphoreType.DMA
    n, t_len, hd = kc.shape
    return pl.pallas_call(
        functools.partial(attend_kernel, lo, hi),
        out_shape=[
            jax.ShapeDtypeStruct(kc.shape, bf16),
            jax.ShapeDtypeStruct(vc.shape, bf16),
            jax.ShapeDtypeStruct((n, 4096), bf16),
        ],
        in_specs=[anyspec] * (4 + len(prev)),
        out_specs=[anyspec] * 3,
        input_output_aliases={4: 0, 5: 1} if prev else {},
        scratch_shapes=[
            pltpu.VMEM((n, 4096), bf16),
            pltpu.VMEM((SLOTS, t_len, hd), bf16),
            pltpu.VMEM((SLOTS, t_len, hd), bf16),
            pltpu.SMEM((n,), jnp.int32),
            pltpu.VMEM((2, 16, NQ * QC), bf16),
            pltpu.VMEM((n, 16, hd), f32),
            pltpu.VMEM((n, hd), f32),
            pltpu.VMEM((n, hd), f32),
            pltpu.VMEM((n, 16, hd), f32),
            dma((SLOTS,)), dma((SLOTS,)), dma((SLOTS,)), dma((SLOTS,)), dma((2,)), dma,
        ],
        compiler_params=pltpu.CompilerParams(vmem_limit_bytes=VMEM_LIMIT),
        cost_estimate=pl.CostEstimate(flops=2_500_000_000 * (hi - lo), bytes_accessed=8_400_000 * (hi - lo), transcendentals=1_000_000),
        name=f"attend{lo}",
    )(lens, qkv, kc, vc, *prev)


NA = 3


def act_kernel(d_ref, r0_ref, r_ref, a_hbm, db, rb, a_ref, dsem, rsem, asem):
    def d_in(i):
        return local_copy(d_ref.at[i], db.at[i], dsem.at[i])

    def r_in(i):
        return local_copy(r_ref.at[i - 1] if i else r0_ref.at[0], rb.at[i], rsem.at[i])

    def a_out(t):
        return local_copy(a_ref.at[t], a_hbm.at[t], asem.at[t])

    for i in range(2 * NA):
        d_in(i).start()
        r_in(i).start()

    def total(i):
        d_in(i).wait()
        r_in(i).wait()
        return (db[i] + rb[i]).astype(bf16).astype(f32)

    for t in range(NA):
        a_ref[t] = (jax.nn.silu(total(2 * t)) * total(2 * t + 1)).astype(bf16)
        if t:
            a_out(t - 1).start()
    a_out(NA - 1).start()
    for t in range(NA):
        a_out(t).wait()


def act(d, r0, r):
    anyspec = pl.BlockSpec(memory_space=pltpu.HBM)
    dma = pltpu.SemaphoreType.DMA
    return pl.pallas_call(
        act_kernel,
        out_shape=jax.ShapeDtypeStruct((NA, ROWS, TILE), bf16),
        in_specs=[anyspec] * 3,
        out_specs=anyspec,
        scratch_shapes=[
            pltpu.VMEM((2 * NA, ROWS, TILE), f32),
            pltpu.VMEM((2 * NA, ROWS, TILE), f32),
            pltpu.VMEM((NA, ROWS, TILE), bf16),
            dma((2 * NA,)), dma((2 * NA,)), dma((NA,)),
        ],
        compiler_params=pltpu.CompilerParams(vmem_limit_bytes=VMEM_LIMIT),
        cost_estimate=pl.CostEstimate(flops=5_000_000, bytes_accessed=4_000_000, transcendentals=200_000),
        name="act",
    )(d, r0, r)


def out_proj_kernel(o1_hbm, o2_hbm, x_hbm, d_ref, r_ref, ao_ref, ax_ref, wao_ref, wmo_ref, y_ref,
                    o1_ref, o2_ref, o_ref, x_ref, db, rb, wao, wmo, ab, ob, zs, zk, zr,
                    osem, xsem, dsem, rsem, asem, waosem, wmosem, pss, psr, fss, fsr, e_s, e_r,
                    o0s, o0r, o1s, o1r, o2s, o2r, o3s, o3r, zss, zrs):
    x = lax.axis_index("x")
    yz = lax.axis_index("yz")
    core = lax.rem(x, 2)
    x_core = x + 1 - 2 * core
    x_chip = lax.rem(x + 2, 4)
    x_diag = x_chip + 1 - 2 * core
    partner = {"x": x_core}
    xpeer = {"x": x_chip}
    ypeer = {"yz": 1 - yz}

    barrier = pltpu.get_barrier_semaphore()
    for dev in (partner, xpeer, ypeer):
        pl.semaphore_signal(barrier, inc=1, device_id=dev, device_id_type=MESH)

    o_in = [local_copy(o1_hbm, o1_ref, osem.at[0]), local_copy(o2_hbm, o2_ref, osem.at[1])]
    for c in o_in:
        c.start()
    first = pl.ds(0, NA)
    own_in = local_copy(ao_ref, ab.at[x, first], asem.at[0])
    chip_in = local_copy(ax_ref, ab.at[x_chip, first], asem.at[1])
    own_in.start()
    chip_in.start()
    loads = [local_copy(d_ref.at[pl.ds(2 * NA, 2)], db, dsem), local_copy(r_ref, rb, rsem)]
    for c in loads:
        c.start()
    for c in o_in:
        c.wait()
    x_in = local_copy(x_hbm, x_ref, xsem)
    x_in.start()

    order = (x, x_chip, x_core, x_diag)

    halves = (pl.ds(pl.multiple_of((1 - yz) * LOC, LOC), LOC), pl.ds(pl.multiple_of(yz * LOC, LOC), LOC))
    accs = (zs, zk)

    def wmo_in(half, n, t):
        rows = pl.multiple_of(order[n] * 2048 + t * TILE, TILE)
        k = 4 * n + t
        return local_copy(wmo_ref.at[pl.ds(rows, TILE), halves[half]], wmo.at[half, k], wmosem.at[half, k])

    def wao_in(half):
        return local_copy(wao_ref.at[:, halves[half]], wao.at[half], waosem.at[half])

    def wmo_start(half, n):
        for t in range(4):
            wmo_in(half, n, t).start()

    wmo_start(0, 0)
    row = lax.broadcasted_iota(jnp.int32, (16, 4096), 0)
    o_ref[...] = jnp.where(row < SPLIT, o1_ref[...].astype(f32), o2_ref[...].astype(f32)).astype(bf16)
    own_half = pl.multiple_of(yz * 2048, 2048)
    peer_half = pl.multiple_of((1 - yz) * 2048, 2048)
    mine = 2 * x + yz
    theirs = 2 * x + 1 - yz
    ob[mine] = o_ref[:, pl.ds(own_half, 2048)]

    for c in loads:
        c.wait()
    gate = (db[0] + rb[0]).astype(bf16).astype(f32)
    up = (db[1] + rb[1]).astype(bf16).astype(f32)
    ab[x, NA] = (jax.nn.silu(gate) * up).astype(bf16)
    pl.semaphore_wait(barrier, 3)

    o_y = remote_copy(o_ref.at[:, pl.ds(peer_half, 2048)], ob.at[mine], o0s, o0r, ypeer)

    def o_hop(k, ss, rs, dev, owner):
        block = ob.at[2 * owner + (yz if k == 0 else 1 - yz)]
        return remote_copy(block, block, ss.at[k], rs.at[k], dev)

    o_part = [o_hop(k, o1s, o1r, partner, x) for k in range(2)]
    o_chip = [o_hop(k, o2s, o2r, xpeer, x) for k in range(2)]
    o_fwd = [o_hop(k, o3s, o3r, partner, x_chip) for k in range(2)]

    def a_hop(owner, tiles, ss, rs, k, dev):
        block = ab.at[owner, tiles]
        return remote_copy(block, block, ss.at[k], rs.at[k], dev)

    last = pl.ds(NA, 1)
    a_part = [a_hop(x, first, pss, psr, 0, partner), a_hop(x, last, pss, psr, 1, partner)]
    a_fwd = [a_hop(x_chip, first, fss, fsr, 0, partner), a_hop(x_chip, last, fss, fsr, 1, partner)]
    a_chip = remote_copy(ab.at[x, last], ab.at[x, last], e_s, e_r, xpeer)

    o_y.start()
    a_chip.start()
    o_chip[0].start()
    o_part[0].start()
    a_part[1].start()
    own_in.wait()
    a_part[0].start()
    chip_in.wait()
    a_fwd[0].start()
    wmo_start(0, 1)
    wmo_start(0, 2)

    def mlp(half, n, t, init=False):
        wmo_in(half, n, t).wait()
        acc = accs[half]
        part = jnp.dot(ab[order[n], t], wmo[half, 4 * n + t], preferred_element_type=f32)
        acc[...] = part if init else acc[...] + part

    chip = x // 2
    own_rows = pl.multiple_of(64 * chip, 64)
    chip_rows = pl.multiple_of(32 * x_chip, 32)
    diag_rows = pl.multiple_of(32 * x_diag, 32)

    def z_y(c, base, m):
        rows = pl.ds(base, m)
        return remote_copy(zs.at[rows], zr.at[rows], zss.at[c], zrs.at[c], ypeer)

    def attn_rows(half, base, m):
        rows = pl.ds(base, m)
        attn = ob[pl.ds(base // 16, m // 16)].reshape(m, 2048)
        accs[half][rows] += jnp.dot(attn, wao[half], preferred_element_type=f32)

    blocks = ((own_rows, 64), (chip_rows, 32), (diag_rows, 32))
    for t in range(4):
        mlp(0, 0, t, init=t == 0)
    o_y.wait()
    o_chip[1].start()
    o_part[1].start()
    wao_in(0).start()
    wmo_start(0, 3)
    wmo_start(1, 0)
    wmo_start(1, 1)
    for t in range(NA):
        mlp(0, 1, t)
    a_part[0].wait()
    for t in range(NA):
        mlp(0, 2, t)
    a_chip.wait()
    a_fwd[1].start()
    mlp(0, 1, NA)
    a_part[1].wait()
    mlp(0, 2, NA)
    o_chip[0].wait()
    o_fwd[0].start()
    wao_in(0).wait()
    for k in range(2):
        o_part[k].wait()
    attn_rows(0, *blocks[0])
    a_fwd[0].wait()
    for t in range(NA):
        mlp(0, 3, t)
    a_fwd[1].wait()
    mlp(0, 3, NA)
    wmo_start(1, 2)
    wmo_start(1, 3)
    wao_in(1).start()
    mlp(1, 0, 0, init=True)
    z_y(0, *blocks[0]).start()
    o_chip[1].wait()
    o_fwd[1].start()
    attn_rows(0, *blocks[1])
    mlp(1, 0, 1)
    z_y(1, *blocks[1]).start()
    for k in range(2):
        o_fwd[k].wait()
    attn_rows(0, *blocks[2])
    mlp(1, 0, 2)
    z_y(2, *blocks[2]).start()
    mlp(1, 0, NA)
    for n in range(1, 4):
        for t in range(4):
            mlp(1, n, t)
    wao_in(1).wait()
    attn_rows(1, 0, ROWS)
    x_in.wait()
    for c, (base, m) in enumerate(blocks):
        z_y(c, base, m).wait()
        rows = pl.ds(base, m)
        y_ref[rows, :] = (x_ref[rows, :].astype(f32) + (zk[rows, :] + zr[rows, :])).astype(bf16)


def out_proj(o1, o2, x_loc, d, r, a_own, a_chip, wao, wmo):
    anyspec = pl.BlockSpec(memory_space=pltpu.HBM)
    vspec = pl.BlockSpec(memory_space=pltpu.VMEM)
    dma = pltpu.SemaphoreType.DMA
    two = dma((2,))
    return pl.pallas_call(
        out_proj_kernel,
        out_shape=jax.ShapeDtypeStruct((ROWS, LOC), bf16),
        in_specs=[anyspec] * 9,
        out_specs=vspec,
        scratch_shapes=[
            pltpu.VMEM((16, 4096), bf16),
            pltpu.VMEM((16, 4096), bf16),
            pltpu.VMEM((16, 4096), bf16),
            pltpu.VMEM((ROWS, LOC), bf16),
            pltpu.VMEM((2, ROWS, TILE), f32),
            pltpu.VMEM((2, ROWS, TILE), f32),
            pltpu.VMEM((2, 2048, LOC), bf16),
            pltpu.VMEM((2, 16, TILE, LOC), bf16),
            pltpu.VMEM((4, 4, ROWS, TILE), bf16),
            pltpu.VMEM((8, 16, 2048), bf16),
            pltpu.VMEM((ROWS, LOC), f32),
            pltpu.VMEM((ROWS, LOC), f32),
            pltpu.VMEM((ROWS, LOC), f32),
            two, dma, dma, dma, two, two, dma((2, 16)),
            two, two, two, two, dma, dma,
            dma, dma, two, two, two, two, two, two, dma((3,)), dma((3,)),
        ],
        compiler_params=pltpu.CompilerParams(
            collective_id=1, has_side_effects=True, vmem_limit_bytes=VMEM_LIMIT - OUT_ROOM),
        cost_estimate=pl.CostEstimate(flops=3_000_000_000, bytes_accessed=26_000_000, transcendentals=0),
        name="out_proj",
    )(o1, o2, x_loc, d, r, a_own, a_chip, wao, wmo)


def solution(mesh):
    both_axes = ("x", "yz")
    row_spec = P("dp", both_axes)
    in_w_spec = P("x", "yz")
    out_w_spec = P("yz", "x")
    cache_spec = P(("dp", "x", "yz"), None, None)
    len_spec = P(("dp", "x", "yz"))
    swap = [(0, 2), (2, 0), (1, 3), (3, 1)]

    def local_layer(x_loc, gain_loc, wqkv_loc, wgate_loc, wup_loc, wao_loc, wmo_loc, kc_loc, vc_loc, len_loc):
        qkv, sa, sb, r0, d = in_proj(x_loc, gain_loc, wqkv_loc, wgate_loc, wup_loc)
        ra = lax.ppermute(sa, "x", swap)
        k_all, v_all, o1 = attend(0, SPLIT, len_loc, qkv, kc_loc, vc_loc)
        sb, o1 = lax.optimization_barrier((sb, o1))
        rb = lax.ppermute(sb, "x", swap)
        a_own = act(d, r0, ra)
        a_chip = lax.ppermute(a_own, "x", swap)
        k_all, v_all, o2 = attend(SPLIT, 16, len_loc, qkv, kc_loc, vc_loc, k_all, v_all)
        y_loc = out_proj(o1, o2, x_loc, d, rb, a_own, a_chip, wao_loc, wmo_loc)
        return y_loc, k_all, v_all

    in_specs = (row_spec, P(both_axes), in_w_spec, in_w_spec, in_w_spec, out_w_spec, out_w_spec, cache_spec, cache_spec, len_spec)
    out_specs = (row_spec, cache_spec, cache_spec)
    return jax.shard_map(local_layer, mesh=mesh, in_specs=in_specs, out_specs=out_specs, check_vma=False)
```

```python
import functools

import jax
import jax.numpy as jnp
from jax import lax
from jax.experimental import pallas as pl
from jax.experimental.pallas import tpu as pltpu
from jax.sharding import PartitionSpec as P

MESH = pl.DeviceIdType.MESH
VMEM_LIMIT = 67043328
ROWS = 128
HD = 256
LOC = 512
TALL = 2 ** 23
OUT_ROOM = 11700000
TILE = 512
SA = 5
SPLIT = 10
NT = 8
QC = 768
NQ = 3
W_FIRST = 8
W_AHEAD = 12

f32 = jnp.float32
bf16 = jnp.bfloat16


def local_copy(src, dst, sem):
    return pltpu.make_async_copy(src, dst, sem)


def remote_copy(src, dst, ssem, rsem, dev):
    return pltpu.make_async_remote_copy(src, dst, ssem, rsem, device_id=dev, device_id_type=MESH)


def in_proj_kernel(x_hbm, g_hbm, wq_ref, wg_ref, wu_ref, qkv_ref, sa_ref, sb_ref, r0_ref, d_ref, xc_ref,
                   wqv, wv, x_ref, g_ref, xr, gr, qout, st, stx, h, qp, qr, qxs, qxr, qf, qyr, sbuf, rbuf, obuf,
                   wqsem, wsem, xs_sem, xr_sem, gs_sem, gr_sem, sts_sem, str_sem,
                   qds_sem, qdr_sem, qxs_sem, qxr_sem, qys_sem, qyr_sem, ds_sem, dr_sem, out_sem, xin_sem, gin_sem, qo_sem, es_sem, er_sem, xc_sem):
    d_model = 4096
    x = lax.axis_index("x")
    yz = lax.axis_index("yz")
    core = lax.rem(x, 2)
    x_core = x + 1 - 2 * core
    x_chip = lax.rem(x + 2, 4)
    x_diag = x_chip + 1 - 2 * core
    me = 2 * x + yz
    partner = {"x": x_core}
    xpeer = {"x": x_chip}
    ypeer = {"yz": 1 - yz}

    barrier = pltpu.get_barrier_semaphore()
    others = []
    for dx in range(4):
        for dy in range(2):
            if dx or dy:
                others.append((lax.rem(x + dx, 4), lax.rem(yz + dy, 2)))
    for ox, oy in others:
        pl.semaphore_signal(barrier, inc=1, device_id={"x": ox, "yz": oy}, device_id_type=MESH)
    x_in = local_copy(x_hbm, x_ref, xin_sem)
    g_in = local_copy(g_hbm, g_ref, gin_sem)
    x_in.start()
    g_in.start()

    def wq_copy(j):
        return local_copy(wq_ref.at[:, pl.ds(QC * j, QC)], wqv.at[j], wqsem.at[j])

    quarters = (x_diag, x_chip, x_core, x)

    def w_start(slot):
        phase = slot // NT
        q = quarters[0]
        for n in range(1, 4):
            q = jnp.where(phase == n, quarters[n], q)
        cols = pl.multiple_of(q * 2048 + (slot % NT) // 2 * TILE, TILE)

        def start(w_hbm):
            local_copy(w_hbm.at[:, pl.ds(cols, TILE)], wv.at[slot], wsem.at[slot]).start()

        if isinstance(slot, int):
            start(wg_ref if slot % 2 == 0 else wu_ref)
        else:
            pl.when(slot % 2 == 0)(lambda: start(wg_ref))
            pl.when(slot % 2 == 1)(lambda: start(wu_ref))

    def w_wait(slot):
        local_copy(wg_ref.at[:, pl.ds(0, TILE)], wv.at[slot], wsem.at[slot]).wait()

    x_in.wait()
    for j in range(NQ):
        wq_copy(j).start()
    for slot in range(W_FIRST):
        w_start(slot)
    g_in.wait()
    xf = x_ref[...].astype(f32)
    s1 = jnp.sum(xf, axis=1, keepdims=True)
    s2 = jnp.sum(xf * xf, axis=1, keepdims=True)
    lane = lax.broadcasted_iota(jnp.int32, (ROWS, ROWS), 1)
    stat = jnp.where(lane == 0, s1, s2).T
    st[me] = stat[0:8]

    pl.semaphore_wait(barrier, 7)

    x_send = remote_copy(x_ref, xr, xs_sem, xr_sem, ypeer)
    g_send = remote_copy(g_ref, gr, gs_sem, gr_sem, ypeer)
    for n, (ox, oy) in enumerate(others):
        remote_copy(st.at[me], stx.at[me], sts_sem.at[n], str_sem.at[me], {"x": ox, "yz": oy}).start()
    g_send.start()
    x_send.start()
    stx[me] = st[me]
    for n, (ox, oy) in enumerate(others):
        src = 2 * ox + oy
        remote_copy(st.at[me], stx.at[src], sts_sem.at[n], str_sem.at[src], {"x": ox, "yz": oy}).wait()
    tot = jnp.sum(stx[...], axis=0)
    tot = jnp.concatenate([tot, jnp.zeros((120, ROWS), f32)], axis=0).T
    mean = tot[:, 0:1] / d_model
    var = tot[:, 1:2] / d_model - mean * mean
    rstd = lax.rsqrt(var + 1e-6)
    own_cols = pl.multiple_of(yz * LOC, LOC)
    peer_cols = pl.multiple_of((1 - yz) * LOC, LOC)
    h[:, pl.ds(own_cols, LOC)] = ((xf - mean) * rstd * g_ref[...].astype(f32).reshape(1, LOC)).astype(bf16)
    x_send.wait()
    g_send.wait()
    h[:, pl.ds(peer_cols, LOC)] = ((xr[...].astype(f32) - mean) * rstd * gr[...].astype(f32).reshape(1, LOC)).astype(bf16)

    for slot in range(W_FIRST, W_AHEAD):
        w_start(slot)

    def q_compute(j):
        wq_copy(j).wait()
        part = jnp.dot(h[...], wqv[j], preferred_element_type=f32)
        qp[j] = part.reshape(4, 32, QC)

    def q_pair(j, k):
        block = (x_diag, x_core)[k]
        return remote_copy(qp.at[j, block], qr.at[j, k], qds_sem.at[j, k], qdr_sem.at[j, k], partner)

    def q_pair_start(j):
        q_pair(j, 0).start()
        q_pair(j, 1).start()

    def q_chip(j):
        return remote_copy(qxs.at[j], qxr.at[j], qxs_sem.at[j], qxr_sem.at[j], xpeer)

    def q_sum(j):
        q_pair(j, 0).wait()
        qxs[j] = qp[j, x_chip] + qr[j, 0]

    def tile(slot):
        w_wait(slot)
        if isinstance(slot, int):
            if slot + W_AHEAD < 4 * NT:
                w_start(slot + W_AHEAD)
        else:
            @pl.when(slot + W_AHEAD < 4 * NT)
            def _():
                w_start(slot + W_AHEAD)
        return jnp.dot(h[...], wv[slot], preferred_element_type=f32)

    def d_copy(i):
        return remote_copy(sbuf.at[i], rbuf.at[i], ds_sem.at[i], dr_sem.at[i], partner)

    def s_out(i):
        dst = sa_ref.at[i - 1] if i <= SA else sb_ref.at[i - 1 - SA]
        return local_copy(obuf.at[i], dst, out_sem.at[i])

    def d_out(i):
        return local_copy(obuf.at[NT + i], d_ref.at[i], out_sem.at[NT + i])

    early = remote_copy(obuf.at[0], r0_ref.at[0], es_sem, er_sem, xpeer)

    q_compute(0)
    q_compute(1)
    q_pair_start(0)
    q_compute(2)
    q_pair_start(1)

    after = {
        0: lambda: q_pair_start(2),
        1: lambda: q_sum(0),
        2: lambda: (q_chip(0).start(), q_sum(1)),
        3: lambda: (q_chip(1).start(), q_sum(2)),
        4: lambda: q_chip(2).start(),
    }
    for i in range(NT):
        sbuf[i] = tile(i)
        if i:
            d_copy(i - 1).start()
        if i in after:
            after[i]()

    for i in range(NT):
        part = tile(NT + i)
        if i == 0:
            d_copy(NT - 1).start()
        d_copy(i).wait()
        obuf[i] = part + rbuf[i]
        if i == 1:
            early.start()
        elif i:
            s_out(i - 1).start()

    own_rows = pl.multiple_of(yz * 16, 16)
    peer_rows = pl.multiple_of((1 - yz) * 16, 16)

    def q_y(j):
        return remote_copy(qf.at[j, pl.ds(peer_rows, 16)], qyr.at[j], qys_sem.at[j], qyr_sem.at[j], ypeer)

    def q_final(j):
        q_pair(j, 1).wait()
        q_chip(j).wait()
        qf[j] = (qp[j, x] + qr[j, 1] + qxr[j]).astype(bf16)
        qout[yz, :, pl.ds(QC * j, QC)] = qf[j, pl.ds(own_rows, 16)]

    def send_tiles(lo, hi):
        def body(i, _):
            sbuf[NT + i] = tile(2 * NT + i)

            @pl.when(i == 0)
            def _():
                s_out(NT - 1).start()

            @pl.when(i > 0)
            def _():
                d_copy(NT + i - 1).start()
            return 0

        lax.fori_loop(lo, hi, body, 0)

    def keep_tiles(lo, hi):
        def body(i, _):
            part = tile(3 * NT + i)

            @pl.when(i == 0)
            def _():
                d_copy(2 * NT - 1).start()
            d_copy(NT + i).wait()
            obuf[NT + i] = part + rbuf[NT + i]

            @pl.when(i > 0)
            def _():
                d_out(i - 1).start()
            return 0

        lax.fori_loop(lo, hi, body, 0)

    send_tiles(0, 3)
    q_final(0)
    send_tiles(3, 4)
    q_y(0).start()
    send_tiles(4, 8)
    keep_tiles(0, 2)
    q_final(1)
    keep_tiles(2, 3)
    q_y(1).start()
    keep_tiles(3, 7)
    q_final(2)
    keep_tiles(7, 8)
    q_y(2).start()
    d_out(NT - 1).start()
    for j in range(NQ):
        q_y(j).wait()
        qout[1 - yz, :, pl.ds(QC * j, QC)] = qyr[j]
    q_out = local_copy(qout, qkv_ref, qo_sem)
    q_out.start()
    x_out = local_copy(x_ref, xc_ref.at[pl.ds(0, ROWS)], xc_sem)
    x_out.start()
    for i in range(NT):
        if i:
            s_out(i).wait()
        d_out(i).wait()
    q_out.wait()
    x_out.wait()
    early.wait()


def in_proj(x_loc, gain, wq, wg, wu):
    anyspec = pl.BlockSpec(memory_space=pltpu.HBM)
    dma = pltpu.SemaphoreType.DMA
    return pl.pallas_call(
        in_proj_kernel,
        out_shape=[
            jax.ShapeDtypeStruct((2, 16, NQ * QC), bf16),
            jax.ShapeDtypeStruct((SA, ROWS, TILE), f32),
            jax.ShapeDtypeStruct((NT - 1 - SA, ROWS, TILE), f32),
            jax.ShapeDtypeStruct((1, ROWS, TILE), f32),
            jax.ShapeDtypeStruct((NT, ROWS, TILE), f32),
            jax.ShapeDtypeStruct((TALL // LOC, LOC), bf16),
        ],
        in_specs=[anyspec] * 5,
        out_specs=[anyspec] * 6,
        scratch_shapes=[
            pltpu.VMEM((NQ, 1024, QC), bf16),
            pltpu.VMEM((4 * NT, 1024, TILE), bf16),
            pltpu.VMEM((ROWS, LOC), bf16),
            pltpu.VMEM((LOC,), bf16),
            pltpu.VMEM((ROWS, LOC), bf16),
            pltpu.VMEM((LOC,), bf16),
            pltpu.VMEM((2, 16, NQ * QC), bf16),
            pltpu.VMEM((8, 8, ROWS), f32),
            pltpu.VMEM((8, 8, ROWS), f32),
            pltpu.VMEM((ROWS, 1024), bf16),
            pltpu.VMEM((NQ, 4, 32, QC), f32),
            pltpu.VMEM((NQ, 2, 32, QC), f32),
            pltpu.VMEM((NQ, 32, QC), f32),
            pltpu.VMEM((NQ, 32, QC), f32),
            pltpu.VMEM((NQ, 32, QC), bf16),
            pltpu.VMEM((NQ, 16, QC), bf16),
            pltpu.VMEM((2 * NT, ROWS, TILE), f32),
            pltpu.VMEM((2 * NT, ROWS, TILE), f32),
            pltpu.VMEM((2 * NT, ROWS, TILE), f32),
            dma((NQ,)), dma((4 * NT,)), dma, dma, dma, dma, dma((7,)), dma((8,)),
            dma((NQ, 2)), dma((NQ, 2)), dma((NQ,)), dma((NQ,)), dma((NQ,)), dma((NQ,)),
            dma((2 * NT,)), dma((2 * NT,)), dma((2 * NT,)), dma, dma, dma, dma, dma, dma,
        ],
        compiler_params=pltpu.CompilerParams(
            collective_id=0, has_side_effects=True, vmem_limit_bytes=VMEM_LIMIT),
        cost_estimate=pl.CostEstimate(flops=5_000_000_000, bytes_accessed=45_000_000, transcendentals=0),
        name="in_proj",
    )(x_loc, gain, wq, wg, wu)


SLOTS = 6


def attend_kernel(lo, hi, len_hbm, qkv_hbm, k_ref, v_ref, *refs):
    if lo:
        refs = refs[2:]
    (ko_ref, vo_ref, o_hbm, o_ref, kb, vb, len_ref, qkv_ref, qs, kns, vns, osc,
     ksem, vsem, kosem, vosem, isem, osem) = refs
    t_len = k_ref.shape[1]

    def k_in(r, s):
        return local_copy(k_ref.at[r], kb.at[s], ksem.at[s])

    def v_in(r, s):
        return local_copy(v_ref.at[r], vb.at[s], vsem.at[s])

    def k_out(r, s):
        return local_copy(kb.at[s], ko_ref.at[r], kosem.at[s])

    def v_out(r, s):
        return local_copy(vb.at[s], vo_ref.at[r], vosem.at[s])

    AHEAD = 4
    len_in = local_copy(len_hbm, len_ref, isem.at[0])
    qkv_in = local_copy(qkv_hbm, qkv_ref, isem.at[1])
    len_in.start()
    qkv_in.start()
    for r in range(lo, lo + 2):
        k_in(r, r % SLOTS).start()
        v_in(r, r % SLOTS).start()
    len_in.wait()
    qkv_in.wait()
    for r in range(lo + 2, lo + AHEAD):
        k_in(r, r % SLOTS).start()
        v_in(r, r % SLOTS).start()
    row = lax.broadcasted_iota(jnp.int32, (16, ROWS), 0)
    lens = jnp.zeros((16, ROWS), jnp.int32)
    for r in range(16):
        lens = jnp.where(row == r, len_ref[r], lens)
    half = lax.broadcasted_iota(jnp.int32, (16, ROWS), 1).astype(f32)
    angles = lens.astype(f32) * 10000.0 ** (-half / ROWS)
    cos_t = jnp.cos(angles)
    sin_t = jnp.sin(angles)
    for g in range(17):
        part, base = (0, g * HD) if g < 9 else (1, (g - 9) * HD)
        a = qkv_ref[part, :, base:base + ROWS].astype(f32)
        b = qkv_ref[part, :, base + ROWS:base + HD].astype(f32)
        lower = (a * cos_t - b * sin_t).astype(bf16).astype(f32)
        upper = (b * cos_t + a * sin_t).astype(bf16).astype(f32)
        if g < 16:
            qs[:, g, 0:ROWS] = lower
            qs[:, g, ROWS:HD] = upper
        else:
            kns[:, 0:ROWS] = lower
            kns[:, ROWS:HD] = upper
    vns[...] = qkv_ref[1, :, 2048:2304].astype(f32)

    row16 = lax.broadcasted_iota(jnp.int32, (16, HD), 0)
    pos = lax.broadcasted_iota(jnp.int32, (16, t_len), 1)

    def body(r, _):
        s = lax.rem(r, SLOTS)
        nxt = r + AHEAD

        @pl.when(nxt < hi)
        def _():
            s2 = lax.rem(nxt, SLOTS)

            @pl.when(nxt - SLOTS >= lo)
            def _():
                k_out(nxt - SLOTS, s2).wait()
                v_out(nxt - SLOTS, s2).wait()
            k_in(nxt, s2).start()
            v_in(nxt, s2).start()

        p = len_ref[r]
        base = pl.multiple_of((p // 16) * 16, 16)
        hit = row16 == p - base
        k_in(r, s).wait()
        krow = kb[s, pl.ds(base, 16), :]
        kb[s, pl.ds(base, 16), :] = jnp.where(hit, kns[pl.ds(r, 1), :].astype(bf16), krow)
        v_in(r, s).wait()
        vrow = vb[s, pl.ds(base, 16), :]
        vb[s, pl.ds(base, 16), :] = jnp.where(hit, vns[pl.ds(r, 1), :].astype(bf16), vrow)
        q = qs[r].astype(bf16)
        sc = lax.dot_general(q, kb[s], (((1,), (1,)), ((), ())), preferred_element_type=f32) * (HD ** -0.5)
        k_out(r, s).start()
        v_out(r, s).start()
        sc = jnp.where(pos <= p, sc, -1e30)
        m = jnp.max(sc, axis=1, keepdims=True)
        e = jnp.exp(sc - m)
        den = jnp.sum(e, axis=1, keepdims=True)
        pr = (e / den).astype(bf16)
        osc[r] = jnp.dot(pr, vb[s], preferred_element_type=f32).astype(bf16).astype(f32)
        return 0

    lax.fori_loop(lo, hi, body, 0)
    for g in range(16):
        o_ref[:, HD * g:HD * (g + 1)] = osc[:, g, :].astype(bf16)
    o_out = local_copy(o_ref, o_hbm.at[pl.ds(0, 16)], osem)
    o_out.start()
    for r in range(max(lo, hi - SLOTS), hi):
        k_out(r, r % SLOTS).wait()
        v_out(r, r % SLOTS).wait()
    o_out.wait()


def attend(lo, hi, lens, qkv, kc, vc, *prev):
    anyspec = pl.BlockSpec(memory_space=pltpu.HBM)
    dma = pltpu.SemaphoreType.DMA
    n, t_len, hd = kc.shape
    return pl.pallas_call(
        functools.partial(attend_kernel, lo, hi),
        out_shape=[
            jax.ShapeDtypeStruct(kc.shape, bf16),
            jax.ShapeDtypeStruct(vc.shape, bf16),
            jax.ShapeDtypeStruct((TALL // 4096, 4096), bf16),
        ],
        in_specs=[anyspec] * (4 + len(prev)),
        out_specs=[anyspec] * 3,
        input_output_aliases={4: 0, 5: 1} if prev else {},
        scratch_shapes=[
            pltpu.VMEM((n, 4096), bf16),
            pltpu.VMEM((SLOTS, t_len, hd), bf16),
            pltpu.VMEM((SLOTS, t_len, hd), bf16),
            pltpu.SMEM((n,), jnp.int32),
            pltpu.VMEM((2, 16, NQ * QC), bf16),
            pltpu.VMEM((n, 16, hd), f32),
            pltpu.VMEM((n, hd), f32),
            pltpu.VMEM((n, hd), f32),
            pltpu.VMEM((n, 16, hd), f32),
            dma((SLOTS,)), dma((SLOTS,)), dma((SLOTS,)), dma((SLOTS,)), dma((2,)), dma,
        ],
        compiler_params=pltpu.CompilerParams(vmem_limit_bytes=VMEM_LIMIT),
        cost_estimate=pl.CostEstimate(flops=2_500_000_000 * (hi - lo), bytes_accessed=8_400_000 * (hi - lo), transcendentals=1_000_000),
        name=f"attend{lo}",
    )(lens, qkv, kc, vc, *prev)


NA = 3


def act_kernel(d_ref, r0_ref, r_ref, a_hbm, at_hbm, db, rb, a_ref, dsem, rsem, asem, tsem):
    def d_in(i):
        return local_copy(d_ref.at[i], db.at[i], dsem.at[i])

    def r_in(i):
        return local_copy(r_ref.at[i - 1] if i else r0_ref.at[0], rb.at[i], rsem.at[i])

    def a_out(t):
        return local_copy(a_ref.at[t], a_hbm.at[t], asem.at[t])

    tall = local_copy(a_ref, at_hbm.at[pl.ds(0, NA)], tsem)

    for i in range(2 * NA):
        d_in(i).start()
        r_in(i).start()

    def total(i):
        d_in(i).wait()
        r_in(i).wait()
        return (db[i] + rb[i]).astype(bf16).astype(f32)

    for t in range(NA):
        a_ref[t] = (jax.nn.silu(total(2 * t)) * total(2 * t + 1)).astype(bf16)
        if t:
            a_out(t - 1).start()
    a_out(NA - 1).start()
    tall.start()
    for t in range(NA):
        a_out(t).wait()
    tall.wait()


def act(d, r0, r):
    anyspec = pl.BlockSpec(memory_space=pltpu.HBM)
    dma = pltpu.SemaphoreType.DMA
    return pl.pallas_call(
        act_kernel,
        out_shape=[
            jax.ShapeDtypeStruct((NA, ROWS, TILE), bf16),
            jax.ShapeDtypeStruct((TALL // (ROWS * TILE), ROWS, TILE), bf16),
        ],
        in_specs=[anyspec] * 3,
        out_specs=[anyspec] * 2,
        scratch_shapes=[
            pltpu.VMEM((2 * NA, ROWS, TILE), f32),
            pltpu.VMEM((2 * NA, ROWS, TILE), f32),
            pltpu.VMEM((NA, ROWS, TILE), bf16),
            dma((2 * NA,)), dma((2 * NA,)), dma((NA,)), dma,
        ],
        compiler_params=pltpu.CompilerParams(vmem_limit_bytes=VMEM_LIMIT),
        cost_estimate=pl.CostEstimate(flops=5_000_000, bytes_accessed=4_000_000, transcendentals=200_000),
        name="act",
    )(d, r0, r)


def out_proj_kernel(o1_hbm, o2_hbm, x_hbm, d_ref, r_ref, ao_ref, ax_ref, wao_ref, wmo_ref, y_ref,
                    o1_ref, o2_ref, o_ref, x_ref, db, rb, wao, wmo, ab, ob, zs, zk, zr,
                    osem, xsem, dsem, rsem, asem, waosem, wmosem, pss, psr, fss, fsr, e_s, e_r,
                    o0s, o0r, o1s, o1r, o2s, o2r, o3s, o3r, zss, zrs):
    x = lax.axis_index("x")
    yz = lax.axis_index("yz")
    core = lax.rem(x, 2)
    x_core = x + 1 - 2 * core
    x_chip = lax.rem(x + 2, 4)
    x_diag = x_chip + 1 - 2 * core
    partner = {"x": x_core}
    xpeer = {"x": x_chip}
    ypeer = {"yz": 1 - yz}

    barrier = pltpu.get_barrier_semaphore()
    for dev in (partner, xpeer, ypeer):
        pl.semaphore_signal(barrier, inc=1, device_id=dev, device_id_type=MESH)

    top = pl.ds(0, 16)
    o_in = [local_copy(o1_hbm.at[top], o1_ref, osem.at[0]), local_copy(o2_hbm.at[top], o2_ref, osem.at[1])]
    for c in o_in:
        c.start()
    first = pl.ds(0, NA)
    own_in = local_copy(ao_ref.at[first], ab.at[x, first], asem.at[0])
    chip_in = local_copy(ax_ref, ab.at[x_chip, first], asem.at[1])
    own_in.start()
    chip_in.start()
    loads = [local_copy(d_ref.at[pl.ds(2 * NA, 2)], db, dsem), local_copy(r_ref, rb, rsem)]
    for c in loads:
        c.start()
    for c in o_in:
        c.wait()
    x_in = local_copy(x_hbm.at[pl.ds(0, ROWS)], x_ref, xsem)
    x_in.start()

    order = (x, x_chip, x_core, x_diag)

    halves = (pl.ds(pl.multiple_of((1 - yz) * LOC, LOC), LOC), pl.ds(pl.multiple_of(yz * LOC, LOC), LOC))
    accs = (zs, zk)

    def wmo_in(half, n, t):
        rows = pl.multiple_of(order[n] * 2048 + t * TILE, TILE)
        k = 4 * n + t
        return local_copy(wmo_ref.at[pl.ds(rows, TILE), halves[half]], wmo.at[half, k], wmosem.at[half, k])

    def wao_in(half):
        return local_copy(wao_ref.at[:, halves[half]], wao.at[half], waosem.at[half])

    def wmo_start(half, n):
        for t in range(4):
            wmo_in(half, n, t).start()

    wmo_start(0, 0)
    row = lax.broadcasted_iota(jnp.int32, (16, 4096), 0)
    o_ref[...] = jnp.where(row < SPLIT, o1_ref[...].astype(f32), o2_ref[...].astype(f32)).astype(bf16)
    own_half = pl.multiple_of(yz * 2048, 2048)
    peer_half = pl.multiple_of((1 - yz) * 2048, 2048)
    mine = 2 * x + yz
    theirs = 2 * x + 1 - yz
    ob[mine] = o_ref[:, pl.ds(own_half, 2048)]

    for c in loads:
        c.wait()
    gate = (db[0] + rb[0]).astype(bf16).astype(f32)
    up = (db[1] + rb[1]).astype(bf16).astype(f32)
    ab[x, NA] = (jax.nn.silu(gate) * up).astype(bf16)
    pl.semaphore_wait(barrier, 3)

    o_y = remote_copy(o_ref.at[:, pl.ds(peer_half, 2048)], ob.at[mine], o0s, o0r, ypeer)

    def o_hop(k, ss, rs, dev, owner):
        block = ob.at[2 * owner + (yz if k == 0 else 1 - yz)]
        return remote_copy(block, block, ss.at[k], rs.at[k], dev)

    o_part = [o_hop(k, o1s, o1r, partner, x) for k in range(2)]
    o_chip = [o_hop(k, o2s, o2r, xpeer, x) for k in range(2)]
    o_fwd = [o_hop(k, o3s, o3r, partner, x_chip) for k in range(2)]

    def a_hop(owner, tiles, ss, rs, k, dev):
        block = ab.at[owner, tiles]
        return remote_copy(block, block, ss.at[k], rs.at[k], dev)

    last = pl.ds(NA, 1)
    a_part = [a_hop(x, first, pss, psr, 0, partner), a_hop(x, last, pss, psr, 1, partner)]
    a_fwd = [a_hop(x_chip, first, fss, fsr, 0, partner), a_hop(x_chip, last, fss, fsr, 1, partner)]
    a_chip = remote_copy(ab.at[x, last], ab.at[x, last], e_s, e_r, xpeer)

    o_y.start()
    a_chip.start()
    o_chip[0].start()
    o_part[0].start()
    a_part[1].start()
    own_in.wait()
    a_part[0].start()
    chip_in.wait()
    a_fwd[0].start()
    wmo_start(0, 1)
    wmo_start(0, 2)

    def mlp(half, n, t, init=False):
        wmo_in(half, n, t).wait()
        acc = accs[half]
        part = jnp.dot(ab[order[n], t], wmo[half, 4 * n + t], preferred_element_type=f32)
        acc[...] = part if init else acc[...] + part

    chip = x // 2
    own_rows = pl.multiple_of(64 * chip, 64)
    chip_rows = pl.multiple_of(32 * x_chip, 32)
    diag_rows = pl.multiple_of(32 * x_diag, 32)

    def z_y(c, base, m):
        rows = pl.ds(base, m)
        return remote_copy(zs.at[rows], zr.at[rows], zss.at[c], zrs.at[c], ypeer)

    def attn_rows(half, base, m):
        rows = pl.ds(base, m)
        attn = ob[pl.ds(base // 16, m // 16)].reshape(m, 2048)
        accs[half][rows] += jnp.dot(attn, wao[half], preferred_element_type=f32)

    blocks = ((own_rows, 64), (chip_rows, 32), (diag_rows, 32))
    for t in range(4):
        mlp(0, 0, t, init=t == 0)
    o_y.wait()
    o_chip[1].start()
    o_part[1].start()
    wao_in(0).start()
    wmo_start(0, 3)
    wmo_start(1, 0)
    wmo_start(1, 1)
    for t in range(NA):
        mlp(0, 1, t)
    a_part[0].wait()
    for t in range(NA):
        mlp(0, 2, t)
    a_chip.wait()
    a_fwd[1].start()
    mlp(0, 1, NA)
    a_part[1].wait()
    mlp(0, 2, NA)
    o_chip[0].wait()
    o_fwd[0].start()
    wao_in(0).wait()
    for k in range(2):
        o_part[k].wait()
    attn_rows(0, *blocks[0])
    a_fwd[0].wait()
    for t in range(NA):
        mlp(0, 3, t)
    a_fwd[1].wait()
    mlp(0, 3, NA)
    wmo_start(1, 2)
    wmo_start(1, 3)
    wao_in(1).start()
    mlp(1, 0, 0, init=True)
    z_y(0, *blocks[0]).start()
    o_chip[1].wait()
    o_fwd[1].start()
    attn_rows(0, *blocks[1])
    mlp(1, 0, 1)
    z_y(1, *blocks[1]).start()
    for k in range(2):
        o_fwd[k].wait()
    attn_rows(0, *blocks[2])
    mlp(1, 0, 2)
    z_y(2, *blocks[2]).start()
    mlp(1, 0, NA)
    for n in range(1, 4):
        for t in range(4):
            mlp(1, n, t)
    wao_in(1).wait()
    attn_rows(1, 0, ROWS)
    x_in.wait()
    for c, (base, m) in enumerate(blocks):
        z_y(c, base, m).wait()
        rows = pl.ds(base, m)
        y_ref[rows, :] = (x_ref[rows, :].astype(f32) + (zk[rows, :] + zr[rows, :])).astype(bf16)


def out_proj(o1, o2, x_loc, d, r, a_own, a_chip, wao, wmo):
    anyspec = pl.BlockSpec(memory_space=pltpu.HBM)
    vspec = pl.BlockSpec(memory_space=pltpu.VMEM)
    dma = pltpu.SemaphoreType.DMA
    two = dma((2,))
    return pl.pallas_call(
        out_proj_kernel,
        out_shape=jax.ShapeDtypeStruct((ROWS, LOC), bf16),
        in_specs=[anyspec] * 9,
        out_specs=vspec,
        scratch_shapes=[
            pltpu.VMEM((16, 4096), bf16),
            pltpu.VMEM((16, 4096), bf16),
            pltpu.VMEM((16, 4096), bf16),
            pltpu.VMEM((ROWS, LOC), bf16),
            pltpu.VMEM((2, ROWS, TILE), f32),
            pltpu.VMEM((2, ROWS, TILE), f32),
            pltpu.VMEM((2, 2048, LOC), bf16),
            pltpu.VMEM((2, 16, TILE, LOC), bf16),
            pltpu.VMEM((4, 4, ROWS, TILE), bf16),
            pltpu.VMEM((8, 16, 2048), bf16),
            pltpu.VMEM((ROWS, LOC), f32),
            pltpu.VMEM((ROWS, LOC), f32),
            pltpu.VMEM((ROWS, LOC), f32),
            two, dma, dma, dma, two, two, dma((2, 16)),
            two, two, two, two, dma, dma,
            dma, dma, two, two, two, two, two, two, dma((3,)), dma((3,)),
        ],
        compiler_params=pltpu.CompilerParams(
            collective_id=1, has_side_effects=True, vmem_limit_bytes=VMEM_LIMIT - OUT_ROOM),
        cost_estimate=pl.CostEstimate(flops=3_000_000_000, bytes_accessed=26_000_000, transcendentals=0),
        name="out_proj",
    )(o1, o2, x_loc, d, r, a_own, a_chip, wao, wmo)


def solution(mesh):
    both_axes = ("x", "yz")
    row_spec = P("dp", both_axes)
    in_w_spec = P("x", "yz")
    out_w_spec = P("yz", "x")
    cache_spec = P(("dp", "x", "yz"), None, None)
    len_spec = P(("dp", "x", "yz"))
    swap = [(0, 2), (2, 0), (1, 3), (3, 1)]

    def local_layer(x_loc, gain_loc, wqkv_loc, wgate_loc, wup_loc, wao_loc, wmo_loc, kc_loc, vc_loc, len_loc):
        qkv, sa, sb, r0, d, x_tall = in_proj(x_loc, gain_loc, wqkv_loc, wgate_loc, wup_loc)
        ra = lax.ppermute(sa, "x", swap)
        k_all, v_all, o1 = attend(0, SPLIT, len_loc, qkv, kc_loc, vc_loc)
        sb, o1 = lax.optimization_barrier((sb, o1))
        rb = lax.ppermute(sb, "x", swap)
        a_own, a_tall = act(d, r0, ra)
        a_chip = lax.ppermute(a_own, "x", swap)
        k_all, v_all, o2 = attend(SPLIT, 16, len_loc, qkv, kc_loc, vc_loc, k_all, v_all)
        y_loc = out_proj(o1, o2, x_tall, d, rb, a_tall, a_chip, wao_loc, wmo_loc)
        return y_loc, k_all, v_all

    in_specs = (row_spec, P(both_axes), in_w_spec, in_w_spec, in_w_spec, out_w_spec, out_w_spec, cache_spec, cache_spec, len_spec)
    out_specs = (row_spec, cache_spec, cache_spec)
    return jax.shard_map(local_layer, mesh=mesh, in_specs=in_specs, out_specs=out_specs, check_vma=False)
```

```python
import functools

import jax
import jax.numpy as jnp
from jax import lax
from jax.experimental import pallas as pl
from jax.experimental.pallas import tpu as pltpu
from jax.sharding import PartitionSpec as P

MESH = pl.DeviceIdType.MESH
VMEM_LIMIT = 67043328
ROWS = 128
HD = 256
LOC = 512
ACT_LIMIT = 46 * 2 ** 20
TALL = 2 ** 23
OUT_ROOM = 11700000
TILE = 512
SA = 5
SPLIT = 10
NT = 8
QC = 768
NQ = 3
W_FIRST = 8
W_AHEAD = 12

f32 = jnp.float32
bf16 = jnp.bfloat16


def local_copy(src, dst, sem):
    return pltpu.make_async_copy(src, dst, sem)


def remote_copy(src, dst, ssem, rsem, dev):
    return pltpu.make_async_remote_copy(src, dst, ssem, rsem, device_id=dev, device_id_type=MESH)


def in_proj_kernel(x_hbm, g_hbm, len_hbm, wq_ref, wg_ref, wu_ref, qkv_ref, sa_ref, sb_ref, r0_ref, d_ref, xc_ref, lens_ref,
                   wqv, wv, x_ref, g_ref, len_s, lens, xr, gr, qout, st, stx, h, qp, qr, qxs, qxr, qf, qyr, sbuf, rbuf, obuf,
                   wqsem, wsem, xs_sem, xr_sem, gs_sem, gr_sem, sts_sem, str_sem,
                   qds_sem, qdr_sem, qxs_sem, qxr_sem, qys_sem, qyr_sem, ds_sem, dr_sem, out_sem, xin_sem, gin_sem, qo_sem, es_sem, er_sem, xc_sem, len_sem, lens_sem):
    d_model = 4096
    x = lax.axis_index("x")
    yz = lax.axis_index("yz")
    core = lax.rem(x, 2)
    x_core = x + 1 - 2 * core
    x_chip = lax.rem(x + 2, 4)
    x_diag = x_chip + 1 - 2 * core
    me = 2 * x + yz
    partner = {"x": x_core}
    xpeer = {"x": x_chip}
    ypeer = {"yz": 1 - yz}

    barrier = pltpu.get_barrier_semaphore()
    others = []
    for dx in range(4):
        for dy in range(2):
            if dx or dy:
                others.append((lax.rem(x + dx, 4), lax.rem(yz + dy, 2)))
    for ox, oy in others:
        pl.semaphore_signal(barrier, inc=1, device_id={"x": ox, "yz": oy}, device_id_type=MESH)
    x_in = local_copy(x_hbm, x_ref, xin_sem)
    g_in = local_copy(g_hbm, g_ref, gin_sem)
    x_in.start()
    g_in.start()
    len_in = local_copy(len_hbm, len_s, len_sem)
    len_in.start()

    def wq_copy(j):
        return local_copy(wq_ref.at[:, pl.ds(QC * j, QC)], wqv.at[j], wqsem.at[j])

    quarters = (x_diag, x_chip, x_core, x)

    def w_start(slot):
        phase = slot // NT
        q = quarters[0]
        for n in range(1, 4):
            q = jnp.where(phase == n, quarters[n], q)
        cols = pl.multiple_of(q * 2048 + (slot % NT) // 2 * TILE, TILE)

        def start(w_hbm):
            local_copy(w_hbm.at[:, pl.ds(cols, TILE)], wv.at[slot], wsem.at[slot]).start()

        if isinstance(slot, int):
            start(wg_ref if slot % 2 == 0 else wu_ref)
        else:
            pl.when(slot % 2 == 0)(lambda: start(wg_ref))
            pl.when(slot % 2 == 1)(lambda: start(wu_ref))

    def w_wait(slot):
        local_copy(wg_ref.at[:, pl.ds(0, TILE)], wv.at[slot], wsem.at[slot]).wait()

    x_in.wait()
    for j in range(NQ):
        wq_copy(j).start()
    for slot in range(W_FIRST):
        w_start(slot)
    g_in.wait()
    xf = x_ref[...].astype(f32)
    s1 = jnp.sum(xf, axis=1, keepdims=True)
    s2 = jnp.sum(xf * xf, axis=1, keepdims=True)
    lane = lax.broadcasted_iota(jnp.int32, (ROWS, ROWS), 1)
    stat = jnp.where(lane == 0, s1, s2).T
    st[me] = stat[0:8]

    pl.semaphore_wait(barrier, 7)

    x_send = remote_copy(x_ref, xr, xs_sem, xr_sem, ypeer)
    g_send = remote_copy(g_ref, gr, gs_sem, gr_sem, ypeer)
    for n, (ox, oy) in enumerate(others):
        remote_copy(st.at[me], stx.at[me], sts_sem.at[n], str_sem.at[me], {"x": ox, "yz": oy}).start()
    g_send.start()
    x_send.start()
    stx[me] = st[me]
    for n, (ox, oy) in enumerate(others):
        src = 2 * ox + oy
        remote_copy(st.at[me], stx.at[src], sts_sem.at[n], str_sem.at[src], {"x": ox, "yz": oy}).wait()
    tot = jnp.sum(stx[...], axis=0)
    tot = jnp.concatenate([tot, jnp.zeros((120, ROWS), f32)], axis=0).T
    mean = tot[:, 0:1] / d_model
    var = tot[:, 1:2] / d_model - mean * mean
    rstd = lax.rsqrt(var + 1e-6)
    own_cols = pl.multiple_of(yz * LOC, LOC)
    peer_cols = pl.multiple_of((1 - yz) * LOC, LOC)
    h[:, pl.ds(own_cols, LOC)] = ((xf - mean) * rstd * g_ref[...].astype(f32).reshape(1, LOC)).astype(bf16)
    x_send.wait()
    g_send.wait()
    h[:, pl.ds(peer_cols, LOC)] = ((xr[...].astype(f32) - mean) * rstd * gr[...].astype(f32).reshape(1, LOC)).astype(bf16)

    for slot in range(W_FIRST, W_AHEAD):
        w_start(slot)

    def q_compute(j):
        wq_copy(j).wait()
        part = jnp.dot(h[...], wqv[j], preferred_element_type=f32)
        qp[j] = part.reshape(4, 32, QC)

    def q_pair(j, k):
        block = (x_diag, x_core)[k]
        return remote_copy(qp.at[j, block], qr.at[j, k], qds_sem.at[j, k], qdr_sem.at[j, k], partner)

    def q_pair_start(j):
        q_pair(j, 0).start()
        q_pair(j, 1).start()

    def q_chip(j):
        return remote_copy(qxs.at[j], qxr.at[j], qxs_sem.at[j], qxr_sem.at[j], xpeer)

    def q_sum(j):
        q_pair(j, 0).wait()
        qxs[j] = qp[j, x_chip] + qr[j, 0]

    def tile(slot):
        w_wait(slot)
        if isinstance(slot, int):
            if slot + W_AHEAD < 4 * NT:
                w_start(slot + W_AHEAD)
        else:
            @pl.when(slot + W_AHEAD < 4 * NT)
            def _():
                w_start(slot + W_AHEAD)
        return jnp.dot(h[...], wv[slot], preferred_element_type=f32)

    def d_copy(i):
        return remote_copy(sbuf.at[i], rbuf.at[i], ds_sem.at[i], dr_sem.at[i], partner)

    def s_out(i):
        dst = sa_ref.at[i - 1] if i <= SA else sb_ref.at[i - 1 - SA]
        return local_copy(obuf.at[i], dst, out_sem.at[i])

    def d_out(i):
        return local_copy(obuf.at[NT + i], d_ref.at[i], out_sem.at[NT + i])

    early = remote_copy(obuf.at[0], r0_ref.at[0], es_sem, er_sem, xpeer)

    len_in.wait()
    row = lax.broadcasted_iota(jnp.int32, (16, ROWS), 0)
    rows = jnp.zeros((16, ROWS), jnp.int32)
    for r in range(16):
        rows = jnp.where(row == r, len_s[r], rows)
    lens[...] = rows

    q_compute(0)
    q_compute(1)
    q_pair_start(0)
    q_compute(2)
    q_pair_start(1)

    after = {
        0: lambda: q_pair_start(2),
        1: lambda: q_sum(0),
        2: lambda: (q_chip(0).start(), q_sum(1)),
        3: lambda: (q_chip(1).start(), q_sum(2)),
        4: lambda: q_chip(2).start(),
    }
    for i in range(NT):
        sbuf[i] = tile(i)
        if i:
            d_copy(i - 1).start()
        if i in after:
            after[i]()

    for i in range(NT):
        part = tile(NT + i)
        if i == 0:
            d_copy(NT - 1).start()
        d_copy(i).wait()
        obuf[i] = part + rbuf[i]
        if i == 1:
            early.start()
        elif i:
            s_out(i - 1).start()

    own_rows = pl.multiple_of(yz * 16, 16)
    peer_rows = pl.multiple_of((1 - yz) * 16, 16)

    def q_y(j):
        return remote_copy(qf.at[j, pl.ds(peer_rows, 16)], qyr.at[j], qys_sem.at[j], qyr_sem.at[j], ypeer)

    def q_final(j):
        q_pair(j, 1).wait()
        q_chip(j).wait()
        qf[j] = (qp[j, x] + qr[j, 1] + qxr[j]).astype(bf16)
        qout[yz, :, pl.ds(QC * j, QC)] = qf[j, pl.ds(own_rows, 16)]

    def send_tiles(lo, hi):
        def body(i, _):
            sbuf[NT + i] = tile(2 * NT + i)

            @pl.when(i == 0)
            def _():
                s_out(NT - 1).start()

            @pl.when(i > 0)
            def _():
                d_copy(NT + i - 1).start()
            return 0

        lax.fori_loop(lo, hi, body, 0)

    def keep_tiles(lo, hi):
        def body(i, _):
            part = tile(3 * NT + i)

            @pl.when(i == 0)
            def _():
                d_copy(2 * NT - 1).start()
            d_copy(NT + i).wait()
            obuf[NT + i] = part + rbuf[NT + i]

            @pl.when(i > 0)
            def _():
                d_out(i - 1).start()
            return 0

        lax.fori_loop(lo, hi, body, 0)

    send_tiles(0, 3)
    q_final(0)
    send_tiles(3, 4)
    q_y(0).start()
    send_tiles(4, 8)
    keep_tiles(0, 2)
    q_final(1)
    keep_tiles(2, 3)
    q_y(1).start()
    keep_tiles(3, 7)
    q_final(2)
    keep_tiles(7, 8)
    q_y(2).start()
    d_out(NT - 1).start()
    for j in range(NQ):
        q_y(j).wait()
        qout[1 - yz, :, pl.ds(QC * j, QC)] = qyr[j]
    q_out = local_copy(qout, qkv_ref.at[pl.ds(0, 2)], qo_sem)
    q_out.start()
    lens_out = local_copy(lens, lens_ref.at[pl.ds(0, 16)], lens_sem)
    lens_out.start()
    x_out = local_copy(x_ref, xc_ref.at[pl.ds(0, ROWS)], xc_sem)
    x_out.start()
    for i in range(NT):
        if i:
            s_out(i).wait()
        d_out(i).wait()
    q_out.wait()
    x_out.wait()
    lens_out.wait()
    early.wait()


def in_proj(x_loc, gain, lens, wq, wg, wu):
    anyspec = pl.BlockSpec(memory_space=pltpu.HBM)
    dma = pltpu.SemaphoreType.DMA
    return pl.pallas_call(
        in_proj_kernel,
        out_shape=[
            jax.ShapeDtypeStruct((TALL // (16 * NQ * QC), 16, NQ * QC), bf16),
            jax.ShapeDtypeStruct((SA, ROWS, TILE), f32),
            jax.ShapeDtypeStruct((NT - 1 - SA, ROWS, TILE), f32),
            jax.ShapeDtypeStruct((1, ROWS, TILE), f32),
            jax.ShapeDtypeStruct((NT, ROWS, TILE), f32),
            jax.ShapeDtypeStruct((TALL // LOC, LOC), bf16),
            jax.ShapeDtypeStruct((TALL // ROWS, ROWS), jnp.int32),
        ],
        in_specs=[anyspec] * 6,
        out_specs=[anyspec] * 7,
        scratch_shapes=[
            pltpu.VMEM((NQ, 1024, QC), bf16),
            pltpu.VMEM((4 * NT, 1024, TILE), bf16),
            pltpu.VMEM((ROWS, LOC), bf16),
            pltpu.VMEM((LOC,), bf16),
            pltpu.SMEM((16,), jnp.int32),
            pltpu.VMEM((16, ROWS), jnp.int32),
            pltpu.VMEM((ROWS, LOC), bf16),
            pltpu.VMEM((LOC,), bf16),
            pltpu.VMEM((2, 16, NQ * QC), bf16),
            pltpu.VMEM((8, 8, ROWS), f32),
            pltpu.VMEM((8, 8, ROWS), f32),
            pltpu.VMEM((ROWS, 1024), bf16),
            pltpu.VMEM((NQ, 4, 32, QC), f32),
            pltpu.VMEM((NQ, 2, 32, QC), f32),
            pltpu.VMEM((NQ, 32, QC), f32),
            pltpu.VMEM((NQ, 32, QC), f32),
            pltpu.VMEM((NQ, 32, QC), bf16),
            pltpu.VMEM((NQ, 16, QC), bf16),
            pltpu.VMEM((2 * NT, ROWS, TILE), f32),
            pltpu.VMEM((2 * NT, ROWS, TILE), f32),
            pltpu.VMEM((2 * NT, ROWS, TILE), f32),
            dma((NQ,)), dma((4 * NT,)), dma, dma, dma, dma, dma((7,)), dma((8,)),
            dma((NQ, 2)), dma((NQ, 2)), dma((NQ,)), dma((NQ,)), dma((NQ,)), dma((NQ,)),
            dma((2 * NT,)), dma((2 * NT,)), dma((2 * NT,)), dma, dma, dma, dma, dma, dma, dma, dma,
        ],
        compiler_params=pltpu.CompilerParams(
            collective_id=0, has_side_effects=True, vmem_limit_bytes=VMEM_LIMIT),
        cost_estimate=pl.CostEstimate(flops=5_000_000_000, bytes_accessed=45_000_000, transcendentals=0),
        name="in_proj",
    )(x_loc, gain, lens, wq, wg, wu)


SLOTS = 6


def attend_kernel(lo, hi, len_hbm, qkv_hbm, k_ref, v_ref, *refs):
    if lo:
        refs = refs[2:]
    (ko_ref, vo_ref, o_hbm, o_ref, kb, vb, len_ref, lens, qkv_ref, qs, kns, vns, osc,
     ksem, vsem, kosem, vosem, isem, osem) = refs
    t_len = k_ref.shape[1]

    def k_in(r, s):
        return local_copy(k_ref.at[r], kb.at[s], ksem.at[s])

    def v_in(r, s):
        return local_copy(v_ref.at[r], vb.at[s], vsem.at[s])

    def k_out(r, s):
        return local_copy(kb.at[s], ko_ref.at[r], kosem.at[s])

    def v_out(r, s):
        return local_copy(vb.at[s], vo_ref.at[r], vosem.at[s])

    AHEAD = 4
    len_in = local_copy(len_hbm.at[pl.ds(0, 16)], len_ref, isem.at[0])
    lens_in = local_copy(len_hbm.at[pl.ds(0, 16)], lens, isem.at[2])
    lens_in.start()
    qkv_in = local_copy(qkv_hbm.at[pl.ds(0, 2)], qkv_ref, isem.at[1])
    len_in.start()
    qkv_in.start()
    for r in range(lo, lo + 2):
        k_in(r, r % SLOTS).start()
        v_in(r, r % SLOTS).start()
    len_in.wait()
    lens_in.wait()
    qkv_in.wait()
    for r in range(lo + 2, lo + AHEAD):
        k_in(r, r % SLOTS).start()
        v_in(r, r % SLOTS).start()
    half = lax.broadcasted_iota(jnp.int32, (16, ROWS), 1).astype(f32)
    angles = lens[...].astype(f32) * 10000.0 ** (-half / ROWS)
    cos_t = jnp.cos(angles)
    sin_t = jnp.sin(angles)
    for g in range(17):
        part, base = (0, g * HD) if g < 9 else (1, (g - 9) * HD)
        a = qkv_ref[part, :, base:base + ROWS].astype(f32)
        b = qkv_ref[part, :, base + ROWS:base + HD].astype(f32)
        lower = (a * cos_t - b * sin_t).astype(bf16).astype(f32)
        upper = (b * cos_t + a * sin_t).astype(bf16).astype(f32)
        if g < 16:
            qs[:, g, 0:ROWS] = lower
            qs[:, g, ROWS:HD] = upper
        else:
            kns[:, 0:ROWS] = lower
            kns[:, ROWS:HD] = upper
    vns[...] = qkv_ref[1, :, 2048:2304].astype(f32)

    row16 = lax.broadcasted_iota(jnp.int32, (16, HD), 0)
    pos = lax.broadcasted_iota(jnp.int32, (16, t_len), 1)

    def body(r, _):
        s = lax.rem(r, SLOTS)
        nxt = r + AHEAD

        @pl.when(nxt < hi)
        def _():
            s2 = lax.rem(nxt, SLOTS)

            @pl.when(nxt - SLOTS >= lo)
            def _():
                k_out(nxt - SLOTS, s2).wait()
                v_out(nxt - SLOTS, s2).wait()
            k_in(nxt, s2).start()
            v_in(nxt, s2).start()

        p = len_ref[r, 0]
        base = pl.multiple_of((p // 16) * 16, 16)
        hit = row16 == p - base
        k_in(r, s).wait()
        krow = kb[s, pl.ds(base, 16), :]
        kb[s, pl.ds(base, 16), :] = jnp.where(hit, kns[pl.ds(r, 1), :].astype(bf16), krow)
        v_in(r, s).wait()
        vrow = vb[s, pl.ds(base, 16), :]
        vb[s, pl.ds(base, 16), :] = jnp.where(hit, vns[pl.ds(r, 1), :].astype(bf16), vrow)
        q = qs[r].astype(bf16)
        sc = lax.dot_general(q, kb[s], (((1,), (1,)), ((), ())), preferred_element_type=f32) * (HD ** -0.5)
        k_out(r, s).start()
        v_out(r, s).start()
        sc = jnp.where(pos <= p, sc, -1e30)
        m = jnp.max(sc, axis=1, keepdims=True)
        e = jnp.exp(sc - m)
        den = jnp.sum(e, axis=1, keepdims=True)
        pr = (e / den).astype(bf16)
        osc[r] = jnp.dot(pr, vb[s], preferred_element_type=f32).astype(bf16).astype(f32)
        return 0

    lax.fori_loop(lo, hi, body, 0)
    for g in range(16):
        o_ref[:, HD * g:HD * (g + 1)] = osc[:, g, :].astype(bf16)
    o_out = local_copy(o_ref, o_hbm.at[pl.ds(0, 16)], osem)
    o_out.start()
    for r in range(max(lo, hi - SLOTS), hi):
        k_out(r, r % SLOTS).wait()
        v_out(r, r % SLOTS).wait()
    o_out.wait()


def attend(lo, hi, lens, qkv, kc, vc, *prev):
    anyspec = pl.BlockSpec(memory_space=pltpu.HBM)
    dma = pltpu.SemaphoreType.DMA
    n, t_len, hd = kc.shape
    return pl.pallas_call(
        functools.partial(attend_kernel, lo, hi),
        out_shape=[
            jax.ShapeDtypeStruct(kc.shape, bf16),
            jax.ShapeDtypeStruct(vc.shape, bf16),
            jax.ShapeDtypeStruct((TALL // 4096, 4096), bf16),
        ],
        in_specs=[anyspec] * (4 + len(prev)),
        out_specs=[anyspec] * 3,
        input_output_aliases={4: 0, 5: 1} if prev else {},
        scratch_shapes=[
            pltpu.VMEM((n, 4096), bf16),
            pltpu.VMEM((SLOTS, t_len, hd), bf16),
            pltpu.VMEM((SLOTS, t_len, hd), bf16),
            pltpu.SMEM((n, ROWS), jnp.int32),
            pltpu.VMEM((n, ROWS), jnp.int32),
            pltpu.VMEM((2, 16, NQ * QC), bf16),
            pltpu.VMEM((n, 16, hd), f32),
            pltpu.VMEM((n, hd), f32),
            pltpu.VMEM((n, hd), f32),
            pltpu.VMEM((n, 16, hd), f32),
            dma((SLOTS,)), dma((SLOTS,)), dma((SLOTS,)), dma((SLOTS,)), dma((3,)), dma,
        ],
        compiler_params=pltpu.CompilerParams(vmem_limit_bytes=VMEM_LIMIT if lo else 44 * 2 ** 20),
        cost_estimate=pl.CostEstimate(flops=2_500_000_000 * (hi - lo), bytes_accessed=8_400_000 * (hi - lo), transcendentals=1_000_000),
        name=f"attend{lo}",
    )(lens, qkv, kc, vc, *prev)


NA = 3


def act_kernel(d_ref, r0_ref, r_ref, a_hbm, at_hbm, a_ref, asem, tsem):
    def a_out(t):
        return local_copy(a_ref.at[t], a_hbm.at[t], asem.at[t])

    tall = local_copy(a_ref, at_hbm.at[pl.ds(0, NA)], tsem)

    def total(i):
        other = r_ref[i - 1] if i else r0_ref[0]
        return (d_ref[i] + other).astype(bf16).astype(f32)

    for t in range(NA):
        a_ref[t] = (jax.nn.silu(total(2 * t)) * total(2 * t + 1)).astype(bf16)
        if t:
            a_out(t - 1).start()
    a_out(NA - 1).start()
    tall.start()
    for t in range(NA):
        a_out(t).wait()
    tall.wait()


def act(d, r0, r):
    anyspec = pl.BlockSpec(memory_space=pltpu.HBM)
    dma = pltpu.SemaphoreType.DMA
    return pl.pallas_call(
        act_kernel,
        out_shape=[
            jax.ShapeDtypeStruct((NA, ROWS, TILE), bf16),
            jax.ShapeDtypeStruct((TALL // (ROWS * TILE), ROWS, TILE), bf16),
        ],
        in_specs=[pl.BlockSpec(memory_space=pltpu.VMEM)] * 3,
        out_specs=[anyspec] * 2,
        scratch_shapes=[
            pltpu.VMEM((NA, ROWS, TILE), bf16),
            dma((NA,)), dma,
        ],
        compiler_params=pltpu.CompilerParams(vmem_limit_bytes=ACT_LIMIT),
        cost_estimate=pl.CostEstimate(flops=5_000_000, bytes_accessed=4_000_000, transcendentals=200_000),
        name="act",
    )(d, r0, r)


def out_proj_kernel(o1_hbm, o2_hbm, x_hbm, d_ref, r_ref, ao_ref, ax_ref, wao_ref, wmo_ref, y_ref,
                    o1_ref, o2_ref, o_ref, x_ref, db, rb, wao, wmo, ab, ob, zs, zk, zr,
                    osem, xsem, dsem, rsem, asem, waosem, wmosem, pss, psr, fss, fsr, e_s, e_r,
                    o0s, o0r, o1s, o1r, o2s, o2r, o3s, o3r, zss, zrs):
    x = lax.axis_index("x")
    yz = lax.axis_index("yz")
    core = lax.rem(x, 2)
    x_core = x + 1 - 2 * core
    x_chip = lax.rem(x + 2, 4)
    x_diag = x_chip + 1 - 2 * core
    partner = {"x": x_core}
    xpeer = {"x": x_chip}
    ypeer = {"yz": 1 - yz}

    barrier = pltpu.get_barrier_semaphore()
    for dev in (partner, xpeer, ypeer):
        pl.semaphore_signal(barrier, inc=1, device_id=dev, device_id_type=MESH)

    top = pl.ds(0, 16)
    o_in = [local_copy(o1_hbm.at[top], o1_ref, osem.at[0]), local_copy(o2_hbm.at[top], o2_ref, osem.at[1])]
    for c in o_in:
        c.start()
    first = pl.ds(0, NA)
    own_in = local_copy(ao_ref.at[first], ab.at[x, first], asem.at[0])
    chip_in = local_copy(ax_ref, ab.at[x_chip, first], asem.at[1])
    own_in.start()
    chip_in.start()
    loads = [local_copy(d_ref.at[pl.ds(2 * NA, 2)], db, dsem), local_copy(r_ref, rb, rsem)]
    for c in loads:
        c.start()
    for c in o_in:
        c.wait()
    x_in = local_copy(x_hbm.at[pl.ds(0, ROWS)], x_ref, xsem)
    x_in.start()

    order = (x, x_chip, x_core, x_diag)

    halves = (pl.ds(pl.multiple_of((1 - yz) * LOC, LOC), LOC), pl.ds(pl.multiple_of(yz * LOC, LOC), LOC))
    accs = (zs, zk)

    def wmo_in(half, n, t):
        rows = pl.multiple_of(order[n] * 2048 + t * TILE, TILE)
        k = 4 * n + t
        return local_copy(wmo_ref.at[pl.ds(rows, TILE), halves[half]], wmo.at[half, k], wmosem.at[half, k])

    def wao_in(half):
        return local_copy(wao_ref.at[:, halves[half]], wao.at[half], waosem.at[half])

    def wmo_start(half, n):
        for t in range(4):
            wmo_in(half, n, t).start()

    wmo_start(0, 0)
    row = lax.broadcasted_iota(jnp.int32, (16, 4096), 0)
    o_ref[...] = jnp.where(row < SPLIT, o1_ref[...].astype(f32), o2_ref[...].astype(f32)).astype(bf16)
    own_half = pl.multiple_of(yz * 2048, 2048)
    peer_half = pl.multiple_of((1 - yz) * 2048, 2048)
    mine = 2 * x + yz
    theirs = 2 * x + 1 - yz
    ob[mine] = o_ref[:, pl.ds(own_half, 2048)]

    for c in loads:
        c.wait()
    gate = (db[0] + rb[0]).astype(bf16).astype(f32)
    up = (db[1] + rb[1]).astype(bf16).astype(f32)
    ab[x, NA] = (jax.nn.silu(gate) * up).astype(bf16)
    pl.semaphore_wait(barrier, 3)

    o_y = remote_copy(o_ref.at[:, pl.ds(peer_half, 2048)], ob.at[mine], o0s, o0r, ypeer)

    def o_hop(k, ss, rs, dev, owner):
        block = ob.at[2 * owner + (yz if k == 0 else 1 - yz)]
        return remote_copy(block, block, ss.at[k], rs.at[k], dev)

    o_part = [o_hop(k, o1s, o1r, partner, x) for k in range(2)]
    o_chip = [o_hop(k, o2s, o2r, xpeer, x) for k in range(2)]
    o_fwd = [o_hop(k, o3s, o3r, partner, x_chip) for k in range(2)]

    def a_hop(owner, tiles, ss, rs, k, dev):
        block = ab.at[owner, tiles]
        return remote_copy(block, block, ss.at[k], rs.at[k], dev)

    last = pl.ds(NA, 1)
    a_part = [a_hop(x, first, pss, psr, 0, partner), a_hop(x, last, pss, psr, 1, partner)]
    a_fwd = [a_hop(x_chip, first, fss, fsr, 0, partner), a_hop(x_chip, last, fss, fsr, 1, partner)]
    a_chip = remote_copy(ab.at[x, last], ab.at[x, last], e_s, e_r, xpeer)

    o_y.start()
    a_chip.start()
    o_chip[0].start()
    o_part[0].start()
    a_part[1].start()
    own_in.wait()
    a_part[0].start()
    chip_in.wait()
    a_fwd[0].start()
    wmo_start(0, 1)
    wmo_start(0, 2)

    def mlp(half, n, t, init=False):
        wmo_in(half, n, t).wait()
        acc = accs[half]
        part = jnp.dot(ab[order[n], t], wmo[half, 4 * n + t], preferred_element_type=f32)
        acc[...] = part if init else acc[...] + part

    chip = x // 2
    own_rows = pl.multiple_of(64 * chip, 64)
    chip_rows = pl.multiple_of(32 * x_chip, 32)
    diag_rows = pl.multiple_of(32 * x_diag, 32)

    def z_y(c, base, m):
        rows = pl.ds(base, m)
        return remote_copy(zs.at[rows], zr.at[rows], zss.at[c], zrs.at[c], ypeer)

    def attn_rows(half, base, m):
        rows = pl.ds(base, m)
        attn = ob[pl.ds(base // 16, m // 16)].reshape(m, 2048)
        accs[half][rows] += jnp.dot(attn, wao[half], preferred_element_type=f32)

    blocks = ((own_rows, 64), (chip_rows, 32), (diag_rows, 32))
    for t in range(4):
        mlp(0, 0, t, init=t == 0)
    o_y.wait()
    o_chip[1].start()
    o_part[1].start()
    wao_in(0).start()
    wmo_start(0, 3)
    wmo_start(1, 0)
    wmo_start(1, 1)
    for t in range(NA):
        mlp(0, 1, t)
    a_part[0].wait()
    for t in range(NA):
        mlp(0, 2, t)
    a_chip.wait()
    a_fwd[1].start()
    mlp(0, 1, NA)
    a_part[1].wait()
    mlp(0, 2, NA)
    o_chip[0].wait()
    o_fwd[0].start()
    wao_in(0).wait()
    for k in range(2):
        o_part[k].wait()
    attn_rows(0, *blocks[0])
    a_fwd[0].wait()
    for t in range(NA):
        mlp(0, 3, t)
    a_fwd[1].wait()
    mlp(0, 3, NA)
    wmo_start(1, 2)
    wmo_start(1, 3)
    wao_in(1).start()
    mlp(1, 0, 0, init=True)
    z_y(0, *blocks[0]).start()
    o_chip[1].wait()
    o_fwd[1].start()
    attn_rows(0, *blocks[1])
    mlp(1, 0, 1)
    z_y(1, *blocks[1]).start()
    for k in range(2):
        o_fwd[k].wait()
    attn_rows(0, *blocks[2])
    mlp(1, 0, 2)
    z_y(2, *blocks[2]).start()
    mlp(1, 0, NA)
    for n in range(1, 4):
        for t in range(4):
            mlp(1, n, t)
    wao_in(1).wait()
    attn_rows(1, 0, ROWS)
    x_in.wait()
    for c, (base, m) in enumerate(blocks):
        z_y(c, base, m).wait()
        rows = pl.ds(base, m)
        y_ref[rows, :] = (x_ref[rows, :].astype(f32) + (zk[rows, :] + zr[rows, :])).astype(bf16)


def out_proj(o1, o2, x_loc, d, r, a_own, a_chip, wao, wmo):
    anyspec = pl.BlockSpec(memory_space=pltpu.HBM)
    vspec = pl.BlockSpec(memory_space=pltpu.VMEM)
    dma = pltpu.SemaphoreType.DMA
    two = dma((2,))
    return pl.pallas_call(
        out_proj_kernel,
        out_shape=jax.ShapeDtypeStruct((ROWS, LOC), bf16),
        in_specs=[anyspec] * 9,
        out_specs=vspec,
        scratch_shapes=[
            pltpu.VMEM((16, 4096), bf16),
            pltpu.VMEM((16, 4096), bf16),
            pltpu.VMEM((16, 4096), bf16),
            pltpu.VMEM((ROWS, LOC), bf16),
            pltpu.VMEM((2, ROWS, TILE), f32),
            pltpu.VMEM((2, ROWS, TILE), f32),
            pltpu.VMEM((2, 2048, LOC), bf16),
            pltpu.VMEM((2, 16, TILE, LOC), bf16),
            pltpu.VMEM((4, 4, ROWS, TILE), bf16),
            pltpu.VMEM((8, 16, 2048), bf16),
            pltpu.VMEM((ROWS, LOC), f32),
            pltpu.VMEM((ROWS, LOC), f32),
            pltpu.VMEM((ROWS, LOC), f32),
            two, dma, dma, dma, two, two, dma((2, 16)),
            two, two, two, two, dma, dma,
            dma, dma, two, two, two, two, two, two, dma((3,)), dma((3,)),
        ],
        compiler_params=pltpu.CompilerParams(
            collective_id=1, has_side_effects=True, vmem_limit_bytes=VMEM_LIMIT - OUT_ROOM),
        cost_estimate=pl.CostEstimate(flops=3_000_000_000, bytes_accessed=26_000_000, transcendentals=0),
        name="out_proj",
    )(o1, o2, x_loc, d, r, a_own, a_chip, wao, wmo)


def solution(mesh):
    both_axes = ("x", "yz")
    row_spec = P("dp", both_axes)
    in_w_spec = P("x", "yz")
    out_w_spec = P("yz", "x")
    cache_spec = P(("dp", "x", "yz"), None, None)
    len_spec = P(("dp", "x", "yz"))
    swap = [(0, 2), (2, 0), (1, 3), (3, 1)]

    def local_layer(x_loc, gain_loc, wqkv_loc, wgate_loc, wup_loc, wao_loc, wmo_loc, kc_loc, vc_loc, len_loc):
        qkv, sa, sb, r0, d, x_tall, lens = in_proj(x_loc, gain_loc, len_loc, wqkv_loc, wgate_loc, wup_loc)
        ra = lax.ppermute(sa, "x", swap)
        k_all, v_all, o1 = attend(0, SPLIT, lens, qkv, kc_loc, vc_loc)
        sb, o1 = lax.optimization_barrier((sb, o1))
        rb = lax.ppermute(sb, "x", swap)
        a_own, a_tall = act(d, r0, ra)
        a_chip = lax.ppermute(a_own, "x", swap)
        k_all, v_all, o2 = attend(SPLIT, 16, lens, qkv, kc_loc, vc_loc, k_all, v_all)
        y_loc = out_proj(o1, o2, x_tall, d, rb, a_tall, a_chip, wao_loc, wmo_loc)
        return y_loc, k_all, v_all

    in_specs = (row_spec, P(both_axes), in_w_spec, in_w_spec, in_w_spec, out_w_spec, out_w_spec, cache_spec, cache_spec, len_spec)
    out_specs = (row_spec, cache_spec, cache_spec)
    return jax.shard_map(local_layer, mesh=mesh, in_specs=in_specs, out_specs=out_specs, check_vma=False)
```

```python
import functools

import jax
import jax.numpy as jnp
from jax import lax
from jax.experimental import pallas as pl
from jax.experimental.pallas import tpu as pltpu
from jax.sharding import PartitionSpec as P

MESH = pl.DeviceIdType.MESH
VMEM_LIMIT = 67043328
ROWS = 128
HD = 256
LOC = 512
SUB = 16
HALF = 64
WIDE = 2048
ACT_LIMIT = 46 * 2 ** 20
TALL = 2 ** 23
OUT_ROOM = 11700000
TILE = 512
SA = 5
SPLIT = 10
NT = 8
QC = 768
NQ = 3
W_FIRST = 8
W_AHEAD = 12

f32 = jnp.float32
bf16 = jnp.bfloat16


def local_copy(src, dst, sem):
    return pltpu.make_async_copy(src, dst, sem)


def remote_copy(src, dst, ssem, rsem, dev):
    return pltpu.make_async_remote_copy(src, dst, ssem, rsem, device_id=dev, device_id_type=MESH)


def in_proj_kernel(x_hbm, g_hbm, len_hbm, wq_ref, wg_ref, wu_ref, qkv_ref, sa_ref, sb_ref, r0_ref, d_ref, xc_ref, lens_ref,
                   wqv, wv, x_ref, g_ref, len_s, lens, xr, gr, qout, st, stx, h, qp, qr, qxs, qxr, qf, qyr, sbuf, rbuf, obuf,
                   wqsem, wsem, xs_sem, xr_sem, gs_sem, gr_sem, sts_sem, str_sem,
                   qds_sem, qdr_sem, qxs_sem, qxr_sem, qys_sem, qyr_sem, ds_sem, dr_sem, out_sem, xin_sem, gin_sem, qo_sem, es_sem, er_sem, xc_sem, len_sem, lens_sem):
    d_model = 4096
    x = lax.axis_index("x")
    yz = lax.axis_index("yz")
    core = lax.rem(x, 2)
    x_core = x + 1 - 2 * core
    x_chip = lax.rem(x + 2, 4)
    x_diag = x_chip + 1 - 2 * core
    me = 2 * x + yz
    partner = {"x": x_core}
    xpeer = {"x": x_chip}
    ypeer = {"yz": 1 - yz}

    barrier = pltpu.get_barrier_semaphore()
    others = []
    for dx in range(4):
        for dy in range(2):
            if dx or dy:
                others.append((lax.rem(x + dx, 4), lax.rem(yz + dy, 2)))
    for ox, oy in others:
        pl.semaphore_signal(barrier, inc=1, device_id={"x": ox, "yz": oy}, device_id_type=MESH)
    x_in = local_copy(x_hbm, x_ref, xin_sem)
    g_in = local_copy(g_hbm, g_ref, gin_sem)
    x_in.start()
    g_in.start()
    len_in = local_copy(len_hbm, len_s, len_sem)
    len_in.start()

    def wq_copy(j):
        return local_copy(wq_ref.at[:, pl.ds(QC * j, QC)], wqv.at[j], wqsem.at[j])

    quarters = (x_diag, x_chip, x_core, x)

    def w_start(slot):
        phase = slot // NT
        q = quarters[0]
        for n in range(1, 4):
            q = jnp.where(phase == n, quarters[n], q)
        cols = pl.multiple_of(q * WIDE + (slot % NT) // 2 * TILE, TILE)

        def start(w_hbm):
            local_copy(w_hbm.at[:, pl.ds(cols, TILE)], wv.at[slot], wsem.at[slot]).start()

        if isinstance(slot, int):
            start(wg_ref if slot % 2 == 0 else wu_ref)
        else:
            pl.when(slot % 2 == 0)(lambda: start(wg_ref))
            pl.when(slot % 2 == 1)(lambda: start(wu_ref))

    def w_wait(slot):
        local_copy(wg_ref.at[:, pl.ds(0, TILE)], wv.at[slot], wsem.at[slot]).wait()

    x_in.wait()
    for j in range(NQ):
        wq_copy(j).start()
    for slot in range(W_FIRST):
        w_start(slot)
    g_in.wait()
    xf = x_ref[...].astype(f32)
    s1 = jnp.sum(xf, axis=1, keepdims=True)
    s2 = jnp.sum(xf * xf, axis=1, keepdims=True)
    lane = lax.broadcasted_iota(jnp.int32, (ROWS, ROWS), 1)
    stat = jnp.where(lane == 0, s1, s2).T
    st[me] = stat[0:8]

    pl.semaphore_wait(barrier, 7)

    x_send = remote_copy(x_ref, xr, xs_sem, xr_sem, ypeer)
    g_send = remote_copy(g_ref, gr, gs_sem, gr_sem, ypeer)
    for n, (ox, oy) in enumerate(others):
        remote_copy(st.at[me], stx.at[me], sts_sem.at[n], str_sem.at[me], {"x": ox, "yz": oy}).start()
    g_send.start()
    x_send.start()
    stx[me] = st[me]
    for n, (ox, oy) in enumerate(others):
        src = 2 * ox + oy
        remote_copy(st.at[me], stx.at[src], sts_sem.at[n], str_sem.at[src], {"x": ox, "yz": oy}).wait()
    tot = jnp.sum(stx[...], axis=0)
    tot = jnp.concatenate([tot, jnp.zeros((120, ROWS), f32)], axis=0).T
    mean = tot[:, 0:1] / d_model
    var = tot[:, 1:2] / d_model - mean * mean
    rstd = lax.rsqrt(var + 1e-6)
    own_cols = pl.multiple_of(yz * LOC, LOC)
    peer_cols = pl.multiple_of((1 - yz) * LOC, LOC)
    h[:, pl.ds(own_cols, LOC)] = ((xf - mean) * rstd * g_ref[...].astype(f32).reshape(1, LOC)).astype(bf16)
    x_send.wait()
    g_send.wait()
    h[:, pl.ds(peer_cols, LOC)] = ((xr[...].astype(f32) - mean) * rstd * gr[...].astype(f32).reshape(1, LOC)).astype(bf16)

    for slot in range(W_FIRST, W_AHEAD):
        w_start(slot)

    def q_compute(j):
        wq_copy(j).wait()
        part = jnp.dot(h[...], wqv[j], preferred_element_type=f32)
        qp[j] = part.reshape(4, 32, QC)

    def q_pair(j, k):
        block = (x_diag, x_core)[k]
        return remote_copy(qp.at[j, block], qr.at[j, k], qds_sem.at[j, k], qdr_sem.at[j, k], partner)

    def q_pair_start(j):
        q_pair(j, 0).start()
        q_pair(j, 1).start()

    def q_chip(j):
        return remote_copy(qxs.at[j], qxr.at[j], qxs_sem.at[j], qxr_sem.at[j], xpeer)

    def q_sum(j):
        q_pair(j, 0).wait()
        qxs[j] = qp[j, x_chip] + qr[j, 0]

    def tile(slot):
        w_wait(slot)
        if isinstance(slot, int):
            if slot + W_AHEAD < 4 * NT:
                w_start(slot + W_AHEAD)
        else:
            @pl.when(slot + W_AHEAD < 4 * NT)
            def _():
                w_start(slot + W_AHEAD)
        return jnp.dot(h[...], wv[slot], preferred_element_type=f32)

    def d_copy(i):
        return remote_copy(sbuf.at[i], rbuf.at[i], ds_sem.at[i], dr_sem.at[i], partner)

    def s_out(i):
        dst = sa_ref.at[i - 1] if i <= SA else sb_ref.at[i - 1 - SA]
        return local_copy(obuf.at[i], dst, out_sem.at[i])

    def d_out(i):
        return local_copy(obuf.at[NT + i], d_ref.at[i], out_sem.at[NT + i])

    early = remote_copy(obuf.at[0], r0_ref.at[0], es_sem, er_sem, xpeer)

    len_in.wait()
    row = lax.broadcasted_iota(jnp.int32, (SUB, ROWS), 0)
    rows = jnp.zeros((SUB, ROWS), jnp.int32)
    for r in range(SUB):
        rows = jnp.where(row == r, len_s[r], rows)
    lens[...] = rows

    q_compute(0)
    q_compute(1)
    q_pair_start(0)
    q_compute(2)
    q_pair_start(1)

    after = {
        0: lambda: q_pair_start(2),
        1: lambda: q_sum(0),
        2: lambda: (q_chip(0).start(), q_sum(1)),
        3: lambda: (q_chip(1).start(), q_sum(2)),
        4: lambda: q_chip(2).start(),
    }
    for i in range(NT):
        sbuf[i] = tile(i)
        if i:
            d_copy(i - 1).start()
        if i in after:
            after[i]()

    for i in range(NT):
        part = tile(NT + i)
        if i == 0:
            d_copy(NT - 1).start()
        d_copy(i).wait()
        obuf[i] = part + rbuf[i]
        if i == 1:
            early.start()
        elif i:
            s_out(i - 1).start()

    own_rows = pl.multiple_of(yz * SUB, SUB)
    peer_rows = pl.multiple_of((1 - yz) * SUB, SUB)

    def q_y(j):
        return remote_copy(qf.at[j, pl.ds(peer_rows, SUB)], qyr.at[j], qys_sem.at[j], qyr_sem.at[j], ypeer)

    def q_final(j):
        q_pair(j, 1).wait()
        q_chip(j).wait()
        qf[j] = (qp[j, x] + qr[j, 1] + qxr[j]).astype(bf16)
        qout[yz, :, pl.ds(QC * j, QC)] = qf[j, pl.ds(own_rows, SUB)]

    def send_tiles(lo, hi):
        def body(i, _):
            sbuf[NT + i] = tile(2 * NT + i)

            @pl.when(i == 0)
            def _():
                s_out(NT - 1).start()

            @pl.when(i > 0)
            def _():
                d_copy(NT + i - 1).start()
            return 0

        lax.fori_loop(lo, hi, body, 0)

    def keep_tiles(lo, hi):
        def body(i, _):
            part = tile(3 * NT + i)

            @pl.when(i == 0)
            def _():
                d_copy(2 * NT - 1).start()
            d_copy(NT + i).wait()
            obuf[NT + i] = part + rbuf[NT + i]

            @pl.when(i > 0)
            def _():
                d_out(i - 1).start()
            return 0

        lax.fori_loop(lo, hi, body, 0)

    send_tiles(0, 3)
    q_final(0)
    send_tiles(3, 4)
    q_y(0).start()
    send_tiles(4, 8)
    keep_tiles(0, 2)
    q_final(1)
    keep_tiles(2, 3)
    q_y(1).start()
    keep_tiles(3, 7)
    q_final(2)
    keep_tiles(7, 8)
    q_y(2).start()
    d_out(NT - 1).start()
    for j in range(NQ):
        q_y(j).wait()
        qout[1 - yz, :, pl.ds(QC * j, QC)] = qyr[j]
    q_out = local_copy(qout, qkv_ref.at[pl.ds(0, 2)], qo_sem)
    q_out.start()
    lens_out = local_copy(lens, lens_ref.at[pl.ds(0, SUB)], lens_sem)
    lens_out.start()
    x_out = local_copy(x_ref, xc_ref.at[pl.ds(0, ROWS)], xc_sem)
    x_out.start()
    for i in range(NT):
        if i:
            s_out(i).wait()
        d_out(i).wait()
    q_out.wait()
    x_out.wait()
    lens_out.wait()
    early.wait()


def in_proj(x_loc, gain, lens, wq, wg, wu):
    anyspec = pl.BlockSpec(memory_space=pltpu.HBM)
    dma = pltpu.SemaphoreType.DMA
    return pl.pallas_call(
        in_proj_kernel,
        out_shape=[
            jax.ShapeDtypeStruct((TALL // (SUB * NQ * QC), SUB, NQ * QC), bf16),
            jax.ShapeDtypeStruct((SA, ROWS, TILE), f32),
            jax.ShapeDtypeStruct((NT - 1 - SA, ROWS, TILE), f32),
            jax.ShapeDtypeStruct((1, ROWS, TILE), f32),
            jax.ShapeDtypeStruct((NT, ROWS, TILE), f32),
            jax.ShapeDtypeStruct((TALL // LOC, LOC), bf16),
            jax.ShapeDtypeStruct((TALL // ROWS, ROWS), jnp.int32),
        ],
        in_specs=[anyspec] * 6,
        out_specs=[anyspec] * 7,
        scratch_shapes=[
            pltpu.VMEM((NQ, 1024, QC), bf16),
            pltpu.VMEM((4 * NT, 1024, TILE), bf16),
            pltpu.VMEM((ROWS, LOC), bf16),
            pltpu.VMEM((LOC,), bf16),
            pltpu.SMEM((SUB,), jnp.int32),
            pltpu.VMEM((SUB, ROWS), jnp.int32),
            pltpu.VMEM((ROWS, LOC), bf16),
            pltpu.VMEM((LOC,), bf16),
            pltpu.VMEM((2, SUB, NQ * QC), bf16),
            pltpu.VMEM((8, 8, ROWS), f32),
            pltpu.VMEM((8, 8, ROWS), f32),
            pltpu.VMEM((ROWS, 1024), bf16),
            pltpu.VMEM((NQ, 4, 32, QC), f32),
            pltpu.VMEM((NQ, 2, 32, QC), f32),
            pltpu.VMEM((NQ, 32, QC), f32),
            pltpu.VMEM((NQ, 32, QC), f32),
            pltpu.VMEM((NQ, 32, QC), bf16),
            pltpu.VMEM((NQ, SUB, QC), bf16),
            pltpu.VMEM((2 * NT, ROWS, TILE), f32),
            pltpu.VMEM((2 * NT, ROWS, TILE), f32),
            pltpu.VMEM((2 * NT, ROWS, TILE), f32),
            dma((NQ,)), dma((4 * NT,)), dma, dma, dma, dma, dma((7,)), dma((8,)),
            dma((NQ, 2)), dma((NQ, 2)), dma((NQ,)), dma((NQ,)), dma((NQ,)), dma((NQ,)),
            dma((2 * NT,)), dma((2 * NT,)), dma((2 * NT,)), dma, dma, dma, dma, dma, dma, dma, dma,
        ],
        compiler_params=pltpu.CompilerParams(
            collective_id=0, has_side_effects=True, vmem_limit_bytes=VMEM_LIMIT),
        cost_estimate=pl.CostEstimate(flops=5_000_000_000, bytes_accessed=45_000_000, transcendentals=0),
        name="in_proj",
    )(x_loc, gain, lens, wq, wg, wu)


SLOTS = 6


def attend_kernel(lo, hi, len_hbm, qkv_hbm, k_ref, v_ref, *refs):
    if lo:
        refs = refs[2:]
    (ko_ref, vo_ref, o_hbm, o_ref, kb, vb, len_ref, lens, qkv_ref, qs, kns, vns, osc,
     ksem, vsem, kosem, vosem, isem, osem) = refs
    t_len = k_ref.shape[1]

    def k_in(r, s):
        return local_copy(k_ref.at[r], kb.at[s], ksem.at[s])

    def v_in(r, s):
        return local_copy(v_ref.at[r], vb.at[s], vsem.at[s])

    def k_out(r, s):
        return local_copy(kb.at[s], ko_ref.at[r], kosem.at[s])

    def v_out(r, s):
        return local_copy(vb.at[s], vo_ref.at[r], vosem.at[s])

    AHEAD = 4
    len_in = local_copy(len_hbm.at[pl.ds(0, SUB)], len_ref, isem.at[0])
    lens_in = local_copy(len_hbm.at[pl.ds(0, SUB)], lens, isem.at[2])
    lens_in.start()
    qkv_in = local_copy(qkv_hbm.at[pl.ds(0, 2)], qkv_ref, isem.at[1])
    len_in.start()
    qkv_in.start()
    for r in range(lo, lo + 2):
        k_in(r, r % SLOTS).start()
        v_in(r, r % SLOTS).start()
    len_in.wait()
    lens_in.wait()
    qkv_in.wait()
    for r in range(lo + 2, lo + AHEAD):
        k_in(r, r % SLOTS).start()
        v_in(r, r % SLOTS).start()
    half = lax.broadcasted_iota(jnp.int32, (SUB, ROWS), 1).astype(f32)
    angles = lens[...].astype(f32) * 10000.0 ** (-half / ROWS)
    cos_t = jnp.cos(angles)
    sin_t = jnp.sin(angles)
    for g in range(17):
        part, base = (0, g * HD) if g < 9 else (1, (g - 9) * HD)
        a = qkv_ref[part, :, base:base + ROWS].astype(f32)
        b = qkv_ref[part, :, base + ROWS:base + HD].astype(f32)
        lower = (a * cos_t - b * sin_t).astype(bf16).astype(f32)
        upper = (b * cos_t + a * sin_t).astype(bf16).astype(f32)
        if g < SUB:
            qs[:, g, 0:ROWS] = lower
            qs[:, g, ROWS:HD] = upper
        else:
            kns[:, 0:ROWS] = lower
            kns[:, ROWS:HD] = upper
    vns[...] = qkv_ref[1, :, WIDE:2304].astype(f32)

    row16 = lax.broadcasted_iota(jnp.int32, (SUB, HD), 0)
    pos = lax.broadcasted_iota(jnp.int32, (SUB, t_len), 1)

    def body(r, _):
        s = lax.rem(r, SLOTS)
        nxt = r + AHEAD

        @pl.when(nxt < hi)
        def _():
            s2 = lax.rem(nxt, SLOTS)

            @pl.when(nxt - SLOTS >= lo)
            def _():
                k_out(nxt - SLOTS, s2).wait()
                v_out(nxt - SLOTS, s2).wait()
            k_in(nxt, s2).start()
            v_in(nxt, s2).start()

        p = len_ref[r, 0]
        base = pl.multiple_of((p // SUB) * SUB, SUB)
        hit = row16 == p - base
        k_in(r, s).wait()
        krow = kb[s, pl.ds(base, SUB), :]
        kb[s, pl.ds(base, SUB), :] = jnp.where(hit, kns[pl.ds(r, 1), :].astype(bf16), krow)
        v_in(r, s).wait()
        vrow = vb[s, pl.ds(base, SUB), :]
        vb[s, pl.ds(base, SUB), :] = jnp.where(hit, vns[pl.ds(r, 1), :].astype(bf16), vrow)
        q = qs[r].astype(bf16)
        sc = lax.dot_general(q, kb[s], (((1,), (1,)), ((), ())), preferred_element_type=f32) * (HD ** -0.5)
        k_out(r, s).start()
        v_out(r, s).start()
        sc = jnp.where(pos <= p, sc, -1e30)
        m = jnp.max(sc, axis=1, keepdims=True)
        e = jnp.exp(sc - m)
        den = jnp.sum(e, axis=1, keepdims=True)
        pr = (e / den).astype(bf16)
        osc[r] = jnp.dot(pr, vb[s], preferred_element_type=f32).astype(bf16).astype(f32)
        return 0

    lax.fori_loop(lo, hi, body, 0)
    for g in range(SUB):
        o_ref[:, HD * g:HD * (g + 1)] = osc[:, g, :].astype(bf16)
    o_out = local_copy(o_ref, o_hbm.at[pl.ds(0, SUB)], osem)
    o_out.start()
    for r in range(max(lo, hi - SLOTS), hi):
        k_out(r, r % SLOTS).wait()
        v_out(r, r % SLOTS).wait()
    o_out.wait()


def attend(lo, hi, lens, qkv, kc, vc, *prev):
    anyspec = pl.BlockSpec(memory_space=pltpu.HBM)
    dma = pltpu.SemaphoreType.DMA
    n, t_len, hd = kc.shape
    return pl.pallas_call(
        functools.partial(attend_kernel, lo, hi),
        out_shape=[
            jax.ShapeDtypeStruct(kc.shape, bf16),
            jax.ShapeDtypeStruct(vc.shape, bf16),
            jax.ShapeDtypeStruct((TALL // 4096, 4096), bf16),
        ],
        in_specs=[anyspec] * (4 + len(prev)),
        out_specs=[anyspec] * 3,
        input_output_aliases={4: 0, 5: 1} if prev else {},
        scratch_shapes=[
            pltpu.VMEM((n, 4096), bf16),
            pltpu.VMEM((SLOTS, t_len, hd), bf16),
            pltpu.VMEM((SLOTS, t_len, hd), bf16),
            pltpu.SMEM((n, ROWS), jnp.int32),
            pltpu.VMEM((n, ROWS), jnp.int32),
            pltpu.VMEM((2, SUB, NQ * QC), bf16),
            pltpu.VMEM((n, SUB, hd), f32),
            pltpu.VMEM((n, hd), f32),
            pltpu.VMEM((n, hd), f32),
            pltpu.VMEM((n, SUB, hd), f32),
            dma((SLOTS,)), dma((SLOTS,)), dma((SLOTS,)), dma((SLOTS,)), dma((3,)), dma,
        ],
        compiler_params=pltpu.CompilerParams(vmem_limit_bytes=VMEM_LIMIT if lo else 44 * 2 ** 20),
        cost_estimate=pl.CostEstimate(flops=2_500_000_000 * (hi - lo), bytes_accessed=8_400_000 * (hi - lo), transcendentals=1_000_000),
        name=f"attend{lo}",
    )(lens, qkv, kc, vc, *prev)


NA = 3


def act_kernel(d_ref, r0_ref, r_ref, a_hbm, at_hbm, a_ref, asem, tsem):
    def a_out(t):
        return local_copy(a_ref.at[t], a_hbm.at[t], asem.at[t])

    tall = local_copy(a_ref, at_hbm.at[pl.ds(0, NA)], tsem)

    def total(i):
        other = r_ref[i - 1] if i else r0_ref[0]
        return (d_ref[i] + other).astype(bf16).astype(f32)

    for t in range(NA):
        a_ref[t] = (jax.nn.silu(total(2 * t)) * total(2 * t + 1)).astype(bf16)
        if t:
            a_out(t - 1).start()
    a_out(NA - 1).start()
    tall.start()
    for t in range(NA):
        a_out(t).wait()
    tall.wait()


def act(d, r0, r):
    anyspec = pl.BlockSpec(memory_space=pltpu.HBM)
    dma = pltpu.SemaphoreType.DMA
    return pl.pallas_call(
        act_kernel,
        out_shape=[
            jax.ShapeDtypeStruct((NA, ROWS, TILE), bf16),
            jax.ShapeDtypeStruct((TALL // (ROWS * TILE), ROWS, TILE), bf16),
        ],
        in_specs=[pl.BlockSpec(memory_space=pltpu.VMEM)] * 3,
        out_specs=[anyspec] * 2,
        scratch_shapes=[
            pltpu.VMEM((NA, ROWS, TILE), bf16),
            dma((NA,)), dma,
        ],
        compiler_params=pltpu.CompilerParams(vmem_limit_bytes=ACT_LIMIT),
        cost_estimate=pl.CostEstimate(flops=5_000_000, bytes_accessed=4_000_000, transcendentals=200_000),
        name="act",
    )(d, r0, r)


def out_proj_kernel(o1_hbm, o2_hbm, x_hbm, d_ref, r_ref, ao_ref, ax_ref, wao_ref, wmo_ref, y_ref,
                    o1_ref, o2_ref, o_ref, x_ref, db, rb, wao, wmo, ab, ob, zs, zk, zr,
                    osem, xsem, dsem, rsem, asem, waosem, wmosem, pss, psr, fss, fsr, e_s, e_r,
                    o0s, o0r, o1s, o1r, o2s, o2r, o3s, o3r, zss, zrs):
    x = lax.axis_index("x")
    yz = lax.axis_index("yz")
    core = lax.rem(x, 2)
    x_core = x + 1 - 2 * core
    x_chip = lax.rem(x + 2, 4)
    x_diag = x_chip + 1 - 2 * core
    partner = {"x": x_core}
    xpeer = {"x": x_chip}
    ypeer = {"yz": 1 - yz}

    barrier = pltpu.get_barrier_semaphore()
    for dev in (partner, xpeer, ypeer):
        pl.semaphore_signal(barrier, inc=1, device_id=dev, device_id_type=MESH)

    top = pl.ds(0, SUB)
    o_in = [local_copy(o1_hbm.at[top], o1_ref, osem.at[0]), local_copy(o2_hbm.at[top], o2_ref, osem.at[1])]
    for c in o_in:
        c.start()
    first = pl.ds(0, NA)
    own_in = local_copy(ao_ref.at[first], ab.at[x, first], asem.at[0])
    chip_in = local_copy(ax_ref, ab.at[x_chip, first], asem.at[1])
    own_in.start()
    chip_in.start()
    loads = [local_copy(d_ref.at[pl.ds(2 * NA, 2)], db, dsem), local_copy(r_ref, rb, rsem)]
    for c in loads:
        c.start()
    for c in o_in:
        c.wait()
    x_in = local_copy(x_hbm.at[pl.ds(0, ROWS)], x_ref, xsem)
    x_in.start()

    order = (x, x_chip, x_core, x_diag)

    halves = (pl.ds(pl.multiple_of((1 - yz) * LOC, LOC), LOC), pl.ds(pl.multiple_of(yz * LOC, LOC), LOC))
    accs = (zs, zk)

    def wmo_in(half, n, t):
        rows = pl.multiple_of(order[n] * WIDE + t * TILE, TILE)
        k = 4 * n + t
        return local_copy(wmo_ref.at[pl.ds(rows, TILE), halves[half]], wmo.at[half, k], wmosem.at[half, k])

    def wao_in(half):
        return local_copy(wao_ref.at[:, halves[half]], wao.at[half], waosem.at[half])

    def wmo_start(half, n):
        for t in range(4):
            wmo_in(half, n, t).start()

    wmo_start(0, 0)
    row = lax.broadcasted_iota(jnp.int32, (SUB, 4096), 0)
    o_ref[...] = jnp.where(row < SPLIT, o1_ref[...].astype(f32), o2_ref[...].astype(f32)).astype(bf16)
    own_half = pl.multiple_of(yz * WIDE, WIDE)
    peer_half = pl.multiple_of((1 - yz) * WIDE, WIDE)
    mine = 2 * x + yz
    theirs = 2 * x + 1 - yz
    ob[mine] = o_ref[:, pl.ds(own_half, WIDE)]

    for c in loads:
        c.wait()
    gate = (db[0] + rb[0]).astype(bf16).astype(f32)
    up = (db[1] + rb[1]).astype(bf16).astype(f32)
    ab[x, NA] = (jax.nn.silu(gate) * up).astype(bf16)
    pl.semaphore_wait(barrier, 3)

    o_y = remote_copy(o_ref.at[:, pl.ds(peer_half, WIDE)], ob.at[mine], o0s, o0r, ypeer)

    def o_hop(k, ss, rs, dev, owner):
        block = ob.at[2 * owner + (yz if k == 0 else 1 - yz)]
        return remote_copy(block, block, ss.at[k], rs.at[k], dev)

    o_part = [o_hop(k, o1s, o1r, partner, x) for k in range(2)]
    o_chip = [o_hop(k, o2s, o2r, xpeer, x) for k in range(2)]
    o_fwd = [o_hop(k, o3s, o3r, partner, x_chip) for k in range(2)]

    def a_hop(owner, tiles, ss, rs, k, dev):
        block = ab.at[owner, tiles]
        return remote_copy(block, block, ss.at[k], rs.at[k], dev)

    chip = x // 2
    own_rows = pl.multiple_of(HALF * chip, HALF)
    peer_rows = pl.multiple_of(HALF - HALF * chip, HALF)

    def last_hop(owner, base, ss, rs, k, dev):
        block = ab.at[owner, NA, pl.ds(base, HALF)]
        return remote_copy(block, block, ss.at[k], rs.at[k], dev)

    last = pl.ds(NA, 1)
    a_part = [a_hop(x, first, pss, psr, 0, partner), a_hop(x, last, pss, psr, 1, partner)]
    a_fwd = [a_hop(x_chip, first, fss, fsr, 0, partner)]
    a_chip = [last_hop(x, peer_rows, e_s, e_r, 0, xpeer), last_hop(x, own_rows, e_s, e_r, 1, xpeer)]
    a_fwd += [last_hop(x_chip, own_rows, fss, fsr, 1, partner), last_hop(x_chip, peer_rows, fss, fsr, 2, partner)]

    o_y.start()
    for c in a_chip:
        c.start()
    o_chip[0].start()
    o_part[0].start()
    a_part[1].start()
    own_in.wait()
    a_part[0].start()
    chip_in.wait()
    a_fwd[0].start()
    wmo_start(0, 1)
    wmo_start(0, 2)
    wao_in(0).start()
    wmo_start(0, 3)

    def mlp(half, n, t, init=False):
        wmo_in(half, n, t).wait()
        acc = accs[half]
        part = jnp.dot(ab[order[n], t], wmo[half, 4 * n + t], preferred_element_type=f32)
        acc[...] = part if init else acc[...] + part

    chip_rows = pl.multiple_of(32 * x_chip, 32)
    diag_rows = pl.multiple_of(32 * x_diag, 32)

    def z_y(c, base, m):
        rows = pl.ds(base, m)
        return remote_copy(zs.at[rows], zr.at[rows], zss.at[c], zrs.at[c], ypeer)

    def attn_rows(half, base, m):
        rows = pl.ds(base, m)
        attn = ob[pl.ds(base // SUB, m // SUB)].reshape(m, WIDE)
        accs[half][rows] += jnp.dot(attn, wao[half], preferred_element_type=f32)

    def mlp_rows(n, base):
        rows = pl.ds(base, HALF)
        zs[rows] += jnp.dot(ab[order[n], NA, rows], wmo[0, 4 * n + NA], preferred_element_type=f32)

    blocks = ((own_rows, HALF), (chip_rows, 32), (diag_rows, 32))
    for t in range(4):
        mlp(0, 0, t, init=t == 0)
    o_y.wait()
    o_chip[1].start()
    o_part[1].start()
    wmo_start(1, 0)
    wmo_start(1, 1)
    for t in range(NA):
        mlp(0, 1, t)
    a_part[0].wait()
    for t in range(NA):
        mlp(0, 2, t)
    a_chip[0].wait()
    a_fwd[1].start()
    a_part[1].wait()
    mlp(0, 2, NA)
    wmo_in(0, 1, NA).wait()
    mlp_rows(1, own_rows)
    wao_in(0).wait()
    for k in range(2):
        o_part[k].wait()
    attn_rows(0, *blocks[0])
    a_fwd[0].wait()
    for t in range(NA):
        mlp(0, 3, t)
    wmo_in(0, 3, NA).wait()
    a_fwd[1].wait()
    mlp_rows(3, own_rows)
    wmo_start(1, 2)
    wmo_start(1, 3)
    wao_in(1).start()
    a_chip[1].wait()
    a_fwd[2].start()
    mlp_rows(1, peer_rows)
    z_y(0, *blocks[0]).start()
    o_chip[0].wait()
    o_fwd[0].start()
    mlp(1, 0, 0, init=True)
    a_fwd[2].wait()
    mlp_rows(3, peer_rows)
    o_chip[1].wait()
    o_fwd[1].start()
    attn_rows(0, *blocks[1])
    mlp(1, 0, 1)
    z_y(1, *blocks[1]).start()
    for k in range(2):
        o_fwd[k].wait()
    attn_rows(0, *blocks[2])
    mlp(1, 0, 2)
    z_y(2, *blocks[2]).start()
    mlp(1, 0, NA)
    for n in range(1, 4):
        for t in range(4):
            mlp(1, n, t)
    wao_in(1).wait()
    attn_rows(1, 0, ROWS)
    x_in.wait()
    for c, (base, m) in enumerate(blocks):
        z_y(c, base, m).wait()
        rows = pl.ds(base, m)
        y_ref[rows, :] = (x_ref[rows, :].astype(f32) + (zk[rows, :] + zr[rows, :])).astype(bf16)


def out_proj(o1, o2, x_loc, d, r, a_own, a_chip, wao, wmo):
    anyspec = pl.BlockSpec(memory_space=pltpu.HBM)
    vspec = pl.BlockSpec(memory_space=pltpu.VMEM)
    dma = pltpu.SemaphoreType.DMA
    two = dma((2,))
    return pl.pallas_call(
        out_proj_kernel,
        out_shape=jax.ShapeDtypeStruct((ROWS, LOC), bf16),
        in_specs=[anyspec] * 9,
        out_specs=vspec,
        scratch_shapes=[
            pltpu.VMEM((SUB, 4096), bf16),
            pltpu.VMEM((SUB, 4096), bf16),
            pltpu.VMEM((SUB, 4096), bf16),
            pltpu.VMEM((ROWS, LOC), bf16),
            pltpu.VMEM((2, ROWS, TILE), f32),
            pltpu.VMEM((2, ROWS, TILE), f32),
            pltpu.VMEM((2, WIDE, LOC), bf16),
            pltpu.VMEM((2, SUB, TILE, LOC), bf16),
            pltpu.VMEM((4, 4, ROWS, TILE), bf16),
            pltpu.VMEM((8, SUB, WIDE), bf16),
            pltpu.VMEM((ROWS, LOC), f32),
            pltpu.VMEM((ROWS, LOC), f32),
            pltpu.VMEM((ROWS, LOC), f32),
            two, dma, dma, dma, two, two, dma((2, SUB)),
            two, two, dma((3,)), dma((3,)), two, two,
            dma, dma, two, two, two, two, two, two, dma((3,)), dma((3,)),
        ],
        compiler_params=pltpu.CompilerParams(
            collective_id=1, has_side_effects=True, vmem_limit_bytes=VMEM_LIMIT - OUT_ROOM),
        cost_estimate=pl.CostEstimate(flops=3_000_000_000, bytes_accessed=26_000_000, transcendentals=0),
        name="out_proj",
    )(o1, o2, x_loc, d, r, a_own, a_chip, wao, wmo)


def solution(mesh):
    both_axes = ("x", "yz")
    row_spec = P("dp", both_axes)
    in_w_spec = P("x", "yz")
    out_w_spec = P("yz", "x")
    cache_spec = P(("dp", "x", "yz"), None, None)
    len_spec = P(("dp", "x", "yz"))
    swap = [(0, 2), (2, 0), (1, 3), (3, 1)]

    def local_layer(x_loc, gain_loc, wqkv_loc, wgate_loc, wup_loc, wao_loc, wmo_loc, kc_loc, vc_loc, len_loc):
        qkv, sa, sb, r0, d, x_tall, lens = in_proj(x_loc, gain_loc, len_loc, wqkv_loc, wgate_loc, wup_loc)
        ra = lax.ppermute(sa, "x", swap)
        k_all, v_all, o1 = attend(0, SPLIT, lens, qkv, kc_loc, vc_loc)
        sb, o1 = lax.optimization_barrier((sb, o1))
        rb = lax.ppermute(sb, "x", swap)
        a_own, a_tall = act(d, r0, ra)
        a_chip = lax.ppermute(a_own, "x", swap)
        k_all, v_all, o2 = attend(SPLIT, SUB, lens, qkv, kc_loc, vc_loc, k_all, v_all)
        y_loc = out_proj(o1, o2, x_tall, d, rb, a_tall, a_chip, wao_loc, wmo_loc)
        return y_loc, k_all, v_all

    in_specs = (row_spec, P(both_axes), in_w_spec, in_w_spec, in_w_spec, out_w_spec, out_w_spec, cache_spec, cache_spec, len_spec)
    out_specs = (row_spec, cache_spec, cache_spec)
    return jax.shard_map(local_layer, mesh=mesh, in_specs=in_specs, out_specs=out_specs, check_vma=False)
```

```python
import functools

import jax
import jax.numpy as jnp
from jax import lax
from jax.experimental import pallas as pl
from jax.experimental.pallas import tpu as pltpu
from jax.sharding import PartitionSpec as P

MESH = pl.DeviceIdType.MESH
VMEM_LIMIT = 67043328
ROWS = 128
HD = 256
LOC = 512
SUB = 16
HALF = 64
WIDE = 2048
ACT_LIMIT = 46 * 2 ** 20
TALL = 2 ** 23
OUT_ROOM = 11700000
TILE = 512
SA = 5
SPLIT = 10
NT = 8
QC = 384
NQ = 6
W_FIRST = 8
W_AHEAD = 12

f32 = jnp.float32
bf16 = jnp.bfloat16


def local_copy(src, dst, sem):
    return pltpu.make_async_copy(src, dst, sem)


def remote_copy(src, dst, ssem, rsem, dev):
    return pltpu.make_async_remote_copy(src, dst, ssem, rsem, device_id=dev, device_id_type=MESH)


def in_proj_kernel(x_hbm, g_hbm, len_hbm, wq_ref, wg_ref, wu_ref, qkv_ref, sa_ref, sb_ref, r0_ref, d_ref, xc_ref, lens_ref,
                   wqv, wv, x_ref, g_ref, len_s, lens, xr, gr, qout, st, stx, h, qp, qr, qxs, qxr, qf, qyr, sbuf, rbuf, obuf,
                   wqsem, wsem, xs_sem, xr_sem, gs_sem, gr_sem, sts_sem, str_sem,
                   qds_sem, qdr_sem, qxs_sem, qxr_sem, qys_sem, qyr_sem, ds_sem, dr_sem, out_sem, xin_sem, gin_sem, qo_sem, es_sem, er_sem, xc_sem, len_sem, lens_sem):
    d_model = 4096
    x = lax.axis_index("x")
    yz = lax.axis_index("yz")
    core = lax.rem(x, 2)
    x_core = x + 1 - 2 * core
    x_chip = lax.rem(x + 2, 4)
    x_diag = x_chip + 1 - 2 * core
    me = 2 * x + yz
    partner = {"x": x_core}
    xpeer = {"x": x_chip}
    ypeer = {"yz": 1 - yz}

    barrier = pltpu.get_barrier_semaphore()
    others = []
    for dx in range(4):
        for dy in range(2):
            if dx or dy:
                others.append((lax.rem(x + dx, 4), lax.rem(yz + dy, 2)))
    for ox, oy in others:
        pl.semaphore_signal(barrier, inc=1, device_id={"x": ox, "yz": oy}, device_id_type=MESH)
    x_in = local_copy(x_hbm, x_ref, xin_sem)
    g_in = local_copy(g_hbm, g_ref, gin_sem)
    x_in.start()
    g_in.start()
    len_in = local_copy(len_hbm, len_s, len_sem)
    len_in.start()

    def wq_copy(j):
        return local_copy(wq_ref.at[:, pl.ds(QC * j, QC)], wqv.at[j], wqsem.at[j])

    quarters = (x_diag, x_chip, x_core, x)

    def w_start(slot):
        phase = slot // NT
        q = quarters[0]
        for n in range(1, 4):
            q = jnp.where(phase == n, quarters[n], q)
        cols = pl.multiple_of(q * WIDE + (slot % NT) // 2 * TILE, TILE)

        def start(w_hbm):
            local_copy(w_hbm.at[:, pl.ds(cols, TILE)], wv.at[slot], wsem.at[slot]).start()

        if isinstance(slot, int):
            start(wg_ref if slot % 2 == 0 else wu_ref)
        else:
            pl.when(slot % 2 == 0)(lambda: start(wg_ref))
            pl.when(slot % 2 == 1)(lambda: start(wu_ref))

    def w_wait(slot):
        local_copy(wg_ref.at[:, pl.ds(0, TILE)], wv.at[slot], wsem.at[slot]).wait()

    x_in.wait()
    for j in range(NQ):
        wq_copy(j).start()
    for slot in range(W_FIRST):
        w_start(slot)
    g_in.wait()
    xf = x_ref[...].astype(f32)
    s1 = jnp.sum(xf, axis=1, keepdims=True)
    s2 = jnp.sum(xf * xf, axis=1, keepdims=True)
    lane = lax.broadcasted_iota(jnp.int32, (ROWS, ROWS), 1)
    stat = jnp.where(lane == 0, s1, s2).T
    st[me] = stat[0:8]

    pl.semaphore_wait(barrier, 7)

    x_send = remote_copy(x_ref, xr, xs_sem, xr_sem, ypeer)
    g_send = remote_copy(g_ref, gr, gs_sem, gr_sem, ypeer)
    for n, (ox, oy) in enumerate(others):
        remote_copy(st.at[me], stx.at[me], sts_sem.at[n], str_sem.at[me], {"x": ox, "yz": oy}).start()
    g_send.start()
    x_send.start()
    stx[me] = st[me]
    for n, (ox, oy) in enumerate(others):
        src = 2 * ox + oy
        remote_copy(st.at[me], stx.at[src], sts_sem.at[n], str_sem.at[src], {"x": ox, "yz": oy}).wait()
    tot = jnp.sum(stx[...], axis=0)
    tot = jnp.concatenate([tot, jnp.zeros((120, ROWS), f32)], axis=0).T
    mean = tot[:, 0:1] / d_model
    var = tot[:, 1:2] / d_model - mean * mean
    rstd = lax.rsqrt(var + 1e-6)
    own_cols = pl.multiple_of(yz * LOC, LOC)
    peer_cols = pl.multiple_of((1 - yz) * LOC, LOC)
    h[:, pl.ds(own_cols, LOC)] = ((xf - mean) * rstd * g_ref[...].astype(f32).reshape(1, LOC)).astype(bf16)
    x_send.wait()
    g_send.wait()
    h[:, pl.ds(peer_cols, LOC)] = ((xr[...].astype(f32) - mean) * rstd * gr[...].astype(f32).reshape(1, LOC)).astype(bf16)

    for slot in range(W_FIRST, W_AHEAD):
        w_start(slot)

    def q_compute(j):
        wq_copy(j).wait()
        part = jnp.dot(h[...], wqv[j], preferred_element_type=f32)
        qp[j] = part.reshape(4, 32, QC)

    def q_pair(j, k):
        block = (x_diag, x_core)[k]
        return remote_copy(qp.at[j, block], qr.at[j, k], qds_sem.at[j, k], qdr_sem.at[j, k], partner)

    def q_pair_start(j):
        q_pair(j, 0).start()
        q_pair(j, 1).start()

    def q_chip(j):
        return remote_copy(qxs.at[j], qxr.at[j], qxs_sem.at[j], qxr_sem.at[j], xpeer)

    def q_sum(j):
        q_pair(j, 0).wait()
        qxs[j] = qp[j, x_chip] + qr[j, 0]

    def tile(slot):
        w_wait(slot)
        if isinstance(slot, int):
            if slot + W_AHEAD < 4 * NT:
                w_start(slot + W_AHEAD)
        else:
            @pl.when(slot + W_AHEAD < 4 * NT)
            def _():
                w_start(slot + W_AHEAD)
        return jnp.dot(h[...], wv[slot], preferred_element_type=f32)

    def d_copy(i):
        return remote_copy(sbuf.at[i], rbuf.at[i], ds_sem.at[i], dr_sem.at[i], partner)

    def s_out(i):
        dst = sa_ref.at[i - 1] if i <= SA else sb_ref.at[i - 1 - SA]
        return local_copy(obuf.at[i], dst, out_sem.at[i])

    def d_out(i):
        return local_copy(obuf.at[NT + i], d_ref.at[i], out_sem.at[NT + i])

    early = remote_copy(obuf.at[0], r0_ref.at[0], es_sem, er_sem, xpeer)

    len_in.wait()
    row = lax.broadcasted_iota(jnp.int32, (SUB, ROWS), 0)
    rows = jnp.zeros((SUB, ROWS), jnp.int32)
    for r in range(SUB):
        rows = jnp.where(row == r, len_s[r], rows)
    lens[...] = rows

    for j in range(NQ):
        q_compute(j)
        if j:
            q_pair_start(j - 1)
    q_sum(0)

    after = {
        0: lambda: (q_pair_start(NQ - 1), q_chip(0).start(), q_sum(1)),
        1: lambda: (q_chip(1).start(), q_sum(2), q_sum(3)),
        2: lambda: (q_chip(2).start(), q_chip(3).start(), q_sum(4)),
        3: lambda: (q_chip(4).start(), q_sum(5)),
        4: lambda: q_chip(5).start(),
    }
    for i in range(NT):
        sbuf[i] = tile(i)
        if i:
            d_copy(i - 1).start()
        if i in after:
            after[i]()

    for i in range(NT):
        part = tile(NT + i)
        if i == 0:
            d_copy(NT - 1).start()
        d_copy(i).wait()
        obuf[i] = part + rbuf[i]
        if i == 1:
            early.start()
        elif i:
            s_out(i - 1).start()

    own_rows = pl.multiple_of(yz * SUB, SUB)
    peer_rows = pl.multiple_of((1 - yz) * SUB, SUB)

    def q_y(j):
        return remote_copy(qf.at[j, pl.ds(peer_rows, SUB)], qyr.at[j], qys_sem.at[j], qyr_sem.at[j], ypeer)

    def q_final(j):
        q_pair(j, 1).wait()
        q_chip(j).wait()
        qf[j] = (qp[j, x] + qr[j, 1] + qxr[j]).astype(bf16)
        qout[yz, :, pl.ds(QC * j, QC)] = qf[j, pl.ds(own_rows, SUB)]

    def send_tiles(lo, hi):
        def body(i, _):
            sbuf[NT + i] = tile(2 * NT + i)

            @pl.when(i == 0)
            def _():
                s_out(NT - 1).start()

            @pl.when(i > 0)
            def _():
                d_copy(NT + i - 1).start()
            return 0

        lax.fori_loop(lo, hi, body, 0)

    def keep_tiles(lo, hi):
        def body(i, _):
            part = tile(3 * NT + i)

            @pl.when(i == 0)
            def _():
                d_copy(2 * NT - 1).start()
            d_copy(NT + i).wait()
            obuf[NT + i] = part + rbuf[NT + i]

            @pl.when(i > 0)
            def _():
                d_out(i - 1).start()
            return 0

        lax.fori_loop(lo, hi, body, 0)

    send_tiles(0, 3)
    for j in range(3):
        q_final(j)
    send_tiles(3, 4)
    for j in range(3):
        q_y(j).start()
    send_tiles(4, 8)
    q_final(3)
    q_final(4)
    keep_tiles(0, 2)
    q_y(3).start()
    q_y(4).start()
    q_final(5)
    keep_tiles(2, 3)
    q_y(5).start()
    keep_tiles(3, 8)
    d_out(NT - 1).start()
    for j in range(NQ):
        q_y(j).wait()
        qout[1 - yz, :, pl.ds(QC * j, QC)] = qyr[j]
    q_out = local_copy(qout, qkv_ref.at[pl.ds(0, 2)], qo_sem)
    q_out.start()
    lens_out = local_copy(lens, lens_ref.at[pl.ds(0, SUB)], lens_sem)
    lens_out.start()
    x_out = local_copy(x_ref, xc_ref.at[pl.ds(0, ROWS)], xc_sem)
    x_out.start()
    for i in range(NT):
        if i:
            s_out(i).wait()
        d_out(i).wait()
    q_out.wait()
    x_out.wait()
    lens_out.wait()
    early.wait()


def in_proj(x_loc, gain, lens, wq, wg, wu):
    anyspec = pl.BlockSpec(memory_space=pltpu.HBM)
    dma = pltpu.SemaphoreType.DMA
    return pl.pallas_call(
        in_proj_kernel,
        out_shape=[
            jax.ShapeDtypeStruct((TALL // (SUB * NQ * QC), SUB, NQ * QC), bf16),
            jax.ShapeDtypeStruct((SA, ROWS, TILE), f32),
            jax.ShapeDtypeStruct((NT - 1 - SA, ROWS, TILE), f32),
            jax.ShapeDtypeStruct((1, ROWS, TILE), f32),
            jax.ShapeDtypeStruct((NT, ROWS, TILE), f32),
            jax.ShapeDtypeStruct((TALL // LOC, LOC), bf16),
            jax.ShapeDtypeStruct((TALL // ROWS, ROWS), jnp.int32),
        ],
        in_specs=[anyspec] * 6,
        out_specs=[anyspec] * 7,
        scratch_shapes=[
            pltpu.VMEM((NQ, 1024, QC), bf16),
            pltpu.VMEM((4 * NT, 1024, TILE), bf16),
            pltpu.VMEM((ROWS, LOC), bf16),
            pltpu.VMEM((LOC,), bf16),
            pltpu.SMEM((SUB,), jnp.int32),
            pltpu.VMEM((SUB, ROWS), jnp.int32),
            pltpu.VMEM((ROWS, LOC), bf16),
            pltpu.VMEM((LOC,), bf16),
            pltpu.VMEM((2, SUB, NQ * QC), bf16),
            pltpu.VMEM((8, 8, ROWS), f32),
            pltpu.VMEM((8, 8, ROWS), f32),
            pltpu.VMEM((ROWS, 1024), bf16),
            pltpu.VMEM((NQ, 4, 32, QC), f32),
            pltpu.VMEM((NQ, 2, 32, QC), f32),
            pltpu.VMEM((NQ, 32, QC), f32),
            pltpu.VMEM((NQ, 32, QC), f32),
            pltpu.VMEM((NQ, 32, QC), bf16),
            pltpu.VMEM((NQ, SUB, QC), bf16),
            pltpu.VMEM((2 * NT, ROWS, TILE), f32),
            pltpu.VMEM((2 * NT, ROWS, TILE), f32),
            pltpu.VMEM((2 * NT, ROWS, TILE), f32),
            dma((NQ,)), dma((4 * NT,)), dma, dma, dma, dma, dma((7,)), dma((8,)),
            dma((NQ, 2)), dma((NQ, 2)), dma((NQ,)), dma((NQ,)), dma((NQ,)), dma((NQ,)),
            dma((2 * NT,)), dma((2 * NT,)), dma((2 * NT,)), dma, dma, dma, dma, dma, dma, dma, dma,
        ],
        compiler_params=pltpu.CompilerParams(
            collective_id=0, has_side_effects=True, vmem_limit_bytes=VMEM_LIMIT),
        cost_estimate=pl.CostEstimate(flops=5_000_000_000, bytes_accessed=45_000_000, transcendentals=0),
        name="in_proj",
    )(x_loc, gain, lens, wq, wg, wu)


SLOTS = 6


def attend_kernel(lo, hi, len_hbm, qkv_hbm, k_ref, v_ref, *refs):
    if lo:
        refs = refs[2:]
    (ko_ref, vo_ref, o_hbm, o_ref, kb, vb, len_ref, lens, qkv_ref, qs, kns, vns, osc,
     ksem, vsem, kosem, vosem, isem, osem) = refs
    t_len = k_ref.shape[1]

    def k_in(r, s):
        return local_copy(k_ref.at[r], kb.at[s], ksem.at[s])

    def v_in(r, s):
        return local_copy(v_ref.at[r], vb.at[s], vsem.at[s])

    def k_out(r, s):
        return local_copy(kb.at[s], ko_ref.at[r], kosem.at[s])

    def v_out(r, s):
        return local_copy(vb.at[s], vo_ref.at[r], vosem.at[s])

    AHEAD = 4
    len_in = local_copy(len_hbm.at[pl.ds(0, SUB)], len_ref, isem.at[0])
    lens_in = local_copy(len_hbm.at[pl.ds(0, SUB)], lens, isem.at[2])
    lens_in.start()
    qkv_in = local_copy(qkv_hbm.at[pl.ds(0, 2)], qkv_ref, isem.at[1])
    len_in.start()
    qkv_in.start()
    for r in range(lo, lo + 2):
        k_in(r, r % SLOTS).start()
        v_in(r, r % SLOTS).start()
    len_in.wait()
    lens_in.wait()
    qkv_in.wait()
    for r in range(lo + 2, lo + AHEAD):
        k_in(r, r % SLOTS).start()
        v_in(r, r % SLOTS).start()
    half = lax.broadcasted_iota(jnp.int32, (SUB, ROWS), 1).astype(f32)
    angles = lens[...].astype(f32) * 10000.0 ** (-half / ROWS)
    cos_t = jnp.cos(angles)
    sin_t = jnp.sin(angles)
    for g in range(17):
        part, base = (0, g * HD) if g < 9 else (1, (g - 9) * HD)
        a = qkv_ref[part, :, base:base + ROWS].astype(f32)
        b = qkv_ref[part, :, base + ROWS:base + HD].astype(f32)
        lower = (a * cos_t - b * sin_t).astype(bf16).astype(f32)
        upper = (b * cos_t + a * sin_t).astype(bf16).astype(f32)
        if g < SUB:
            qs[:, g, 0:ROWS] = lower
            qs[:, g, ROWS:HD] = upper
        else:
            kns[:, 0:ROWS] = lower
            kns[:, ROWS:HD] = upper
    vns[...] = qkv_ref[1, :, WIDE:2304].astype(f32)

    row16 = lax.broadcasted_iota(jnp.int32, (SUB, HD), 0)
    pos = lax.broadcasted_iota(jnp.int32, (SUB, t_len), 1)

    def body(r, _):
        s = lax.rem(r, SLOTS)
        nxt = r + AHEAD

        @pl.when(nxt < hi)
        def _():
            s2 = lax.rem(nxt, SLOTS)

            @pl.when(nxt - SLOTS >= lo)
            def _():
                k_out(nxt - SLOTS, s2).wait()
                v_out(nxt - SLOTS, s2).wait()
            k_in(nxt, s2).start()
            v_in(nxt, s2).start()

        p = len_ref[r, 0]
        base = pl.multiple_of((p // SUB) * SUB, SUB)
        hit = row16 == p - base
        k_in(r, s).wait()
        krow = kb[s, pl.ds(base, SUB), :]
        kb[s, pl.ds(base, SUB), :] = jnp.where(hit, kns[pl.ds(r, 1), :].astype(bf16), krow)
        v_in(r, s).wait()
        vrow = vb[s, pl.ds(base, SUB), :]
        vb[s, pl.ds(base, SUB), :] = jnp.where(hit, vns[pl.ds(r, 1), :].astype(bf16), vrow)
        q = qs[r].astype(bf16)
        sc = lax.dot_general(q, kb[s], (((1,), (1,)), ((), ())), preferred_element_type=f32) * (HD ** -0.5)
        k_out(r, s).start()
        v_out(r, s).start()
        sc = jnp.where(pos <= p, sc, -1e30)
        m = jnp.max(sc, axis=1, keepdims=True)
        e = jnp.exp(sc - m)
        den = jnp.sum(e, axis=1, keepdims=True)
        pr = (e / den).astype(bf16)
        osc[r] = jnp.dot(pr, vb[s], preferred_element_type=f32).astype(bf16).astype(f32)
        return 0

    lax.fori_loop(lo, hi, body, 0)
    for g in range(SUB):
        o_ref[:, HD * g:HD * (g + 1)] = osc[:, g, :].astype(bf16)
    o_out = local_copy(o_ref, o_hbm.at[pl.ds(0, SUB)], osem)
    o_out.start()
    for r in range(max(lo, hi - SLOTS), hi):
        k_out(r, r % SLOTS).wait()
        v_out(r, r % SLOTS).wait()
    o_out.wait()


def attend(lo, hi, lens, qkv, kc, vc, *prev):
    anyspec = pl.BlockSpec(memory_space=pltpu.HBM)
    dma = pltpu.SemaphoreType.DMA
    n, t_len, hd = kc.shape
    return pl.pallas_call(
        functools.partial(attend_kernel, lo, hi),
        out_shape=[
            jax.ShapeDtypeStruct(kc.shape, bf16),
            jax.ShapeDtypeStruct(vc.shape, bf16),
            jax.ShapeDtypeStruct((TALL // 4096, 4096), bf16),
        ],
        in_specs=[anyspec] * (4 + len(prev)),
        out_specs=[anyspec] * 3,
        input_output_aliases={4: 0, 5: 1} if prev else {},
        scratch_shapes=[
            pltpu.VMEM((n, 4096), bf16),
            pltpu.VMEM((SLOTS, t_len, hd), bf16),
            pltpu.VMEM((SLOTS, t_len, hd), bf16),
            pltpu.SMEM((n, ROWS), jnp.int32),
            pltpu.VMEM((n, ROWS), jnp.int32),
            pltpu.VMEM((2, SUB, NQ * QC), bf16),
            pltpu.VMEM((n, SUB, hd), f32),
            pltpu.VMEM((n, hd), f32),
            pltpu.VMEM((n, hd), f32),
            pltpu.VMEM((n, SUB, hd), f32),
            dma((SLOTS,)), dma((SLOTS,)), dma((SLOTS,)), dma((SLOTS,)), dma((3,)), dma,
        ],
        compiler_params=pltpu.CompilerParams(vmem_limit_bytes=VMEM_LIMIT if lo else 44 * 2 ** 20),
        cost_estimate=pl.CostEstimate(flops=2_500_000_000 * (hi - lo), bytes_accessed=8_400_000 * (hi - lo), transcendentals=1_000_000),
        name=f"attend{lo}",
    )(lens, qkv, kc, vc, *prev)


NA = 3


def act_kernel(d_ref, r0_ref, r_ref, a_hbm, at_hbm, a_ref, asem, tsem):
    def a_out(t):
        return local_copy(a_ref.at[t], a_hbm.at[t], asem.at[t])

    tall = local_copy(a_ref, at_hbm.at[pl.ds(0, NA)], tsem)

    def total(i):
        other = r_ref[i - 1] if i else r0_ref[0]
        return (d_ref[i] + other).astype(bf16).astype(f32)

    for t in range(NA):
        a_ref[t] = (jax.nn.silu(total(2 * t)) * total(2 * t + 1)).astype(bf16)
        if t:
            a_out(t - 1).start()
    a_out(NA - 1).start()
    tall.start()
    for t in range(NA):
        a_out(t).wait()
    tall.wait()


def act(d, r0, r):
    anyspec = pl.BlockSpec(memory_space=pltpu.HBM)
    dma = pltpu.SemaphoreType.DMA
    return pl.pallas_call(
        act_kernel,
        out_shape=[
            jax.ShapeDtypeStruct((NA, ROWS, TILE), bf16),
            jax.ShapeDtypeStruct((TALL // (ROWS * TILE), ROWS, TILE), bf16),
        ],
        in_specs=[pl.BlockSpec(memory_space=pltpu.VMEM)] * 3,
        out_specs=[anyspec] * 2,
        scratch_shapes=[
            pltpu.VMEM((NA, ROWS, TILE), bf16),
            dma((NA,)), dma,
        ],
        compiler_params=pltpu.CompilerParams(vmem_limit_bytes=ACT_LIMIT),
        cost_estimate=pl.CostEstimate(flops=5_000_000, bytes_accessed=4_000_000, transcendentals=200_000),
        name="act",
    )(d, r0, r)


def out_proj_kernel(o1_hbm, o2_hbm, x_hbm, d_ref, r_ref, ao_ref, ax_ref, wao_ref, wmo_ref, y_ref,
                    o1_ref, o2_ref, o_ref, x_ref, db, rb, wao, wmo, ab, ob, zs, zk, zr,
                    osem, xsem, dsem, rsem, asem, waosem, wmosem, pss, psr, fss, fsr, e_s, e_r,
                    o0s, o0r, o1s, o1r, o2s, o2r, o3s, o3r, zss, zrs):
    x = lax.axis_index("x")
    yz = lax.axis_index("yz")
    core = lax.rem(x, 2)
    x_core = x + 1 - 2 * core
    x_chip = lax.rem(x + 2, 4)
    x_diag = x_chip + 1 - 2 * core
    partner = {"x": x_core}
    xpeer = {"x": x_chip}
    ypeer = {"yz": 1 - yz}

    barrier = pltpu.get_barrier_semaphore()
    for dev in (partner, xpeer, ypeer):
        pl.semaphore_signal(barrier, inc=1, device_id=dev, device_id_type=MESH)

    top = pl.ds(0, SUB)
    o_in = [local_copy(o1_hbm.at[top], o1_ref, osem.at[0]), local_copy(o2_hbm.at[top], o2_ref, osem.at[1])]
    for c in o_in:
        c.start()
    first = pl.ds(0, NA)
    own_in = local_copy(ao_ref.at[first], ab.at[x, first], asem.at[0])
    chip_in = local_copy(ax_ref, ab.at[x_chip, first], asem.at[1])
    own_in.start()
    chip_in.start()
    loads = [local_copy(d_ref.at[pl.ds(2 * NA, 2)], db, dsem), local_copy(r_ref, rb, rsem)]
    for c in loads:
        c.start()
    for c in o_in:
        c.wait()
    x_in = local_copy(x_hbm.at[pl.ds(0, ROWS)], x_ref, xsem)
    x_in.start()

    order = (x, x_chip, x_core, x_diag)

    halves = (pl.ds(pl.multiple_of((1 - yz) * LOC, LOC), LOC), pl.ds(pl.multiple_of(yz * LOC, LOC), LOC))
    accs = (zs, zk)

    def wmo_in(half, n, t):
        rows = pl.multiple_of(order[n] * WIDE + t * TILE, TILE)
        k = 4 * n + t
        return local_copy(wmo_ref.at[pl.ds(rows, TILE), halves[half]], wmo.at[half, k], wmosem.at[half, k])

    def wao_in(half):
        return local_copy(wao_ref.at[:, halves[half]], wao.at[half], waosem.at[half])

    def wmo_start(half, n):
        for t in range(4):
            wmo_in(half, n, t).start()

    wmo_start(0, 0)
    row = lax.broadcasted_iota(jnp.int32, (SUB, 4096), 0)
    o_ref[...] = jnp.where(row < SPLIT, o1_ref[...].astype(f32), o2_ref[...].astype(f32)).astype(bf16)
    own_half = pl.multiple_of(yz * WIDE, WIDE)
    peer_half = pl.multiple_of((1 - yz) * WIDE, WIDE)
    mine = 2 * x + yz
    theirs = 2 * x + 1 - yz
    ob[mine] = o_ref[:, pl.ds(own_half, WIDE)]

    for c in loads:
        c.wait()
    gate = (db[0] + rb[0]).astype(bf16).astype(f32)
    up = (db[1] + rb[1]).astype(bf16).astype(f32)
    ab[x, NA] = (jax.nn.silu(gate) * up).astype(bf16)
    pl.semaphore_wait(barrier, 3)

    o_y = remote_copy(o_ref.at[:, pl.ds(peer_half, WIDE)], ob.at[mine], o0s, o0r, ypeer)

    def o_hop(k, ss, rs, dev, owner):
        block = ob.at[2 * owner + (yz if k == 0 else 1 - yz)]
        return remote_copy(block, block, ss.at[k], rs.at[k], dev)

    o_part = [o_hop(k, o1s, o1r, partner, x) for k in range(2)]
    o_chip = [o_hop(k, o2s, o2r, xpeer, x) for k in range(2)]
    o_fwd = [o_hop(k, o3s, o3r, partner, x_chip) for k in range(2)]

    def a_hop(owner, tiles, ss, rs, k, dev):
        block = ab.at[owner, tiles]
        return remote_copy(block, block, ss.at[k], rs.at[k], dev)

    chip = x // 2
    own_rows = pl.multiple_of(HALF * chip, HALF)
    peer_rows = pl.multiple_of(HALF - HALF * chip, HALF)

    def last_hop(owner, base, ss, rs, k, dev):
        block = ab.at[owner, NA, pl.ds(base, HALF)]
        return remote_copy(block, block, ss.at[k], rs.at[k], dev)

    last = pl.ds(NA, 1)
    a_part = [a_hop(x, first, pss, psr, 0, partner), a_hop(x, last, pss, psr, 1, partner)]
    a_fwd = [a_hop(x_chip, first, fss, fsr, 0, partner)]
    a_chip = [last_hop(x, peer_rows, e_s, e_r, 0, xpeer), last_hop(x, own_rows, e_s, e_r, 1, xpeer)]
    a_fwd += [last_hop(x_chip, own_rows, fss, fsr, 1, partner), last_hop(x_chip, peer_rows, fss, fsr, 2, partner)]

    o_y.start()
    for c in a_chip:
        c.start()
    o_chip[0].start()
    o_part[0].start()
    a_part[1].start()
    own_in.wait()
    a_part[0].start()
    chip_in.wait()
    a_fwd[0].start()
    wmo_start(0, 1)
    wmo_start(0, 2)
    wao_in(0).start()
    wmo_start(0, 3)

    def mlp(half, n, t, init=False):
        wmo_in(half, n, t).wait()
        acc = accs[half]
        part = jnp.dot(ab[order[n], t], wmo[half, 4 * n + t], preferred_element_type=f32)
        acc[...] = part if init else acc[...] + part

    chip_rows = pl.multiple_of(32 * x_chip, 32)
    diag_rows = pl.multiple_of(32 * x_diag, 32)

    def z_y(c, base, m):
        rows = pl.ds(base, m)
        return remote_copy(zs.at[rows], zr.at[rows], zss.at[c], zrs.at[c], ypeer)

    def attn_rows(half, base, m):
        rows = pl.ds(base, m)
        attn = ob[pl.ds(base // SUB, m // SUB)].reshape(m, WIDE)
        accs[half][rows] += jnp.dot(attn, wao[half], preferred_element_type=f32)

    def mlp_rows(n, base):
        rows = pl.ds(base, HALF)
        zs[rows] += jnp.dot(ab[order[n], NA, rows], wmo[0, 4 * n + NA], preferred_element_type=f32)

    blocks = ((own_rows, HALF), (chip_rows, 32), (diag_rows, 32))
    for t in range(4):
        mlp(0, 0, t, init=t == 0)
    o_y.wait()
    o_chip[1].start()
    o_part[1].start()
    wmo_start(1, 0)
    wmo_start(1, 1)
    for t in range(NA):
        mlp(0, 1, t)
    a_part[0].wait()
    for t in range(NA):
        mlp(0, 2, t)
    a_chip[0].wait()
    a_fwd[1].start()
    a_part[1].wait()
    mlp(0, 2, NA)
    wmo_in(0, 1, NA).wait()
    mlp_rows(1, own_rows)
    wao_in(0).wait()
    for k in range(2):
        o_part[k].wait()
    attn_rows(0, *blocks[0])
    a_fwd[0].wait()
    for t in range(NA):
        mlp(0, 3, t)
    wmo_in(0, 3, NA).wait()
    a_fwd[1].wait()
    mlp_rows(3, own_rows)
    wmo_start(1, 2)
    wmo_start(1, 3)
    wao_in(1).start()
    a_chip[1].wait()
    a_fwd[2].start()
    mlp_rows(1, peer_rows)
    z_y(0, *blocks[0]).start()
    o_chip[0].wait()
    o_fwd[0].start()
    mlp(1, 0, 0, init=True)
    a_fwd[2].wait()
    mlp_rows(3, peer_rows)
    o_chip[1].wait()
    o_fwd[1].start()
    attn_rows(0, *blocks[1])
    mlp(1, 0, 1)
    z_y(1, *blocks[1]).start()
    for k in range(2):
        o_fwd[k].wait()
    attn_rows(0, *blocks[2])
    mlp(1, 0, 2)
    z_y(2, *blocks[2]).start()
    mlp(1, 0, NA)
    for n in range(1, 4):
        for t in range(4):
            mlp(1, n, t)
    wao_in(1).wait()
    attn_rows(1, 0, ROWS)
    x_in.wait()
    for c, (base, m) in enumerate(blocks):
        z_y(c, base, m).wait()
        rows = pl.ds(base, m)
        y_ref[rows, :] = (x_ref[rows, :].astype(f32) + (zk[rows, :] + zr[rows, :])).astype(bf16)


def out_proj(o1, o2, x_loc, d, r, a_own, a_chip, wao, wmo):
    anyspec = pl.BlockSpec(memory_space=pltpu.HBM)
    vspec = pl.BlockSpec(memory_space=pltpu.VMEM)
    dma = pltpu.SemaphoreType.DMA
    two = dma((2,))
    return pl.pallas_call(
        out_proj_kernel,
        out_shape=jax.ShapeDtypeStruct((ROWS, LOC), bf16),
        in_specs=[anyspec] * 9,
        out_specs=vspec,
        scratch_shapes=[
            pltpu.VMEM((SUB, 4096), bf16),
            pltpu.VMEM((SUB, 4096), bf16),
            pltpu.VMEM((SUB, 4096), bf16),
            pltpu.VMEM((ROWS, LOC), bf16),
            pltpu.VMEM((2, ROWS, TILE), f32),
            pltpu.VMEM((2, ROWS, TILE), f32),
            pltpu.VMEM((2, WIDE, LOC), bf16),
            pltpu.VMEM((2, SUB, TILE, LOC), bf16),
            pltpu.VMEM((4, 4, ROWS, TILE), bf16),
            pltpu.VMEM((8, SUB, WIDE), bf16),
            pltpu.VMEM((ROWS, LOC), f32),
            pltpu.VMEM((ROWS, LOC), f32),
            pltpu.VMEM((ROWS, LOC), f32),
            two, dma, dma, dma, two, two, dma((2, SUB)),
            two, two, dma((3,)), dma((3,)), two, two,
            dma, dma, two, two, two, two, two, two, dma((3,)), dma((3,)),
        ],
        compiler_params=pltpu.CompilerParams(
            collective_id=1, has_side_effects=True, vmem_limit_bytes=VMEM_LIMIT - OUT_ROOM),
        cost_estimate=pl.CostEstimate(flops=3_000_000_000, bytes_accessed=26_000_000, transcendentals=0),
        name="out_proj",
    )(o1, o2, x_loc, d, r, a_own, a_chip, wao, wmo)


def solution(mesh):
    both_axes = ("x", "yz")
    row_spec = P("dp", both_axes)
    in_w_spec = P("x", "yz")
    out_w_spec = P("yz", "x")
    cache_spec = P(("dp", "x", "yz"), None, None)
    len_spec = P(("dp", "x", "yz"))
    swap = [(0, 2), (2, 0), (1, 3), (3, 1)]

    def local_layer(x_loc, gain_loc, wqkv_loc, wgate_loc, wup_loc, wao_loc, wmo_loc, kc_loc, vc_loc, len_loc):
        qkv, sa, sb, r0, d, x_tall, lens = in_proj(x_loc, gain_loc, len_loc, wqkv_loc, wgate_loc, wup_loc)
        ra = lax.ppermute(sa, "x", swap)
        k_all, v_all, o1 = attend(0, SPLIT, lens, qkv, kc_loc, vc_loc)
        sb, o1 = lax.optimization_barrier((sb, o1))
        rb = lax.ppermute(sb, "x", swap)
        a_own, a_tall = act(d, r0, ra)
        a_chip = lax.ppermute(a_own, "x", swap)
        k_all, v_all, o2 = attend(SPLIT, SUB, lens, qkv, kc_loc, vc_loc, k_all, v_all)
        y_loc = out_proj(o1, o2, x_tall, d, rb, a_tall, a_chip, wao_loc, wmo_loc)
        return y_loc, k_all, v_all

    in_specs = (row_spec, P(both_axes), in_w_spec, in_w_spec, in_w_spec, out_w_spec, out_w_spec, cache_spec, cache_spec, len_spec)
    out_specs = (row_spec, cache_spec, cache_spec)
    return jax.shard_map(local_layer, mesh=mesh, in_specs=in_specs, out_specs=out_specs, check_vma=False)
```

```python
import functools

import jax
import jax.numpy as jnp
from jax import lax
from jax.experimental import pallas as pl
from jax.experimental.pallas import tpu as pltpu
from jax.sharding import PartitionSpec as P

MESH = pl.DeviceIdType.MESH
VMEM_LIMIT = 67043328
ROWS = 128
HD = 256
LOC = 512
SUB = 16
HALF = 64
WIDE = 2048
ACT_LIMIT = 46 * 2 ** 20
TALL = 2 ** 23
OUT_ROOM = 11700000
TILE = 512
SA = 5
SPLIT = 10
NT = 8
QC = 384
NQ = 6
W_FIRST = 8
W_AHEAD = 12

f32 = jnp.float32
bf16 = jnp.bfloat16


def local_copy(src, dst, sem):
    return pltpu.make_async_copy(src, dst, sem)


def remote_copy(src, dst, ssem, rsem, dev):
    return pltpu.make_async_remote_copy(src, dst, ssem, rsem, device_id=dev, device_id_type=MESH)


def in_proj_kernel(x_hbm, g_hbm, len_hbm, wq_ref, wg_ref, wu_ref, qkv_ref, sa_ref, sb_ref, r0_ref, d_ref, xc_ref, lens_ref,
                   wqv, wv, x_ref, g_ref, len_s, lens, xr, gr, qout, st, stx, h, qp, qr, qxs, qxr, qf, qyr, sbuf, rbuf, obuf,
                   wqsem, wsem, xs_sem, xr_sem, gs_sem, gr_sem, sts_sem, str_sem,
                   qds_sem, qdr_sem, qxs_sem, qxr_sem, qys_sem, qyr_sem, ds_sem, dr_sem, out_sem, xin_sem, gin_sem, qo_sem, es_sem, er_sem, xc_sem, len_sem, lens_sem):
    d_model = 4096
    x = lax.axis_index("x")
    yz = lax.axis_index("yz")
    core = lax.rem(x, 2)
    x_core = x + 1 - 2 * core
    x_chip = lax.rem(x + 2, 4)
    x_diag = x_chip + 1 - 2 * core
    me = 2 * x + yz
    partner = {"x": x_core}
    xpeer = {"x": x_chip}
    ypeer = {"yz": 1 - yz}

    barrier = pltpu.get_barrier_semaphore()
    others = []
    for dx in range(4):
        for dy in range(2):
            if dx or dy:
                others.append((lax.rem(x + dx, 4), lax.rem(yz + dy, 2)))
    for ox, oy in others:
        pl.semaphore_signal(barrier, inc=1, device_id={"x": ox, "yz": oy}, device_id_type=MESH)
    x_in = local_copy(x_hbm, x_ref, xin_sem)
    g_in = local_copy(g_hbm, g_ref, gin_sem)
    x_in.start()
    g_in.start()
    len_in = local_copy(len_hbm, len_s, len_sem)
    len_in.start()

    def wq_copy(j):
        return local_copy(wq_ref.at[:, pl.ds(QC * j, QC)], wqv.at[j], wqsem.at[j])

    quarters = (x_diag, x_chip, x_core, x)

    def w_start(slot):
        phase = slot // NT
        q = quarters[0]
        for n in range(1, 4):
            q = jnp.where(phase == n, quarters[n], q)
        cols = pl.multiple_of(q * WIDE + (slot % NT) // 2 * TILE, TILE)

        def start(w_hbm):
            local_copy(w_hbm.at[:, pl.ds(cols, TILE)], wv.at[slot], wsem.at[slot]).start()

        if isinstance(slot, int):
            start(wg_ref if slot % 2 == 0 else wu_ref)
        else:
            pl.when(slot % 2 == 0)(lambda: start(wg_ref))
            pl.when(slot % 2 == 1)(lambda: start(wu_ref))

    def w_wait(slot):
        local_copy(wg_ref.at[:, pl.ds(0, TILE)], wv.at[slot], wsem.at[slot]).wait()

    x_in.wait()
    for j in range(NQ):
        wq_copy(j).start()
    for slot in range(W_FIRST):
        w_start(slot)
    g_in.wait()
    xf = x_ref[...].astype(f32)
    s1 = jnp.sum(xf, axis=1, keepdims=True)
    s2 = jnp.sum(xf * xf, axis=1, keepdims=True)
    lane = lax.broadcasted_iota(jnp.int32, (ROWS, ROWS), 1)
    stat = jnp.where(lane == 0, s1, s2).T
    st[me] = stat[0:8]

    pl.semaphore_wait(barrier, 7)

    x_send = remote_copy(x_ref, xr, xs_sem, xr_sem, ypeer)
    g_send = remote_copy(g_ref, gr, gs_sem, gr_sem, ypeer)
    for n, (ox, oy) in enumerate(others):
        remote_copy(st.at[me], stx.at[me], sts_sem.at[n], str_sem.at[me], {"x": ox, "yz": oy}).start()
    g_send.start()
    x_send.start()
    stx[me] = st[me]
    for n, (ox, oy) in enumerate(others):
        src = 2 * ox + oy
        remote_copy(st.at[me], stx.at[src], sts_sem.at[n], str_sem.at[src], {"x": ox, "yz": oy}).wait()
    tot = jnp.sum(stx[...], axis=0)
    tot = jnp.concatenate([tot, jnp.zeros((120, ROWS), f32)], axis=0).T
    mean = tot[:, 0:1] / d_model
    var = tot[:, 1:2] / d_model - mean * mean
    rstd = lax.rsqrt(var + 1e-6)
    own_cols = pl.multiple_of(yz * LOC, LOC)
    peer_cols = pl.multiple_of((1 - yz) * LOC, LOC)
    h[:, pl.ds(own_cols, LOC)] = ((xf - mean) * rstd * g_ref[...].astype(f32).reshape(1, LOC)).astype(bf16)
    x_send.wait()
    g_send.wait()
    h[:, pl.ds(peer_cols, LOC)] = ((xr[...].astype(f32) - mean) * rstd * gr[...].astype(f32).reshape(1, LOC)).astype(bf16)

    for slot in range(W_FIRST, W_AHEAD):
        w_start(slot)

    def q_compute(j):
        wq_copy(j).wait()
        part = jnp.dot(h[...], wqv[j], preferred_element_type=f32)
        qp[j] = part.reshape(4, 32, QC)

    def q_pair(j, k):
        block = (x_diag, x_core)[k]
        return remote_copy(qp.at[j, block], qr.at[j, k], qds_sem.at[j, k], qdr_sem.at[j, k], partner)

    def q_pair_start(j):
        q_pair(j, 0).start()
        q_pair(j, 1).start()

    def q_chip(j):
        return remote_copy(qxs.at[j], qxr.at[j], qxs_sem.at[j], qxr_sem.at[j], xpeer)

    def q_sum(j):
        q_pair(j, 0).wait()
        qxs[j] = qp[j, x_chip] + qr[j, 0]

    def tile(slot):
        w_wait(slot)
        if isinstance(slot, int):
            if slot + W_AHEAD < 4 * NT:
                w_start(slot + W_AHEAD)
        else:
            @pl.when(slot + W_AHEAD < 4 * NT)
            def _():
                w_start(slot + W_AHEAD)
        return jnp.dot(h[...], wv[slot], preferred_element_type=f32)

    def d_copy(i):
        return remote_copy(sbuf.at[i], rbuf.at[i], ds_sem.at[i], dr_sem.at[i], partner)

    def s_out(i):
        dst = sa_ref.at[i - 1] if i <= SA else sb_ref.at[i - 1 - SA]
        return local_copy(obuf.at[i], dst, out_sem.at[i])

    def d_out(i):
        return local_copy(obuf.at[NT + i], d_ref.at[i], out_sem.at[NT + i])

    early = remote_copy(obuf.at[0], r0_ref.at[0], es_sem, er_sem, xpeer)

    len_in.wait()
    row = lax.broadcasted_iota(jnp.int32, (SUB, ROWS), 0)
    rows = jnp.zeros((SUB, ROWS), jnp.int32)
    for r in range(SUB):
        rows = jnp.where(row == r, len_s[r], rows)
    lens[...] = rows

    for j in range(NQ):
        q_compute(j)
        if j:
            q_pair_start(j - 1)
    q_sum(0)

    after = {
        0: lambda: (q_pair_start(NQ - 1), q_chip(0).start(), q_sum(1)),
        1: lambda: (q_chip(1).start(), q_sum(2), q_sum(3)),
        2: lambda: (q_chip(2).start(), q_chip(3).start(), q_sum(4)),
        3: lambda: (q_chip(4).start(), q_sum(5)),
        4: lambda: q_chip(5).start(),
    }
    for i in range(NT):
        sbuf[i] = tile(i)
        if i:
            d_copy(i - 1).start()
        if i in after:
            after[i]()

    for i in range(NT):
        part = tile(NT + i)
        if i == 0:
            d_copy(NT - 1).start()
        d_copy(i).wait()
        obuf[i] = part + rbuf[i]
        if i == 1:
            early.start()
        elif i:
            s_out(i - 1).start()

    own_rows = pl.multiple_of(yz * SUB, SUB)
    peer_rows = pl.multiple_of((1 - yz) * SUB, SUB)

    def q_y(j):
        return remote_copy(qf.at[j, pl.ds(peer_rows, SUB)], qyr.at[j], qys_sem.at[j], qyr_sem.at[j], ypeer)

    def q_final(j):
        q_pair(j, 1).wait()
        q_chip(j).wait()
        qf[j] = (qp[j, x] + qr[j, 1] + qxr[j]).astype(bf16)
        qout[yz, :, pl.ds(QC * j, QC)] = qf[j, pl.ds(own_rows, SUB)]

    def send_tiles(lo, hi):
        def body(i, _):
            sbuf[NT + i] = tile(2 * NT + i)

            @pl.when(i == 0)
            def _():
                s_out(NT - 1).start()

            @pl.when(i > 0)
            def _():
                d_copy(NT + i - 1).start()
            return 0

        lax.fori_loop(lo, hi, body, 0)

    def keep_tiles(lo, hi):
        def body(i, _):
            part = tile(3 * NT + i)

            @pl.when(i == 0)
            def _():
                d_copy(2 * NT - 1).start()
            d_copy(NT + i).wait()
            obuf[NT + i] = part + rbuf[NT + i]

            @pl.when(i > 0)
            def _():
                d_out(i - 1).start()
            return 0

        lax.fori_loop(lo, hi, body, 0)

    send_tiles(0, 3)
    for j in range(3):
        q_final(j)
    send_tiles(3, 4)
    for j in range(3):
        q_y(j).start()
    send_tiles(4, 8)
    q_final(3)
    q_final(4)
    keep_tiles(0, 2)
    q_y(3).start()
    q_y(4).start()
    q_final(5)
    keep_tiles(2, 3)
    q_y(5).start()
    keep_tiles(3, 8)
    d_out(NT - 1).start()
    for j in range(NQ):
        q_y(j).wait()
        qout[1 - yz, :, pl.ds(QC * j, QC)] = qyr[j]
    q_out = local_copy(qout, qkv_ref.at[pl.ds(0, 2)], qo_sem)
    q_out.start()
    lens_out = local_copy(lens, lens_ref.at[pl.ds(0, SUB)], lens_sem)
    lens_out.start()
    x_out = local_copy(x_ref, xc_ref.at[pl.ds(0, ROWS)], xc_sem)
    x_out.start()
    for i in range(NT):
        if i:
            s_out(i).wait()
        d_out(i).wait()
    q_out.wait()
    x_out.wait()
    lens_out.wait()
    early.wait()


def in_proj(x_loc, gain, lens, wq, wg, wu):
    anyspec = pl.BlockSpec(memory_space=pltpu.HBM)
    dma = pltpu.SemaphoreType.DMA
    return pl.pallas_call(
        in_proj_kernel,
        out_shape=[
            jax.ShapeDtypeStruct((TALL // (SUB * NQ * QC), SUB, NQ * QC), bf16),
            jax.ShapeDtypeStruct((SA, ROWS, TILE), f32),
            jax.ShapeDtypeStruct((NT - 1 - SA, ROWS, TILE), f32),
            jax.ShapeDtypeStruct((1, ROWS, TILE), f32),
            jax.ShapeDtypeStruct((NT, ROWS, TILE), f32),
            jax.ShapeDtypeStruct((TALL // LOC, LOC), bf16),
            jax.ShapeDtypeStruct((TALL // ROWS, ROWS), jnp.int32),
        ],
        in_specs=[anyspec] * 6,
        out_specs=[anyspec] * 7,
        scratch_shapes=[
            pltpu.VMEM((NQ, 1024, QC), bf16),
            pltpu.VMEM((4 * NT, 1024, TILE), bf16),
            pltpu.VMEM((ROWS, LOC), bf16),
            pltpu.VMEM((LOC,), bf16),
            pltpu.SMEM((SUB,), jnp.int32),
            pltpu.VMEM((SUB, ROWS), jnp.int32),
            pltpu.VMEM((ROWS, LOC), bf16),
            pltpu.VMEM((LOC,), bf16),
            pltpu.VMEM((2, SUB, NQ * QC), bf16),
            pltpu.VMEM((8, 8, ROWS), f32),
            pltpu.VMEM((8, 8, ROWS), f32),
            pltpu.VMEM((ROWS, 1024), bf16),
            pltpu.VMEM((NQ, 4, 32, QC), f32),
            pltpu.VMEM((NQ, 2, 32, QC), f32),
            pltpu.VMEM((NQ, 32, QC), f32),
            pltpu.VMEM((NQ, 32, QC), f32),
            pltpu.VMEM((NQ, 32, QC), bf16),
            pltpu.VMEM((NQ, SUB, QC), bf16),
            pltpu.VMEM((2 * NT, ROWS, TILE), f32),
            pltpu.VMEM((2 * NT, ROWS, TILE), f32),
            pltpu.VMEM((2 * NT, ROWS, TILE), f32),
            dma((NQ,)), dma((4 * NT,)), dma, dma, dma, dma, dma((7,)), dma((8,)),
            dma((NQ, 2)), dma((NQ, 2)), dma((NQ,)), dma((NQ,)), dma((NQ,)), dma((NQ,)),
            dma((2 * NT,)), dma((2 * NT,)), dma((2 * NT,)), dma, dma, dma, dma, dma, dma, dma, dma,
        ],
        compiler_params=pltpu.CompilerParams(
            collective_id=0, has_side_effects=True, vmem_limit_bytes=VMEM_LIMIT),
        cost_estimate=pl.CostEstimate(flops=5_000_000_000, bytes_accessed=45_000_000, transcendentals=0),
        name="in_proj",
    )(x_loc, gain, lens, wq, wg, wu)


SLOTS = 6


def attend_kernel(lo, hi, len_hbm, qkv_hbm, k_ref, v_ref, *refs):
    if lo:
        refs = refs[2:]
    (ko_ref, vo_ref, o_hbm, o_ref, kb, vb, len_ref, lens, qkv_ref, qs, kns, vns, osc,
     ksem, vsem, kosem, vosem, isem, osem) = refs
    t_len = k_ref.shape[1]

    def k_in(r, s):
        return local_copy(k_ref.at[r], kb.at[s], ksem.at[s])

    def v_in(r, s):
        return local_copy(v_ref.at[r], vb.at[s], vsem.at[s])

    def k_out(r, s):
        return local_copy(kb.at[s], ko_ref.at[r], kosem.at[s])

    def v_out(r, s):
        return local_copy(vb.at[s], vo_ref.at[r], vosem.at[s])

    AHEAD = 4
    len_in = local_copy(len_hbm.at[pl.ds(0, SUB)], len_ref, isem.at[0])
    lens_in = local_copy(len_hbm.at[pl.ds(0, SUB)], lens, isem.at[2])
    lens_in.start()
    qkv_in = local_copy(qkv_hbm.at[pl.ds(0, 2)], qkv_ref, isem.at[1])
    len_in.start()
    qkv_in.start()
    for r in range(lo, lo + 2):
        k_in(r, r % SLOTS).start()
        v_in(r, r % SLOTS).start()
    len_in.wait()
    lens_in.wait()
    qkv_in.wait()
    for r in range(lo + 2, lo + AHEAD):
        k_in(r, r % SLOTS).start()
        v_in(r, r % SLOTS).start()
    half = lax.broadcasted_iota(jnp.int32, (SUB, ROWS), 1).astype(f32)
    angles = lens[...].astype(f32) * 10000.0 ** (-half / ROWS)
    cos_t = jnp.cos(angles)
    sin_t = jnp.sin(angles)
    for g in range(17):
        part, base = (0, g * HD) if g < 9 else (1, (g - 9) * HD)
        a = qkv_ref[part, :, base:base + ROWS].astype(f32)
        b = qkv_ref[part, :, base + ROWS:base + HD].astype(f32)
        lower = (a * cos_t - b * sin_t).astype(bf16).astype(f32)
        upper = (b * cos_t + a * sin_t).astype(bf16).astype(f32)
        if g < SUB:
            qs[:, g, 0:ROWS] = lower
            qs[:, g, ROWS:HD] = upper
        else:
            kns[:, 0:ROWS] = lower
            kns[:, ROWS:HD] = upper
    vns[...] = qkv_ref[1, :, WIDE:2304].astype(f32)

    row16 = lax.broadcasted_iota(jnp.int32, (SUB, HD), 0)
    pos = lax.broadcasted_iota(jnp.int32, (SUB, t_len), 1)

    def body(r, _):
        s = lax.rem(r, SLOTS)
        nxt = r + AHEAD

        @pl.when(nxt < hi)
        def _():
            s2 = lax.rem(nxt, SLOTS)

            @pl.when(nxt - SLOTS >= lo)
            def _():
                k_out(nxt - SLOTS, s2).wait()
                v_out(nxt - SLOTS, s2).wait()
            k_in(nxt, s2).start()
            v_in(nxt, s2).start()

        p = len_ref[r, 0]
        base = pl.multiple_of((p // SUB) * SUB, SUB)
        hit = row16 == p - base
        k_in(r, s).wait()
        krow = kb[s, pl.ds(base, SUB), :]
        kb[s, pl.ds(base, SUB), :] = jnp.where(hit, kns[pl.ds(r, 1), :].astype(bf16), krow)
        v_in(r, s).wait()
        vrow = vb[s, pl.ds(base, SUB), :]
        vb[s, pl.ds(base, SUB), :] = jnp.where(hit, vns[pl.ds(r, 1), :].astype(bf16), vrow)
        q = qs[r].astype(bf16)
        sc = lax.dot_general(q, kb[s], (((1,), (1,)), ((), ())), preferred_element_type=f32) * (HD ** -0.5)
        k_out(r, s).start()
        v_out(r, s).start()
        sc = jnp.where(pos <= p, sc, -1e30)
        m = jnp.max(sc, axis=1, keepdims=True)
        e = jnp.exp(sc - m)
        den = jnp.sum(e, axis=1, keepdims=True)
        pr = (e / den).astype(bf16)
        osc[r] = jnp.dot(pr, vb[s], preferred_element_type=f32).astype(bf16).astype(f32)
        return 0

    lax.fori_loop(lo, hi, body, 0)
    for g in range(SUB):
        o_ref[:, HD * g:HD * (g + 1)] = osc[:, g, :].astype(bf16)
    o_out = local_copy(o_ref, o_hbm.at[pl.ds(0, SUB)], osem)
    o_out.start()
    for r in range(max(lo, hi - SLOTS), hi):
        k_out(r, r % SLOTS).wait()
        v_out(r, r % SLOTS).wait()
    o_out.wait()


def attend(lo, hi, lens, qkv, kc, vc, *prev):
    anyspec = pl.BlockSpec(memory_space=pltpu.HBM)
    dma = pltpu.SemaphoreType.DMA
    n, t_len, hd = kc.shape
    return pl.pallas_call(
        functools.partial(attend_kernel, lo, hi),
        out_shape=[
            jax.ShapeDtypeStruct(kc.shape, bf16),
            jax.ShapeDtypeStruct(vc.shape, bf16),
            jax.ShapeDtypeStruct((TALL // 4096, 4096), bf16),
        ],
        in_specs=[anyspec] * (4 + len(prev)),
        out_specs=[anyspec] * 3,
        input_output_aliases={4: 0, 5: 1} if prev else {},
        scratch_shapes=[
            pltpu.VMEM((n, 4096), bf16),
            pltpu.VMEM((SLOTS, t_len, hd), bf16),
            pltpu.VMEM((SLOTS, t_len, hd), bf16),
            pltpu.SMEM((n, ROWS), jnp.int32),
            pltpu.VMEM((n, ROWS), jnp.int32),
            pltpu.VMEM((2, SUB, NQ * QC), bf16),
            pltpu.VMEM((n, SUB, hd), f32),
            pltpu.VMEM((n, hd), f32),
            pltpu.VMEM((n, hd), f32),
            pltpu.VMEM((n, SUB, hd), f32),
            dma((SLOTS,)), dma((SLOTS,)), dma((SLOTS,)), dma((SLOTS,)), dma((3,)), dma,
        ],
        compiler_params=pltpu.CompilerParams(vmem_limit_bytes=VMEM_LIMIT if lo else 44 * 2 ** 20),
        cost_estimate=pl.CostEstimate(flops=2_500_000_000 * (hi - lo), bytes_accessed=8_400_000 * (hi - lo), transcendentals=1_000_000),
        name=f"attend{lo}",
    )(lens, qkv, kc, vc, *prev)


NA = 3


def act_kernel(d_ref, r0_ref, r_ref, a_hbm, at_hbm, a_ref, asem, tsem):
    def a_out(t):
        return local_copy(a_ref.at[t], a_hbm.at[t], asem.at[t])

    tall = local_copy(a_ref, at_hbm.at[pl.ds(0, NA)], tsem)

    def total(i):
        other = r_ref[i - 1] if i else r0_ref[0]
        return (d_ref[i] + other).astype(bf16).astype(f32)

    for t in range(NA):
        a_ref[t] = (jax.nn.silu(total(2 * t)) * total(2 * t + 1)).astype(bf16)
        if t:
            a_out(t - 1).start()
    a_out(NA - 1).start()
    tall.start()
    for t in range(NA):
        a_out(t).wait()
    tall.wait()


def act(d, r0, r):
    anyspec = pl.BlockSpec(memory_space=pltpu.HBM)
    dma = pltpu.SemaphoreType.DMA
    return pl.pallas_call(
        act_kernel,
        out_shape=[
            jax.ShapeDtypeStruct((NA, ROWS, TILE), bf16),
            jax.ShapeDtypeStruct((TALL // (ROWS * TILE), ROWS, TILE), bf16),
        ],
        in_specs=[pl.BlockSpec(memory_space=pltpu.VMEM)] * 3,
        out_specs=[anyspec] * 2,
        scratch_shapes=[
            pltpu.VMEM((NA, ROWS, TILE), bf16),
            dma((NA,)), dma,
        ],
        compiler_params=pltpu.CompilerParams(vmem_limit_bytes=ACT_LIMIT),
        cost_estimate=pl.CostEstimate(flops=5_000_000, bytes_accessed=4_000_000, transcendentals=200_000),
        name="act",
    )(d, r0, r)


def out_proj_kernel(o1_hbm, o2_hbm, x_hbm, d_ref, r_ref, ao_ref, ax_ref, wao_ref, wmo_ref, y_ref,
                    o1_ref, o2_ref, o_ref, x_ref, db, rb, wao, wmo, ab, ob, zs, zk, zr,
                    osem, xsem, dsem, rsem, asem, waosem, wmosem, pss, psr, fss, fsr, e_s, e_r,
                    o0s, o0r, o1s, o1r, o2s, o2r, o3s, o3r, zss, zrs):
    x = lax.axis_index("x")
    yz = lax.axis_index("yz")
    core = lax.rem(x, 2)
    x_core = x + 1 - 2 * core
    x_chip = lax.rem(x + 2, 4)
    x_diag = x_chip + 1 - 2 * core
    partner = {"x": x_core}
    xpeer = {"x": x_chip}
    ypeer = {"yz": 1 - yz}

    barrier = pltpu.get_barrier_semaphore()
    for dev in (partner, xpeer, ypeer):
        pl.semaphore_signal(barrier, inc=1, device_id=dev, device_id_type=MESH)

    top = pl.ds(0, SUB)
    o_in = [local_copy(o1_hbm.at[top], o1_ref, osem.at[0]), local_copy(o2_hbm.at[top], o2_ref, osem.at[1])]
    for c in o_in:
        c.start()
    first = pl.ds(0, NA)
    own_in = local_copy(ao_ref.at[first], ab.at[x, first], asem.at[0])
    chip_in = local_copy(ax_ref, ab.at[x_chip, first], asem.at[1])
    loads = [local_copy(d_ref.at[pl.ds(2 * NA, 2)], db, dsem), local_copy(r_ref, rb, rsem)]
    for c in loads:
        c.start()
    for c in o_in:
        c.wait()
    x_in = local_copy(x_hbm.at[pl.ds(0, ROWS)], x_ref, xsem)
    own_in.start()
    chip_in.start()
    x_in.start()

    order = (x, x_chip, x_core, x_diag)

    halves = (pl.ds(pl.multiple_of((1 - yz) * LOC, LOC), LOC), pl.ds(pl.multiple_of(yz * LOC, LOC), LOC))
    accs = (zs, zk)

    def wmo_in(half, n, t):
        rows = pl.multiple_of(order[n] * WIDE + t * TILE, TILE)
        k = 4 * n + t
        return local_copy(wmo_ref.at[pl.ds(rows, TILE), halves[half]], wmo.at[half, k], wmosem.at[half, k])

    def wao_in(half):
        return local_copy(wao_ref.at[:, halves[half]], wao.at[half], waosem.at[half])

    def wmo_start(half, n):
        for t in range(4):
            wmo_in(half, n, t).start()

    row = lax.broadcasted_iota(jnp.int32, (SUB, 4096), 0)
    o_ref[...] = jnp.where(row < SPLIT, o1_ref[...].astype(f32), o2_ref[...].astype(f32)).astype(bf16)
    own_half = pl.multiple_of(yz * WIDE, WIDE)
    peer_half = pl.multiple_of((1 - yz) * WIDE, WIDE)
    mine = 2 * x + yz
    theirs = 2 * x + 1 - yz
    ob[mine] = o_ref[:, pl.ds(own_half, WIDE)]

    for c in loads:
        c.wait()
    wmo_start(0, 0)
    gate = (db[0] + rb[0]).astype(bf16).astype(f32)
    up = (db[1] + rb[1]).astype(bf16).astype(f32)
    ab[x, NA] = (jax.nn.silu(gate) * up).astype(bf16)
    pl.semaphore_wait(barrier, 3)

    o_y = remote_copy(o_ref.at[:, pl.ds(peer_half, WIDE)], ob.at[mine], o0s, o0r, ypeer)

    def o_hop(k, ss, rs, dev, owner):
        block = ob.at[2 * owner + (yz if k == 0 else 1 - yz)]
        return remote_copy(block, block, ss.at[k], rs.at[k], dev)

    o_part = [o_hop(k, o1s, o1r, partner, x) for k in range(2)]
    o_chip = [o_hop(k, o2s, o2r, xpeer, x) for k in range(2)]
    o_fwd = [o_hop(k, o3s, o3r, partner, x_chip) for k in range(2)]

    def a_hop(owner, tiles, ss, rs, k, dev):
        block = ab.at[owner, tiles]
        return remote_copy(block, block, ss.at[k], rs.at[k], dev)

    chip = x // 2
    own_rows = pl.multiple_of(HALF * chip, HALF)
    peer_rows = pl.multiple_of(HALF - HALF * chip, HALF)

    def last_hop(owner, base, ss, rs, k, dev):
        block = ab.at[owner, NA, pl.ds(base, HALF)]
        return remote_copy(block, block, ss.at[k], rs.at[k], dev)

    last = pl.ds(NA, 1)
    a_part = [a_hop(x, first, pss, psr, 0, partner), a_hop(x, last, pss, psr, 1, partner)]
    a_fwd = [a_hop(x_chip, first, fss, fsr, 0, partner)]
    a_chip = [last_hop(x, peer_rows, e_s, e_r, 0, xpeer), last_hop(x, own_rows, e_s, e_r, 1, xpeer)]
    a_fwd += [last_hop(x_chip, own_rows, fss, fsr, 1, partner), last_hop(x_chip, peer_rows, fss, fsr, 2, partner)]

    o_y.start()
    for c in a_chip:
        c.start()
    o_chip[0].start()
    o_part[0].start()
    a_part[1].start()
    own_in.wait()
    a_part[0].start()
    chip_in.wait()
    a_fwd[0].start()
    wmo_start(0, 1)
    wmo_start(0, 2)
    wao_in(0).start()
    wmo_start(0, 3)

    def mlp(half, n, t, init=False):
        wmo_in(half, n, t).wait()
        acc = accs[half]
        part = jnp.dot(ab[order[n], t], wmo[half, 4 * n + t], preferred_element_type=f32)
        acc[...] = part if init else acc[...] + part

    chip_rows = pl.multiple_of(32 * x_chip, 32)
    diag_rows = pl.multiple_of(32 * x_diag, 32)

    def z_y(c, base, m):
        rows = pl.ds(base, m)
        return remote_copy(zs.at[rows], zr.at[rows], zss.at[c], zrs.at[c], ypeer)

    def attn_rows(half, base, m):
        rows = pl.ds(base, m)
        attn = ob[pl.ds(base // SUB, m // SUB)].reshape(m, WIDE)
        accs[half][rows] += jnp.dot(attn, wao[half], preferred_element_type=f32)

    def mlp_rows(n, base):
        rows = pl.ds(base, HALF)
        zs[rows] += jnp.dot(ab[order[n], NA, rows], wmo[0, 4 * n + NA], preferred_element_type=f32)

    blocks = ((own_rows, HALF), (chip_rows, 32), (diag_rows, 32))
    for t in range(4):
        mlp(0, 0, t, init=t == 0)
    o_y.wait()
    o_chip[1].start()
    o_part[1].start()
    wmo_start(1, 0)
    wmo_start(1, 1)
    for t in range(NA):
        mlp(0, 1, t)
    a_part[0].wait()
    for t in range(NA):
        mlp(0, 2, t)
    a_chip[0].wait()
    a_fwd[1].start()
    a_part[1].wait()
    mlp(0, 2, NA)
    wmo_in(0, 1, NA).wait()
    mlp_rows(1, own_rows)
    wao_in(0).wait()
    for k in range(2):
        o_part[k].wait()
    attn_rows(0, *blocks[0])
    a_fwd[0].wait()
    for t in range(NA):
        mlp(0, 3, t)
    wmo_in(0, 3, NA).wait()
    a_fwd[1].wait()
    mlp_rows(3, own_rows)
    wmo_start(1, 2)
    wmo_start(1, 3)
    wao_in(1).start()
    a_chip[1].wait()
    a_fwd[2].start()
    mlp_rows(1, peer_rows)
    z_y(0, *blocks[0]).start()
    o_chip[0].wait()
    o_fwd[0].start()
    mlp(1, 0, 0, init=True)
    a_fwd[2].wait()
    mlp_rows(3, peer_rows)
    o_chip[1].wait()
    o_fwd[1].start()
    attn_rows(0, *blocks[1])
    mlp(1, 0, 1)
    z_y(1, *blocks[1]).start()
    for k in range(2):
        o_fwd[k].wait()
    attn_rows(0, *blocks[2])
    mlp(1, 0, 2)
    z_y(2, *blocks[2]).start()
    mlp(1, 0, NA)
    for n in range(1, 4):
        for t in range(4):
            mlp(1, n, t)
    wao_in(1).wait()
    attn_rows(1, 0, ROWS)
    x_in.wait()
    for c, (base, m) in enumerate(blocks):
        z_y(c, base, m).wait()
        rows = pl.ds(base, m)
        y_ref[rows, :] = (x_ref[rows, :].astype(f32) + (zk[rows, :] + zr[rows, :])).astype(bf16)


def out_proj(o1, o2, x_loc, d, r, a_own, a_chip, wao, wmo):
    anyspec = pl.BlockSpec(memory_space=pltpu.HBM)
    vspec = pl.BlockSpec(memory_space=pltpu.VMEM)
    dma = pltpu.SemaphoreType.DMA
    two = dma((2,))
    return pl.pallas_call(
        out_proj_kernel,
        out_shape=jax.ShapeDtypeStruct((ROWS, LOC), bf16),
        in_specs=[anyspec] * 9,
        out_specs=vspec,
        scratch_shapes=[
            pltpu.VMEM((SUB, 4096), bf16),
            pltpu.VMEM((SUB, 4096), bf16),
            pltpu.VMEM((SUB, 4096), bf16),
            pltpu.VMEM((ROWS, LOC), bf16),
            pltpu.VMEM((2, ROWS, TILE), f32),
            pltpu.VMEM((2, ROWS, TILE), f32),
            pltpu.VMEM((2, WIDE, LOC), bf16),
            pltpu.VMEM((2, SUB, TILE, LOC), bf16),
            pltpu.VMEM((4, 4, ROWS, TILE), bf16),
            pltpu.VMEM((8, SUB, WIDE), bf16),
            pltpu.VMEM((ROWS, LOC), f32),
            pltpu.VMEM((ROWS, LOC), f32),
            pltpu.VMEM((ROWS, LOC), f32),
            two, dma, dma, dma, two, two, dma((2, SUB)),
            two, two, dma((3,)), dma((3,)), two, two,
            dma, dma, two, two, two, two, two, two, dma((3,)), dma((3,)),
        ],
        compiler_params=pltpu.CompilerParams(
            collective_id=1, has_side_effects=True, vmem_limit_bytes=VMEM_LIMIT - OUT_ROOM),
        cost_estimate=pl.CostEstimate(flops=3_000_000_000, bytes_accessed=26_000_000, transcendentals=0),
        name="out_proj",
    )(o1, o2, x_loc, d, r, a_own, a_chip, wao, wmo)


def solution(mesh):
    both_axes = ("x", "yz")
    row_spec = P("dp", both_axes)
    in_w_spec = P("x", "yz")
    out_w_spec = P("yz", "x")
    cache_spec = P(("dp", "x", "yz"), None, None)
    len_spec = P(("dp", "x", "yz"))
    swap = [(0, 2), (2, 0), (1, 3), (3, 1)]

    def local_layer(x_loc, gain_loc, wqkv_loc, wgate_loc, wup_loc, wao_loc, wmo_loc, kc_loc, vc_loc, len_loc):
        qkv, sa, sb, r0, d, x_tall, lens = in_proj(x_loc, gain_loc, len_loc, wqkv_loc, wgate_loc, wup_loc)
        ra = lax.ppermute(sa, "x", swap)
        k_all, v_all, o1 = attend(0, SPLIT, lens, qkv, kc_loc, vc_loc)
        sb, o1 = lax.optimization_barrier((sb, o1))
        rb = lax.ppermute(sb, "x", swap)
        a_own, a_tall = act(d, r0, ra)
        a_chip = lax.ppermute(a_own, "x", swap)
        k_all, v_all, o2 = attend(SPLIT, SUB, lens, qkv, kc_loc, vc_loc, k_all, v_all)
        y_loc = out_proj(o1, o2, x_tall, d, rb, a_tall, a_chip, wao_loc, wmo_loc)
        return y_loc, k_all, v_all

    in_specs = (row_spec, P(both_axes), in_w_spec, in_w_spec, in_w_spec, out_w_spec, out_w_spec, cache_spec, cache_spec, len_spec)
    out_specs = (row_spec, cache_spec, cache_spec)
    return jax.shard_map(local_layer, mesh=mesh, in_specs=in_specs, out_specs=out_specs, check_vma=False)
```
